128 devices in a mesh: slab: 32 (over z, y, core), sub: 4 (over x).
Axes of the slice: x: 4, y: 4, z: 4, core: 2. Of those that a mesh axis runs over, the one named last changes fastest.
Arguments:
- factor_obs: float32 [128, 64, 64, 512], P('slab', 'sub'), may hold values from -0.1484375 to 0.1484375
- factor_ctrl: float32 [128, 64, 64, 512], P('slab', 'sub'), may hold values from -0.1484375 to 0.1484375
- diffusivity: float32 [128, 4096], P('slab', 'sub'), may hold values from 0.5 to 2
- input_map: float32 [4, 128, 4096], P(None, 'slab', 'sub'), may hold values from -1 to 1
- output_map: float32 [4, 128, 4096], P(None, 'slab', 'sub'), may hold values from -1 to 1
- start_block: float32 [512, 128], replicated, may hold values from -6 to 6
- order: int32 [1], replicated, may hold values from 64 to 128
Outputs:
- reduced_mass: float32 [128, 128], replicated
- reduced_state: float32 [128, 128], replicated
- reduced_input: float32 [128, 4], replicated
- reduced_output: float32 [4, 128], replicated
The draws below stay inside these ranges and needn't reach their ends.
All inputs are finite; a program needn't handle non-finite values.
Results may differ from the reference program's by a relative error of at most 0.00017.
Values sent between devices are 32-bit elements; how exact they have to be, the bound alone decides.
No kernel may reach another device: no remote copies, remote signals or barrier semaphores. Data moves between devices by JAX's collectives and lax.ppermute only.
A program may use at most 128 MiB of HBM per device.

```python
import math
import jax
import jax.numpy as jnp
from jax import lax

NX = 64
RANK = 512
RMAX = 128
NIN = 4
NOUT = 4
POWER = 2
NZ = 128
NY = 64
NYX = 4096
NCELL = 524288


def factor_draw(key, salt):
    key = jax.random.fold_in(key, salt)
    entry_key, level_key = jax.random.split(key)
    entries = jnp.clip(jax.random.normal(entry_key, (NZ, NY, NX, RANK), jnp.float32), -6.0, 6.0)
    level = jax.random.uniform(level_key, (NZ, NY, NX), jnp.float32) * math.log(10.0)
    rising = 1.0 + 2.0 * jnp.arange(NZ, dtype=jnp.float32) / max(NZ - 1, 1)
    scales = jnp.exp(level) * rising[:, None, None] / 9.65 * float(NCELL * RANK) ** (-0.25)
    return (entries * scales[..., None]).astype(jnp.float32)


def draw_factor_obs(key, part):
    return factor_draw(key, 11)


def draw_factor_ctrl(key, part):
    return factor_draw(key, 23)


def block_levels(rng, dims, pieces, smallest, high):
    def one(dim, parts):
        heights = jax.random.uniform(jax.random.fold_in(jax.random.fold_in(rng, 6), dim), (parts,), jnp.float32, smallest / len(pieces), high / len(pieces))
        return jnp.repeat(jnp.exp(heights), dims[dim] // parts).reshape((-1,) + (1,) * (len(dims) - dim - 1))

    level = one(*pieces[0])
    for cut in pieces[1:]:
        level = level * one(*cut)
    return level


def centred(rng, shape, spread, limit, cuts=(), kind=jnp.bfloat16):
    values = spread * jax.random.normal(rng, shape, jnp.float32)
    if cuts:
        values = values * block_levels(rng, shape, cuts, -0.22, 0.18)
    return jnp.clip(values, -limit, limit).astype(kind)


def setup_inputs(seed: int = 0) -> dict:
    key_list = jax.random.split(jax.random.key(seed), 8)
    factor_obs = draw_factor_obs(jax.random.fold_in(key_list[7], 71), 0)
    factor_ctrl = draw_factor_ctrl(jax.random.fold_in(key_list[7], 71), 0)
    diffusivity = jnp.clip(jnp.exp(math.log(2.0) - 1.3862944 * jax.random.uniform(key_list[2], (NZ, NYX), jnp.float32) ** block_levels(key_list[2], (NZ, NYX), ((0, 32), (1, 4)), -0.2, 0.2)), 0.5, 2.0)
    input_map = centred(key_list[3], (NIN, NZ, NYX), (max(NCELL // RANK // 32, 1)) ** -0.5, 1.0, ((1, 32), (2, 4)), jnp.float32)
    output_map = centred(key_list[4], (NOUT, NZ, NYX), (max(NCELL // RANK // 32, 1)) ** -0.5, 1.0, ((1, 32), (2, 4)), jnp.float32)
    start_block = centred(key_list[5], (RANK, RMAX), 1.0, 6.0, (), jnp.float32)
    order = jax.random.randint(key_list[6], (1,), RMAX // 2, RMAX + 1).astype(jnp.int32)
    return dict(factor_obs=factor_obs, factor_ctrl=factor_ctrl, diffusivity=diffusivity, input_map=input_map, output_map=output_map, start_block=start_block, order=order)


def matmul(first, second):
    return jnp.dot(first.astype(jnp.float32), second.astype(jnp.float32), precision=lax.Precision.HIGHEST, preferred_element_type=jnp.float32)

def orthonormal(start):
    gram = matmul(start.T, start)
    lower_factor = jnp.linalg.cholesky(gram)
    return lax.linalg.triangular_solve(lower_factor, start, left_side=False, lower=True, transpose_a=True)

def subspace_bases(cross_gram, start_block):
    right_basis = orthonormal(matmul(cross_gram.T, start_block))
    left_basis = orthonormal(matmul(cross_gram, right_basis))
    for repeat in range(POWER - 1):
        right_basis = orthonormal(matmul(cross_gram.T, left_basis))
        left_basis = orthonormal(matmul(cross_gram, right_basis))
    return (left_basis, right_basis)

def apply_stencil(field, conduct):
    padded = jnp.pad(field, ((1, 1), (1, 1), (1, 1), (0, 0)))
    center = padded[1:-1, 1:-1, 1:-1]
    beside = padded[2:, 1:-1, 1:-1] + padded[:-2, 1:-1, 1:-1]
    beside = beside + padded[1:-1, 2:, 1:-1] + padded[1:-1, :-2, 1:-1]
    beside = beside + padded[1:-1, 1:-1, 2:] + padded[1:-1, 1:-1, :-2]
    return conduct[..., None] * (beside - 6.0 * center) / 6.0

def reference(factor_obs, factor_ctrl, diffusivity, input_map, output_map, start_block, order):
    cell_count = NZ * NY * NX
    observe = factor_obs.reshape(cell_count, RANK)
    control = factor_ctrl.reshape(cell_count, RANK)
    cross_gram = matmul(observe.T, control)
    left_basis, right_basis = subspace_bases(cross_gram, start_block)
    ctrl_space = matmul(control, right_basis)
    obs_space = matmul(observe, left_basis)
    conduct = diffusivity.reshape(NZ, NY, NX)
    applied = apply_stencil(ctrl_space.reshape(NZ, NY, NX, RMAX), conduct).reshape(cell_count, RMAX)
    kept_mask = (jnp.arange(RMAX, dtype=jnp.int32) < order[0]).astype(jnp.float32)
    square_mask = kept_mask[:, None] * kept_mask[None, :]
    reduced_mass = square_mask * matmul(left_basis.T, matmul(cross_gram, right_basis))
    reduced_state = square_mask * matmul(obs_space.T, applied)
    drive = input_map.reshape(NIN, cell_count)
    sense = output_map.reshape(NOUT, cell_count)
    reduced_input = kept_mask[:, None] * matmul(drive, obs_space).T
    reduced_output = kept_mask[None, :] * matmul(sense, ctrl_space)
    return (reduced_mass, reduced_state, reduced_input, reduced_output)
```

```python
import functools

import jax
import jax.numpy as jnp
from jax import lax
from jax.experimental import pallas as pl
from jax.experimental.pallas import tpu as pltpu
from jax.sharding import PartitionSpec as P

ALL = ("slab", "sub")
F32 = jnp.float32
BF16 = jnp.bfloat16
PANEL = 32


def split2(x):
    high = x.astype(BF16)
    return high, (x - high.astype(F32)).astype(BF16)


def split3(x):
    high = x.astype(BF16)
    rest = x - high.astype(F32)
    mid = rest.astype(BF16)
    return high, mid, (rest - mid.astype(F32)).astype(BF16)


def product(a, b, contract=((1,), (0,))):
    return lax.dot_general(a, b, (contract, ((), ())), preferred_element_type=F32)


def product3(a, b, contract=((1,), (0,))):
    ah, al = split2(a)
    bh, bl = split2(b)
    return product(ah, bh, contract) + (product(ah, bl, contract) + product(al, bh, contract))


def product6(a, b, contract=((1,), (0,))):
    a0, a1, a2 = split3(a)
    b0, b1, b2 = split3(b)
    dot = functools.partial(product, contract=contract)
    small = dot(a1, b1) + (dot(a0, b2) + dot(a2, b0))
    return dot(a0, b0) + ((dot(a0, b1) + dot(a1, b0)) + small)


def rows_split(rows):
    both = jnp.concatenate([rows, rows], axis=0)
    high = both.astype(BF16).astype(F32)
    place = lax.broadcasted_iota(jnp.int32, both.shape, 0)
    halves = jnp.where(place < rows.shape[0], high, both - high)
    return jnp.concatenate([halves, jnp.zeros_like(halves)], axis=0).astype(BF16)


def add_products(total, extra, turned, few, right):
    count = turned.shape[0]
    th, tl = split2(turned)
    rh, rl = split2(right)
    first = product(jnp.concatenate([th, tl, few], axis=0), rh)
    second = product(jnp.concatenate([th, few], axis=0), rl)
    total[...] += first[:count] + (first[count : 2 * count] + second[:count])
    extra[...] += first[2 * count :] + second[count:]


def gram_kernel(steps, obs, ctrl, sense, gram, few, zlow, zhigh, ylow, yhigh, total, extra):
    step = pl.program_id(0)

    @pl.when(step == 0)
    def _():
        total[...] = jnp.zeros_like(total)
        extra[...] = jnp.zeros_like(extra)

    right = ctrl[...]
    side = ylow.shape[0]

    @pl.when(step < 2)
    def _():
        zlow[...] = right

    @pl.when(step >= steps - 2)
    def _():
        zhigh[...] = right

    @pl.when(step % 2 == 0)
    def _():
        ylow[...] = right[:side]

    @pl.when(step % 2 == 1)
    def _():
        yhigh[...] = right[right.shape[0] - side :]

    add_products(total, extra, obs[...].T, rows_split(sense[...]), right)

    @pl.when(step == steps - 1)
    def _():
        half = gram.shape[3]
        for side_index in range(2):
            cols = total[:, side_index * half : (side_index + 1) * half]
            gram[:, side_index] = cols.reshape(gram.shape[0], gram.shape[2], half)
        few[...] = extra[:8]


def local_gram(observe, control, sense, lines, points):
    cells, rank = control.shape
    steps = 8
    rows = cells // steps
    plane = 2 * rows
    block = pl.BlockSpec((rows, rank), lambda i: (i, 0))
    return pl.pallas_call(
        functools.partial(gram_kernel, steps),
        grid=(steps,),
        in_specs=[block, block, pl.BlockSpec((sense.shape[0], rows), lambda i: (0, i))],
        out_specs=[
            pl.BlockSpec((64, 2, 8, rank // 2), lambda i: (0, 0, 0, 0)),
            pl.BlockSpec((8, rank), lambda i: (0, 0)),
            pl.BlockSpec((rows, rank), lambda i: (jnp.minimum(i, 1), 0)),
            pl.BlockSpec((rows, rank), lambda i: (jnp.maximum(i - (steps - 2), 0), 0)),
            pl.BlockSpec((points, rank), lambda i: (i // 2, 0)),
            pl.BlockSpec((points, rank), lambda i: (i // 2, 0)),
        ],
        out_shape=[
            jax.ShapeDtypeStruct((64, 2, 8, rank // 2), F32),
            jax.ShapeDtypeStruct((8, rank), F32),
            jax.ShapeDtypeStruct((plane, rank), F32),
            jax.ShapeDtypeStruct((plane, rank), F32),
            jax.ShapeDtypeStruct((steps // 2 * points, rank), F32),
            jax.ShapeDtypeStruct((steps // 2 * points, rank), F32),
        ],
        scratch_shapes=[pltpu.VMEM((rank, rank), F32), pltpu.VMEM((16, rank), F32)],
        compiler_params=pltpu.CompilerParams(vmem_limit_bytes=40 << 20),
        cost_estimate=pl.CostEstimate(
            flops=6 * cells * rank * rank, bytes_accessed=24 << 20, transcendentals=0
        ),
        name="local_gram",
    )(observe, control, sense)


def stencil_kernel(
    steps, lines, points,
    obs, conduct, drive, few_ctrl, ctrl, zlow, zhigh, ylow, yhigh,
    out, field, total, extra, sems,
):
    step = pl.program_id(0)
    planes = steps // 2
    inner = pl.ds(1, lines)
    copies = [pltpu.make_async_copy(zlow, field.at[0, inner], sems.at[0])]
    for p in range(planes):
        copies.append(pltpu.make_async_copy(ctrl.at[p], field.at[p + 1, inner], sems.at[p + 1]))
    copies.append(pltpu.make_async_copy(zhigh, field.at[planes + 1, inner], sems.at[planes + 1]))
    sides = [
        pltpu.make_async_copy(ylow, field.at[pl.ds(1, planes), 0], sems.at[planes + 2]),
        pltpu.make_async_copy(yhigh, field.at[pl.ds(1, planes), lines + 1], sems.at[planes + 3]),
    ]

    @pl.when(step == 0)
    def _():
        for copy in copies[:3] + sides + copies[3:]:
            copy.start()
        total[...] = jnp.zeros_like(total)
        extra[...] = jnp.zeros_like(extra)
        for copy in copies[:3] + sides:
            copy.wait()

    for p in range(1, planes):

        @pl.when(step == 2 * p)
        def _():
            copies[p + 2].wait()

    p = step // 2
    half = lines // 2
    line = (step % 2) * half

    def part(plane, first):
        return field[plane, pl.ds(first, half)]

    center = part(p + 1, line + 1)
    beside = part(p + 2, line + 1) + part(p, line + 1)
    beside = beside + part(p + 1, line + 2) + part(p + 1, line)
    rows = half * points
    rank = center.shape[-1]
    center = center.reshape(rows, rank)
    beside = beside.reshape(rows, rank)
    place = lax.broadcasted_iota(jnp.int32, (rows, rank), 0) % points
    beside = beside + jnp.where(place > 0, pltpu.roll(center, 1, 0), 0.0)
    beside = beside + jnp.where(place < points - 1, pltpu.roll(center, rows - 1, 0), 0.0)
    applied = (beside - 6.0 * center).T * (conduct[0] * (1.0 / 6.0))
    add_products(total, extra, applied, rows_split(drive[...]), obs[...])

    @pl.when(step == steps - 1)
    def _():
        width = rank // 2
        for side_index in range(2):
            cols = total[:, side_index * width : (side_index + 1) * width]
            out[:, side_index, :, :width] = cols.reshape(out.shape[0], out.shape[2], width)
        summed = jnp.concatenate([extra[0:4] + extra[4:8], few_ctrl[0:4] + few_ctrl[4:8]], axis=0)
        wide = jnp.concatenate([summed, jnp.zeros((120, rank), F32)], axis=0).T
        out[:, 0, :, width:] = wide.reshape(out.shape[0], out.shape[2], 128)
        out[:, 1, :, width:] = jnp.zeros((out.shape[0], out.shape[2], 128), F32)


def local_operator(observe, control4, conduct, drive, few_ctrl, zlow, zhigh, ylow, yhigh):
    planes, lines, points, rank = control4.shape
    cells = planes * lines * points
    steps = 2 * planes
    rows = cells // steps
    anywhere = pl.BlockSpec(memory_space=pl.ANY)
    return pl.pallas_call(
        functools.partial(stencil_kernel, steps, lines, points),
        grid=(steps,),
        in_specs=[
            pl.BlockSpec((rows, rank), lambda i: (i, 0)),
            pl.BlockSpec((1, 1, rows), lambda i: (i, 0, 0)),
            pl.BlockSpec((drive.shape[0], rows), lambda i: (0, i)),
            pl.BlockSpec((8, rank), lambda i: (0, 0)),
        ]
        + [anywhere] * 5,
        out_specs=pl.BlockSpec((64, 2, 8, rank // 2 + 128), lambda i: (0, 0, 0, 0)),
        out_shape=jax.ShapeDtypeStruct((64, 2, 8, rank // 2 + 128), F32),
        scratch_shapes=[
            pltpu.VMEM((planes + 2, lines + 2, points, rank), F32),
            pltpu.VMEM((rank, rank), F32),
            pltpu.VMEM((16, rank), F32),
            pltpu.SemaphoreType.DMA((planes + 4,)),
        ],
        compiler_params=pltpu.CompilerParams(vmem_limit_bytes=44 << 20),
        cost_estimate=pl.CostEstimate(
            flops=6 * cells * rank * rank, bytes_accessed=24 << 20, transcendentals=0
        ),
        name="local_operator",
    )(
        observe,
        conduct.reshape(steps, 1, rows),
        drive,
        few_ctrl,
        control4,
        zlow.reshape(lines, points, rank),
        zhigh.reshape(lines, points, rank),
        ylow.reshape(planes, points, rank),
        yhigh.reshape(planes, points, rank),
    )


def sum_kernel(parts, out):
    whole = jnp.sum(parts[...], axis=0, keepdims=True)
    out[...] = jnp.broadcast_to(whole, out.shape)


def summed_everywhere(parts, name):
    shape = parts.shape
    tiles = parts.reshape(shape[0] * shape[1], *shape[2:])
    arrived = lax.all_to_all(tiles, ALL, 0, 0, tiled=True)
    copies = pl.pallas_call(
        sum_kernel,
        out_shape=jax.ShapeDtypeStruct(tiles.shape, F32),
        cost_estimate=pl.CostEstimate(
            flops=tiles.size, bytes_accessed=8 * tiles.size, transcendentals=0
        ),
        name="sum_" + name,
    )(arrived)
    return lax.all_to_all(copies, ALL, 0, 0, tiled=True).reshape(shape)


def inverse_factor(work):
    size = work.shape[0]
    for first in range(0, size, PANEL):
        last = first + PANEL
        panel = [work[first + 8 * g : first + 8 * g + 8, :] for g in range(PANEL // 8)]
        groups = PANEL // 8
        columns = {}
        for k in range(PANEL):
            for g in range(k // 8, groups):
                columns[k, g] = jnp.broadcast_to(
                    panel[g][:, first + k : first + k + 1], (8, 128)
                )
        place = lax.broadcasted_iota(jnp.int32, (8, 128), 0)
        for j in range(PANEL):
            gj, sj = divmod(j, 8)
            pivot = jnp.broadcast_to(columns[j, gj][sj : sj + 1], (8, 128))
            scale = lax.rsqrt(pivot)
            lower = {}
            for g in range(gj, groups):
                lower[g] = columns[j, g] * scale
            row = jnp.broadcast_to(panel[gj][sj : sj + 1], (8, 256))
            row = row * jnp.concatenate([scale, scale], axis=1)
            for k in range(j + 1, PANEL):
                gk, sk = divmod(k, 8)
                across = jnp.broadcast_to(lower[gk][sk : sk + 1], (8, 128))
                for g in range(gk, groups):
                    columns[k, g] = columns[k, g] - lower[g] * across
            for g in range(gj, groups):
                weight = lower[g]
                if g == gj:
                    weight = jnp.where(place > sj, weight, 0.0)
                wide = jnp.concatenate([weight, weight], axis=1)
                panel[g] = panel[g] - wide * row
            wide_place = lax.broadcasted_iota(jnp.int32, (8, 256), 0)
            panel[gj] = jnp.where(wide_place == sj, row, panel[gj])
        for g in range(groups):
            work[first + 8 * g : first + 8 * g + 8, :] = panel[g]
        if last < size:
            done = jnp.concatenate(panel, axis=0)
            u0, u1, u2 = split3(done)
            left = jnp.concatenate([u0, u0, u1, u1, u0, u2], axis=0)[:, :size]
            right = jnp.concatenate([u0, u1, u0, u1, u2, u0], axis=0)
            change = product(left, right, ((0,), (0,)))
            work[last:, :] -= change[last:, :]


def bases_kernel(turn_start, gram, start, right_out, left_out, image_out, cross, basis, image, work):
    rank = cross.shape[0]
    half = rank // 2
    for side_index in range(2):
        cols = gram[:, side_index].reshape(rank, half)
        cross[:, side_index * half : (side_index + 1) * half] = cols
    basis[...] = start[...].T if turn_start else start[...]
    size = basis.shape[0]
    eye = (
        lax.broadcasted_iota(jnp.int32, (size, size), 0)
        == lax.broadcasted_iota(jnp.int32, (size, size), 1)
    ).astype(F32)

    @pl.loop(0, 2)
    def _(turn):
        @pl.when(turn == 0)
        def _():
            image[...] = product3(basis[...], cross[...])

        @pl.when(turn == 1)
        def _():
            image[...] = product3(basis[...], cross[...], ((1,), (1,)))

        held = image[...]
        work[:, :size] = product6(held, held, ((1,), (1,)))
        work[:, size:] = eye
        inverse_factor(work)
        basis[...] = product6(work[:, size:], held)

        @pl.when(turn == 0)
        def _():
            right_out[...] = basis[...]

    left_out[...] = basis[...]
    image_out[...] = image[...]


def two_bases(gram, start, turn_start, name):
    rank = gram.shape[0] * gram.shape[2]
    size = 128
    shape = jax.ShapeDtypeStruct((size, rank), F32)
    return pl.pallas_call(
        functools.partial(bases_kernel, turn_start),
        out_shape=[shape, shape, shape],
        scratch_shapes=[
            pltpu.VMEM((rank, rank), F32),
            pltpu.VMEM((size, rank), F32),
            pltpu.VMEM((size, rank), F32),
            pltpu.VMEM((size, 2 * size), F32),
        ],
        compiler_params=pltpu.CompilerParams(vmem_limit_bytes=24 << 20),
        cost_estimate=pl.CostEstimate(
            flops=10_000_000_000, bytes_accessed=4 << 20, transcendentals=0
        ),
        name=name,
    )(gram, start)


def finish_kernel(order, right, left, image, oper, mass, state, inputs, outputs, turned):
    size, rank = right.shape
    half = rank // 2
    for side_index in range(2):
        cols = oper[:, side_index, :, :half].reshape(rank, half)
        turned[:, side_index * half : (side_index + 1) * half] = cols
    few = oper[:, 0, :, half:].reshape(rank, 128)
    kept_col = lax.broadcasted_iota(jnp.int32, (size, size), 0) < order[0]
    kept_row = lax.broadcasted_iota(jnp.int32, (size, size), 1) < order[0]
    kept = jnp.logical_and(kept_col, kept_row).astype(F32)
    both = ((1,), (1,))
    mass[...] = kept * product6(left[...], image[...], both)
    state[...] = kept * product3(left[...], product3(right[...], turned[...]), both)
    inputs[...] = (kept_col.astype(F32) * product3(left[...], few))[:, :4]
    outputs[...] = (kept_row.astype(F32) * product3(right[...], few).T)[4:8]


def finish(order, right, left, image, oper):
    size, rank = right.shape
    vmem = pl.BlockSpec(memory_space=pltpu.VMEM)
    return pl.pallas_call(
        finish_kernel,
        in_specs=[pl.BlockSpec(memory_space=pltpu.SMEM)] + [vmem] * 4,
        out_specs=[vmem] * 4,
        out_shape=[
            jax.ShapeDtypeStruct((size, size), F32),
            jax.ShapeDtypeStruct((size, size), F32),
            jax.ShapeDtypeStruct((size, 4), F32),
            jax.ShapeDtypeStruct((4, size), F32),
        ],
        scratch_shapes=[pltpu.VMEM((rank, rank), F32)],
        compiler_params=pltpu.CompilerParams(vmem_limit_bytes=24 << 20),
        cost_estimate=pl.CostEstimate(
            flops=1_000_000_000, bytes_accessed=4 << 20, transcendentals=0
        ),
        name="finish",
    )(order, right, left, image, oper)


def from_neighbours(low_face, high_face, axis):
    count = lax.axis_size(axis)
    up = [(i, i + 1) for i in range(count - 1)]
    down = [(b, a) for a, b in up]
    return lax.ppermute(high_face, axis, up), lax.ppermute(low_face, axis, down)


def on_device(factor_obs, factor_ctrl, diffusivity, input_map, output_map, start_block, order):
    planes, lines, points, rank = factor_ctrl.shape
    cells = planes * lines * points
    observe = factor_obs.reshape(cells, rank)
    control = factor_ctrl.reshape(cells, rank)
    drive = input_map.reshape(input_map.shape[0], cells)
    sense = output_map.reshape(output_map.shape[0], cells)
    gram, few_ctrl, zlow, zhigh, ylow, yhigh = local_gram(observe, control, sense, lines, points)
    gram = summed_everywhere(gram, "gram")
    zlow, zhigh = from_neighbours(zlow, zhigh, "slab")
    ylow, yhigh = from_neighbours(ylow, yhigh, "sub")
    oper = local_operator(
        observe, factor_ctrl, diffusivity, drive, few_ctrl, zlow, zhigh, ylow, yhigh
    )
    oper = summed_everywhere(oper, "operator")
    _, left, _ = two_bases(gram, start_block, True, "first_bases")
    right, left, image = two_bases(gram, left, False, "second_bases")
    return finish(order, right, left, image, oper)


def solution(mesh):
    placed = (
        P("slab", "sub", None, None),
        P("slab", "sub", None, None),
        P("slab", "sub"),
        P(None, "slab", "sub"),
        P(None, "slab", "sub"),
        P(),
        P(),
    )
    return jax.shard_map(
        on_device, mesh=mesh, in_specs=placed, out_specs=(P(), P(), P(), P()), check_vma=False
    )
```

```python
import functools

import jax
import jax.numpy as jnp
from jax import lax
from jax.experimental import pallas as pl
from jax.experimental.pallas import tpu as pltpu
from jax.sharding import PartitionSpec as P


ALL = ("slab", "sub")
F32 = jnp.float32
BF16 = jnp.bfloat16
PANEL = 32


def split2(x):
    high = x.astype(BF16)
    return high, (x - high.astype(F32)).astype(BF16)


def split3(x):
    high = x.astype(BF16)
    rest = x - high.astype(F32)
    mid = rest.astype(BF16)
    return high, mid, (rest - mid.astype(F32)).astype(BF16)


def product(a, b, contract=((1,), (0,))):
    return lax.dot_general(a, b, (contract, ((), ())), preferred_element_type=F32)


def product3(a, b, contract=((1,), (0,))):
    ah, al = split2(a)
    bh, bl = split2(b)
    return product(ah, bh, contract) + (product(ah, bl, contract) + product(al, bh, contract))


def product6(a, b, contract=((1,), (0,))):
    a0, a1, a2 = split3(a)
    b0, b1, b2 = split3(b)
    dot = functools.partial(product, contract=contract)
    small = dot(a1, b1) + (dot(a0, b2) + dot(a2, b0))
    return dot(a0, b0) + ((dot(a0, b1) + dot(a1, b0)) + small)


def rows_split(rows):
    both = jnp.concatenate([rows, rows], axis=0)
    high = both.astype(BF16).astype(F32)
    place = lax.broadcasted_iota(jnp.int32, both.shape, 0)
    halves = jnp.where(place < rows.shape[0], high, both - high)
    return jnp.concatenate([halves, jnp.zeros_like(halves)], axis=0).astype(BF16)


def add_products(total, extra, turned, few, right):
    count = turned.shape[0]
    th, tl = split2(turned)
    rh, rl = split2(right)
    top = jnp.concatenate([th, tl, th], axis=1)
    bottom = jnp.concatenate([few, jnp.zeros_like(few), few], axis=1)
    result = product(
        jnp.concatenate([top, bottom], axis=0), jnp.concatenate([rh, rh, rl], axis=0)
    )
    total[...] += result[:count]
    extra[...] += result[count:]


def in_chunks(total, out):
    width = total.shape[1] // 2
    for side in range(2):
        cols = total[:, side * width : (side + 1) * width]
        out[:, side, :, :width] = cols.reshape(out.shape[0], out.shape[2], width)


def gram_kernel(obs, ctrl, sense, gram, few, obs_here, ctrl_here, total, extra, obs_sems, ctrl_sems):
    planes = obs.shape[0]

    def copies(p):
        return (
            pltpu.make_async_copy(obs.at[p], obs_here.at[p], obs_sems.at[p]),
            pltpu.make_async_copy(ctrl.at[p], ctrl_here.at[p], ctrl_sems.at[p]),
        )

    for p in range(planes):
        for copy in copies(p):
            copy.start()
    total[...] = jnp.zeros_like(total)
    extra[...] = jnp.zeros_like(extra)

    @pl.loop(0, planes)
    def _(p):
        for copy in copies(p):
            copy.wait()
        rows = rows_split(sense[:, pl.ds(pl.multiple_of(p * obs.shape[1], 128), obs.shape[1])])
        add_products(total, extra, obs_here[p].T, rows, ctrl_here[p])

    in_chunks(total, gram)
    few[...] = extra[:8]


def local_gram(observe, control, sense):
    blocks, rows, rank = observe.shape
    anywhere = pl.BlockSpec(memory_space=pltpu.HBM)
    vmem = pl.BlockSpec(memory_space=pltpu.VMEM)
    return pl.pallas_call(
        gram_kernel,
        in_specs=[anywhere, anywhere, vmem],
        out_specs=[vmem, vmem],
        out_shape=[
            jax.ShapeDtypeStruct((64, 2, 8, rank // 2), F32),
            jax.ShapeDtypeStruct((8, rank), F32),
        ],
        scratch_shapes=[
            pltpu.VMEM((blocks, rows, rank), F32),
            pltpu.VMEM((blocks, rows, rank), F32),
            pltpu.VMEM((rank, rank), F32),
            pltpu.VMEM((16, rank), F32),
            pltpu.SemaphoreType.DMA((blocks,)),
            pltpu.SemaphoreType.DMA((blocks,)),
        ],
        compiler_params=pltpu.CompilerParams(vmem_limit_bytes=60 << 20),
        cost_estimate=pl.CostEstimate(
            flops=6 * blocks * rows * rank * rank, bytes_accessed=18 << 20, transcendentals=0
        ),
        name="local_gram",
    )(observe, control, sense)


def stencil_kernel(
    lines, points,
    obs, conduct, drive, few_ctrl, ctrl, zlow, zhigh, ylow, yhigh,
    out, field, obs_here, total, extra, sems, obs_sems,
):
    steps = obs.shape[0]
    planes = steps // 2
    inner = pl.ds(1, lines)
    copies = [pltpu.make_async_copy(zlow, field.at[0, inner], sems.at[0])]
    for p in range(planes):
        copies.append(pltpu.make_async_copy(ctrl.at[p], field.at[p + 1, inner], sems.at[p + 1]))
    copies.append(pltpu.make_async_copy(zhigh, field.at[planes + 1, inner], sems.at[planes + 1]))
    sides = [
        pltpu.make_async_copy(ylow, field.at[pl.ds(1, planes), 0], sems.at[planes + 2]),
        pltpu.make_async_copy(yhigh, field.at[pl.ds(1, planes), lines + 1], sems.at[planes + 3]),
    ]

    def obs_copy(step):
        return pltpu.make_async_copy(obs.at[step], obs_here.at[step], obs_sems.at[step])

    for copy in copies[:3] + sides:
        copy.start()
    obs_copy(0).start()
    obs_copy(1).start()
    for p in range(1, planes):
        copies[p + 2].start()
        obs_copy(2 * p).start()
        obs_copy(2 * p + 1).start()
    total[...] = jnp.zeros_like(total)
    extra[...] = jnp.zeros_like(extra)
    for copy in copies[:3] + sides:
        copy.wait()

    @pl.loop(0, steps)
    def _(step):
        for p in range(1, planes):

            @pl.when(step == 2 * p)
            def _():
                copies[p + 2].wait()

        obs_copy(step).wait()
        p = step // 2
        half = lines // 2
        line = (step % 2) * half

        def part(plane, first):
            return field[plane, pl.ds(first, half)]

        center = part(p + 1, line + 1)
        beside = part(p + 2, line + 1) + part(p, line + 1)
        beside = beside + part(p + 1, line + 2) + part(p + 1, line)
        rows = half * points
        rank = center.shape[-1]
        center = center.reshape(rows, rank)
        beside = beside.reshape(rows, rank)
        place = lax.broadcasted_iota(jnp.int32, (rows, rank), 0) % points
        beside = beside + jnp.where(place > 0, pltpu.roll(center, 1, 0), 0.0)
        beside = beside + jnp.where(place < points - 1, pltpu.roll(center, rows - 1, 0), 0.0)
        applied = (beside - 6.0 * center).T * (conduct[step] * (1.0 / 6.0))
        some = rows_split(drive[:, pl.ds(pl.multiple_of(step * rows, 128), rows)])
        add_products(total, extra, applied, some, obs_here[step])

    in_chunks(total, out)
    rank = total.shape[1]
    summed = jnp.concatenate([extra[0:4] + extra[4:8], few_ctrl[0:4] + few_ctrl[4:8]], axis=0)
    wide = jnp.concatenate([summed, jnp.zeros((120, rank), F32)], axis=0).T
    out[:, 0, :, rank // 2 :] = wide.reshape(out.shape[0], out.shape[2], 128)
    out[:, 1, :, rank // 2 :] = jnp.zeros((out.shape[0], out.shape[2], 128), F32)


def local_operator(observe, control, conduct, drive, few_ctrl, zlow, zhigh, ylow, yhigh):
    planes, lines, points, rank = control.shape
    steps = 2 * planes
    rows = lines * points // 2
    anywhere = pl.BlockSpec(memory_space=pltpu.HBM)
    vmem = pl.BlockSpec(memory_space=pltpu.VMEM)
    return pl.pallas_call(
        functools.partial(stencil_kernel, lines, points),
        in_specs=[anywhere, vmem, vmem, vmem] + [anywhere] * 5,
        out_specs=vmem,
        out_shape=jax.ShapeDtypeStruct((64, 2, 8, rank // 2 + 128), F32),
        scratch_shapes=[
            pltpu.VMEM((planes + 2, lines + 2, points, rank), F32),
            pltpu.VMEM((steps, rows, rank), F32),
            pltpu.VMEM((rank, rank), F32),
            pltpu.VMEM((16, rank), F32),
            pltpu.SemaphoreType.DMA((planes + 4,)),
            pltpu.SemaphoreType.DMA((steps,)),
        ],
        compiler_params=pltpu.CompilerParams(vmem_limit_bytes=44 << 20),
        cost_estimate=pl.CostEstimate(
            flops=6 * steps * rows * rank * rank, bytes_accessed=24 << 20, transcendentals=0
        ),
        name="local_operator",
    )(
        observe.reshape(steps, rows, rank),
        conduct.reshape(steps, 1, rows),
        drive,
        few_ctrl,
        control,
        zlow.reshape(lines, points, rank),
        zhigh.reshape(lines, points, rank),
        ylow.reshape(planes, points, rank),
        yhigh.reshape(planes, points, rank),
    )


def sum_kernel(parts, out):
    whole = jnp.sum(parts[...], axis=0, keepdims=True)
    out[...] = jnp.broadcast_to(whole, out.shape)


def scattered(parts):
    tiles = parts.reshape(parts.shape[0] * parts.shape[1], *parts.shape[2:])
    return lax.all_to_all(tiles, ALL, 0, 0, tiled=True)


def summed_copies(arrived):
    return pl.pallas_call(
        sum_kernel,
        out_shape=jax.ShapeDtypeStruct(arrived.shape, F32),
        compiler_params=pltpu.CompilerParams(vmem_limit_bytes=6 << 20),
        cost_estimate=pl.CostEstimate(
            flops=arrived.size, bytes_accessed=8 * arrived.size, transcendentals=0
        ),
        name="sum_gram",
    )(arrived)


def project_kernel(side, parts, left, out):
    block = jnp.sum(parts[...], axis=0)
    half = left.shape[1] // 2
    mine = jnp.where(side[0] == 0, left[:, :half], left[:, half:])
    turned = product3(block[:, :half], mine, ((1,), (1,)))
    whole = jnp.concatenate([turned, block[:, half:]], axis=1)
    out[...] = jnp.broadcast_to(whole[None], out.shape)


def projected_copies(arrived, left):
    side = lax.axis_index("sub") & 1
    vmem = pl.BlockSpec(memory_space=pltpu.VMEM)
    return pl.pallas_call(
        project_kernel,
        in_specs=[pl.BlockSpec(memory_space=pltpu.SMEM), vmem, vmem],
        out_specs=vmem,
        out_shape=jax.ShapeDtypeStruct((arrived.shape[0], 8, 256), F32),
        compiler_params=pltpu.CompilerParams(vmem_limit_bytes=8 << 20),
        cost_estimate=pl.CostEstimate(
            flops=arrived.size, bytes_accessed=8 * arrived.size, transcendentals=0
        ),
        name="project",
    )(side.reshape(1).astype(jnp.int32), arrived, left)


def gathered(copies):
    tiles = lax.all_to_all(copies, ALL, 0, 0, tiled=True)
    return tiles.reshape(64, 2, *tiles.shape[1:])


def inverse_factor(work):
    size = work.shape[0]
    for first in range(0, size, PANEL):
        last = first + PANEL
        panel = [work[first + 8 * g : first + 8 * g + 8, :] for g in range(PANEL // 8)]
        groups = PANEL // 8
        columns = {}
        for k in range(PANEL):
            for g in range(k // 8, groups):
                columns[k, g] = jnp.broadcast_to(
                    panel[g][:, first + k : first + k + 1], (8, 128)
                )
        place = lax.broadcasted_iota(jnp.int32, (8, 128), 0)
        for j in range(PANEL):
            gj, sj = divmod(j, 8)
            pivot = jnp.broadcast_to(columns[j, gj][sj : sj + 1], (8, 128))
            scale = lax.rsqrt(pivot)
            lower = {}
            for g in range(gj, groups):
                lower[g] = columns[j, g] * scale
            row = jnp.broadcast_to(panel[gj][sj : sj + 1], (8, 256))
            row = row * jnp.concatenate([scale, scale], axis=1)
            for k in range(j + 1, PANEL):
                gk, sk = divmod(k, 8)
                across = jnp.broadcast_to(lower[gk][sk : sk + 1], (8, 128))
                for g in range(gk, groups):
                    columns[k, g] = columns[k, g] - lower[g] * across
            for g in range(gj, groups):
                weight = lower[g]
                if g == gj:
                    weight = jnp.where(place > sj, weight, 0.0)
                wide = jnp.concatenate([weight, weight], axis=1)
                panel[g] = panel[g] - wide * row
            wide_place = lax.broadcasted_iota(jnp.int32, (8, 256), 0)
            panel[gj] = jnp.where(wide_place == sj, row, panel[gj])
        for g in range(groups):
            work[first + 8 * g : first + 8 * g + 8, :] = panel[g]
        if last < size:
            done = jnp.concatenate(panel, axis=0)
            u0, u1, u2 = split3(done)
            left = jnp.concatenate([u0, u0, u1, u1, u0, u2], axis=0)[:, :size]
            right = jnp.concatenate([u0, u1, u0, u1, u2, u0], axis=0)
            change = product(left, right, ((0,), (0,)))
            work[last:, :] -= change[last:, :]


def bases_kernel(gram, start, right_out, left_out, image_out, cross, basis, work):
    rank = cross.shape[0]
    half = rank // 2
    for side in range(2):
        cross[:, side * half : (side + 1) * half] = gram[:, side].reshape(rank, half)
    basis[...] = start[...].T
    size = basis.shape[0]
    eye = (
        lax.broadcasted_iota(jnp.int32, (size, size), 0)
        == lax.broadcasted_iota(jnp.int32, (size, size), 1)
    ).astype(F32)

    @pl.loop(0, 4)
    def _(turn):
        @pl.when(turn % 2 == 0)
        def _():
            image_out[...] = product3(basis[...], cross[...])

        @pl.when(turn % 2 == 1)
        def _():
            image_out[...] = product3(basis[...], cross[...], ((1,), (1,)))

        held = image_out[...]
        work[:, :size] = product6(held, held, ((1,), (1,)))
        work[:, size:] = eye
        inverse_factor(work)
        basis[...] = product6(work[:, size:], held)

        @pl.when(turn == 2)
        def _():
            right_out[...] = basis[...]

    left_out[...] = basis[...]


def bases(gram, start):
    rank, size = start.shape
    shape = jax.ShapeDtypeStruct((size, rank), F32)
    return pl.pallas_call(
        bases_kernel,
        out_shape=[shape, shape, shape],
        scratch_shapes=[
            pltpu.VMEM((rank, rank), F32),
            pltpu.VMEM((size, rank), F32),
            pltpu.VMEM((size, 2 * size), F32),
        ],
        compiler_params=pltpu.CompilerParams(vmem_limit_bytes=16 << 20),
        cost_estimate=pl.CostEstimate(
            flops=20_000_000_000, bytes_accessed=4 << 20, transcendentals=0
        ),
        name="bases",
    )(gram, start)


def finish_kernel(order, right, left, image, blocks, mass, state, inputs, outputs):
    size, rank = right.shape
    turned = (blocks[:, 0, :, :size] + blocks[:, 1, :, :size]).reshape(rank, size)
    few = blocks[:, 0, :, size:].reshape(rank, 128)
    kept_col = lax.broadcasted_iota(jnp.int32, (size, size), 0) < order[0]
    kept_row = lax.broadcasted_iota(jnp.int32, (size, size), 1) < order[0]
    kept = jnp.logical_and(kept_col, kept_row).astype(F32)
    mass[...] = kept * product6(left[...], image[...], ((1,), (1,)))
    state[...] = kept * product3(right[...], turned).T
    inputs[...] = (kept_row.astype(F32) * product3(left[...], few).T)[:4]
    outputs[...] = (kept_row.astype(F32) * product3(right[...], few).T)[4:8]


def finish(order, right, left, image, blocks):
    size, _ = right.shape
    vmem = pl.BlockSpec(memory_space=pltpu.VMEM)
    return pl.pallas_call(
        finish_kernel,
        in_specs=[pl.BlockSpec(memory_space=pltpu.SMEM)] + [vmem] * 4,
        out_specs=[vmem] * 4,
        out_shape=[
            jax.ShapeDtypeStruct((size, size), F32),
            jax.ShapeDtypeStruct((size, size), F32),
            jax.ShapeDtypeStruct((4, size), F32),
            jax.ShapeDtypeStruct((4, size), F32),
        ],
        compiler_params=pltpu.CompilerParams(vmem_limit_bytes=16 << 20),
        cost_estimate=pl.CostEstimate(
            flops=1_000_000_000, bytes_accessed=4 << 20, transcendentals=0
        ),
        name="finish",
    )(order, right, left, image, blocks)


def from_neighbours(low_face, high_face, axis):
    count = lax.axis_size(axis)
    up = [(i, i + 1) for i in range(count - 1)]
    down = [(b, a) for a, b in up]
    return lax.ppermute(high_face, axis, up), lax.ppermute(low_face, axis, down)


def reduced(factor_obs, factor_ctrl, diffusivity, input_map, output_map, start_block, order):
    planes, lines, points, rank = factor_ctrl.shape
    cells = planes * lines * points
    drive = input_map.reshape(input_map.shape[0], cells)
    sense = output_map.reshape(output_map.shape[0], cells)
    zlow, zhigh = from_neighbours(factor_ctrl[:1], factor_ctrl[-1:], "slab")
    ylow, yhigh = from_neighbours(factor_ctrl[:, :1], factor_ctrl[:, -1:], "sub")
    gram, few_ctrl = local_gram(
        factor_obs.reshape(planes, lines * points, rank),
        factor_ctrl.reshape(planes, lines * points, rank),
        sense,
    )
    gram = summed_copies(scattered(gram))
    gram = gathered(gram)
    oper = local_operator(
        factor_obs, factor_ctrl, diffusivity, drive, few_ctrl, zlow, zhigh, ylow, yhigh
    )
    oper = scattered(oper)
    right, left, image = bases(gram, start_block)
    blocks = gathered(projected_copies(oper, left))
    mass, state, inputs, outputs = finish(order, right, left, image, blocks)
    return mass, state, inputs.T, outputs


def solution(mesh):
    placed = (
        P("slab", "sub", None, None),
        P("slab", "sub", None, None),
        P("slab", "sub"),
        P(None, "slab", "sub"),
        P(None, "slab", "sub"),
        P(),
        P(),
    )
    return jax.shard_map(
        reduced, mesh=mesh, in_specs=placed, out_specs=(P(), P(), P(), P()), check_vma=False
    )
```

```python
import functools

import jax
import jax.numpy as jnp
from jax import lax
from jax.experimental import pallas as pl
from jax.experimental.pallas import tpu as pltpu
from jax.sharding import PartitionSpec as P


ALL = ("slab", "sub")
F32 = jnp.float32
BF16 = jnp.bfloat16
PANEL = 32
AHEAD = 3


def split2(x):
    high = x.astype(BF16)
    return high, (x - high.astype(F32)).astype(BF16)


def split3(x):
    high = x.astype(BF16)
    rest = x - high.astype(F32)
    mid = rest.astype(BF16)
    return high, mid, (rest - mid.astype(F32)).astype(BF16)


def product(a, b, contract=((1,), (0,))):
    return lax.dot_general(a, b, (contract, ((), ())), preferred_element_type=F32)


def product3(a, b, contract=((1,), (0,))):
    ah, al = split2(a)
    bh, bl = split2(b)
    return product(ah, bh, contract) + (product(ah, bl, contract) + product(al, bh, contract))


def product6(a, b, contract=((1,), (0,))):
    a0, a1, a2 = split3(a)
    b0, b1, b2 = split3(b)
    dot = functools.partial(product, contract=contract)
    small = dot(a1, b1) + (dot(a0, b2) + dot(a2, b0))
    return dot(a0, b0) + ((dot(a0, b1) + dot(a1, b0)) + small)


def rows_split(rows):
    both = jnp.concatenate([rows, rows], axis=0)
    high = both.astype(BF16).astype(F32)
    place = lax.broadcasted_iota(jnp.int32, both.shape, 0)
    halves = jnp.where(place < rows.shape[0], high, both - high)
    return jnp.concatenate([halves, jnp.zeros_like(halves)], axis=0).astype(BF16)


def add_products(total, turned, right, extra=None, few=None):
    count = turned.shape[0]
    th, tl = split2(turned)
    rh, rl = split2(right)
    left = jnp.concatenate([th, tl, th], axis=1)
    if few is not None:
        bottom = jnp.concatenate([few, jnp.zeros_like(few), few], axis=1)
        left = jnp.concatenate([left, bottom], axis=0)
    result = product(left, jnp.concatenate([rh, rh, rl], axis=0))
    total[...] += result[:count]
    if few is not None:
        extra[...] += result[count:]


def plane_rows(rows, plane, first, size):
    chosen = jnp.zeros((rows.shape[0], size), F32)
    for p in range(rows.shape[1]):
        chosen = jnp.where(plane == p, rows[:, p, pl.ds(first, size)], chosen)
    return rows_split(chosen)


def gram_kernel(
    obs, ctrl, sense,
    gram, few, zlow, zhigh, ylow, yhigh,
    obs_here, ctrl_here, total, extra, obs_sems, ctrl_sems, z_sems, low_sems, high_sems,
):
    steps, rows, _ = obs.shape
    points = ylow.shape[1]

    def copies(i):
        return (
            pltpu.make_async_copy(obs.at[i], obs_here.at[i], obs_sems.at[i]),
            pltpu.make_async_copy(ctrl.at[i], ctrl_here.at[i], ctrl_sems.at[i]),
        )

    def z_copy(i):
        source = ctrl_here.at[i if i < 2 else steps - 4 + i]
        return pltpu.make_async_copy(source, (zlow if i < 2 else zhigh).at[i % 2], z_sems.at[i])

    def low_copy(p):
        source = ctrl_here.at[2 * p, pl.ds(0, points)]
        return pltpu.make_async_copy(source, ylow.at[p], low_sems.at[p])

    def high_copy(p):
        source = ctrl_here.at[2 * p + 1, pl.ds(rows - points, points)]
        return pltpu.make_async_copy(source, yhigh.at[p], high_sems.at[p])

    for i in range(AHEAD):
        for copy in copies(i):
            copy.start()
    total[...] = jnp.zeros_like(total)
    extra[...] = jnp.zeros_like(extra)

    @pl.loop(0, steps)
    def _(i):
        for copy in copies(i):
            copy.wait()

        @pl.when(i + AHEAD < steps)
        def _():
            for copy in copies(i + AHEAD):
                copy.start()

        for j in range(4):

            @pl.when(i == (j if j < 2 else steps - 4 + j))
            def _():
                z_copy(j).start()

        @pl.when(i % 2 == 0)
        def _():
            low_copy(i // 2).start()

        @pl.when(i % 2 == 1)
        def _():
            high_copy(i // 2).start()

        first = pl.multiple_of((i % 2) * rows, 128)
        some = plane_rows(sense, i // 2, first, rows)
        add_products(total, obs_here[i].T, ctrl_here[i], extra, some)

    width = total.shape[1] // 2
    for side in range(2):
        cols = total[:, side * width : (side + 1) * width]
        gram[:, side] = cols.reshape(gram.shape[0], gram.shape[2], width)
    few[...] = extra[:8]
    for i in range(4):
        z_copy(i).wait()
    for p in range(steps // 2):
        low_copy(p).wait()
        high_copy(p).wait()


def local_gram(observe, control, sense, points):
    steps, rows, rank = observe.shape
    anywhere = pl.BlockSpec(memory_space=pltpu.HBM)
    vmem = pl.BlockSpec(memory_space=pltpu.VMEM)
    face = jax.ShapeDtypeStruct((2, rows, rank), F32)
    edge = jax.ShapeDtypeStruct((steps // 2, points, rank), F32)
    return pl.pallas_call(
        gram_kernel,
        in_specs=[anywhere, anywhere, vmem],
        out_specs=[vmem, vmem] + [anywhere] * 4,
        out_shape=[
            jax.ShapeDtypeStruct((64, 2, 8, rank // 2), F32),
            jax.ShapeDtypeStruct((8, rank), F32),
            face,
            face,
            edge,
            edge,
        ],
        scratch_shapes=[
            pltpu.VMEM((steps, rows, rank), F32),
            pltpu.VMEM((steps, rows, rank), F32),
            pltpu.VMEM((rank, rank), F32),
            pltpu.VMEM((16, rank), F32),
            pltpu.SemaphoreType.DMA((steps,)),
            pltpu.SemaphoreType.DMA((steps,)),
            pltpu.SemaphoreType.DMA((4,)),
            pltpu.SemaphoreType.DMA((steps // 2,)),
            pltpu.SemaphoreType.DMA((steps // 2,)),
        ],
        compiler_params=pltpu.CompilerParams(vmem_limit_bytes=58 << 20),
        cost_estimate=pl.CostEstimate(
            flops=6 * steps * rows * rank * rank, bytes_accessed=24 << 20, transcendentals=0
        ),
        name="local_gram",
    )(observe, control, sense)


def inner_kernel(
    lines, points,
    obs, ctrl, conduct, drive, total, extra, field, obs_here, obs_sems, ctrl_sems,
):
    planes = ctrl.shape[0]
    inner = pl.ds(1, lines)
    rank = total.shape[0]

    def ctrl_copy(p):
        return pltpu.make_async_copy(ctrl.at[p], field.at[p + 1, inner], ctrl_sems.at[p])

    def obs_copy(p):
        return pltpu.make_async_copy(obs.at[p], obs_here.at[p], obs_sems.at[p])

    for p in range(2):
        ctrl_copy(p).start()
        obs_copy(p).start()
    total[...] = jnp.zeros_like(total)
    extra[...] = jnp.zeros_like(extra)
    empty = jnp.zeros((points, rank), F32)
    for p in range(planes):
        field[p + 1, 0] = empty
        field[p + 1, lines + 1] = empty
    for line in range(1, lines + 1):
        field[0, line] = empty
        field[planes + 1, line] = empty
    ctrl_copy(0).wait()

    @pl.loop(0, planes)
    def _(p):
        @pl.when(p + 1 < planes)
        def _():
            ctrl_copy(p + 1).wait()

        @pl.when(p + 2 < planes)
        def _():
            ctrl_copy(p + 2).start()
            obs_copy(p + 2).start()

        obs_copy(p).wait()
        half = lines // 2
        rows = half * points
        for line in (0, half):

            def part(plane, first):
                return field[plane, first : first + half]

            center = part(p + 1, line + 1)
            beside = part(p + 2, line + 1) + part(p, line + 1)
            beside = beside + part(p + 1, line + 2) + part(p + 1, line)
            center = center.reshape(rows, rank)
            beside = beside.reshape(rows, rank)
            place = lax.broadcasted_iota(jnp.int32, (rows, rank), 0) % points
            beside = beside + jnp.where(place > 0, pltpu.roll(center, 1, 0), 0.0)
            beside = beside + jnp.where(place < points - 1, pltpu.roll(center, rows - 1, 0), 0.0)
            first = line * points
            scale = conduct[p][:, first : first + rows] * (1.0 / 6.0)
            applied = (beside - 6.0 * center).T * scale
            some = plane_rows(drive, p, first, rows)
            add_products(total, applied, obs_here[p, first : first + rows], extra, some)


def inner_operator(observe, control, conduct, drive):
    planes, lines, points, rank = control.shape
    cells = lines * points
    anywhere = pl.BlockSpec(memory_space=pltpu.HBM)
    vmem = pl.BlockSpec(memory_space=pltpu.VMEM)
    return pl.pallas_call(
        functools.partial(inner_kernel, lines, points),
        in_specs=[anywhere, anywhere, vmem, vmem],
        out_specs=[vmem, vmem],
        out_shape=[
            jax.ShapeDtypeStruct((rank, rank), F32),
            jax.ShapeDtypeStruct((16, rank), F32),
        ],
        scratch_shapes=[
            pltpu.VMEM((planes + 2, lines + 2, points, rank), F32),
            pltpu.VMEM((planes, cells, rank), F32),
            pltpu.SemaphoreType.DMA((planes,)),
            pltpu.SemaphoreType.DMA((planes,)),
        ],
        compiler_params=pltpu.CompilerParams(vmem_limit_bytes=58 << 20),
        cost_estimate=pl.CostEstimate(
            flops=6 * planes * cells * rank * rank, bytes_accessed=18 << 20, transcendentals=0
        ),
        name="inner_operator",
    )(observe.reshape(planes, cells, rank), control, conduct.reshape(planes, 1, cells), drive)


def outer_kernel(
    obs, zlow, zhigh, ylow, yhigh, z_conduct, y_conduct, inner, extra, few_ctrl,
    out, z_field, z_obs, y_field, y_obs, total, sems,
):
    planes, lines, points, rank = obs.shape

    def copies(i):
        if i < 2:
            plane = (planes - 1) * i
            return (
                pltpu.make_async_copy((zhigh if i else zlow), z_field.at[i], sems.at[2 * i]),
                pltpu.make_async_copy(obs.at[plane], z_obs.at[i], sems.at[2 * i + 1]),
            )
        line = (lines - 1) * (i - 2)
        place = pl.ds(planes * (i - 2), planes)
        return (
            pltpu.make_async_copy((yhigh if i == 3 else ylow), y_field.at[place], sems.at[2 * i]),
            pltpu.make_async_copy(obs.at[:, line], y_obs.at[place], sems.at[2 * i + 1]),
        )

    for i in (2, 3, 0, 1):
        for copy in copies(i):
            copy.start()
    total[...] = inner[...]
    for i in (2, 3):
        for copy in copies(i):
            copy.wait()
    rows = 2 * planes * points
    applied = y_field[...].reshape(rows, rank).T * (y_conduct[...] * (1.0 / 6.0))
    add_products(total, applied, y_obs[...].reshape(rows, rank))
    for i in range(2):
        for copy in copies(i):
            copy.wait()
        rows = lines * points
        applied = z_field[i].reshape(rows, rank).T * (z_conduct[i] * (1.0 / 6.0))
        add_products(total, applied, z_obs[i].reshape(rows, rank))

    width = rank // 2
    for side in range(2):
        cols = total[:, side * width : (side + 1) * width]
        out[:, side, :, :width] = cols.reshape(out.shape[0], out.shape[2], width)
    summed = jnp.concatenate([extra[0:4] + extra[4:8], few_ctrl[0:4] + few_ctrl[4:8]], axis=0)
    wide = jnp.concatenate([summed, jnp.zeros((120, rank), F32)], axis=0).T
    out[:, 0, :, width:] = wide.reshape(out.shape[0], out.shape[2], 128)
    out[:, 1, :, width:] = jnp.zeros((out.shape[0], out.shape[2], 128), F32)


def with_outer(observe, faces, conduct, inner, extra, few_ctrl):
    planes, lines, points, rank = observe.shape
    zlow, zhigh, ylow, yhigh = faces
    cells = lines * points
    z_conduct = jnp.stack([conduct[0], conduct[-1]]).reshape(2, 1, cells)
    y_conduct = jnp.stack([conduct[:, :points], conduct[:, cells - points :]])
    anywhere = pl.BlockSpec(memory_space=pltpu.HBM)
    vmem = pl.BlockSpec(memory_space=pltpu.VMEM)
    return pl.pallas_call(
        outer_kernel,
        in_specs=[anywhere] * 5 + [vmem] * 5,
        out_specs=vmem,
        out_shape=jax.ShapeDtypeStruct((64, 2, 8, rank // 2 + 128), F32),
        scratch_shapes=[
            pltpu.VMEM((2, lines, points, rank), F32),
            pltpu.VMEM((2, lines, points, rank), F32),
            pltpu.VMEM((2 * planes, points, rank), F32),
            pltpu.VMEM((2 * planes, points, rank), F32),
            pltpu.VMEM((rank, rank), F32),
            pltpu.SemaphoreType.DMA((8,)),
        ],
        compiler_params=pltpu.CompilerParams(vmem_limit_bytes=58 << 20),
        cost_estimate=pl.CostEstimate(
            flops=15 * cells * rank * rank, bytes_accessed=14 << 20, transcendentals=0
        ),
        name="outer_operator",
    )(
        observe,
        zlow.reshape(lines, points, rank),
        zhigh.reshape(lines, points, rank),
        ylow,
        yhigh,
        z_conduct,
        y_conduct.reshape(1, 2 * planes * points),
        inner,
        extra,
        few_ctrl,
    )


def sum_kernel(parts, out):
    whole = jnp.sum(parts[...], axis=0, keepdims=True)
    out[...] = jnp.broadcast_to(whole, out.shape)


def scattered(parts):
    tiles = parts.reshape(parts.shape[0] * parts.shape[1], *parts.shape[2:])
    return lax.all_to_all(tiles, ALL, 0, 0, tiled=True)


def summed_copies(arrived):
    return pl.pallas_call(
        sum_kernel,
        out_shape=jax.ShapeDtypeStruct(arrived.shape, F32),
        compiler_params=pltpu.CompilerParams(vmem_limit_bytes=6 << 20),
        cost_estimate=pl.CostEstimate(
            flops=arrived.size, bytes_accessed=8 * arrived.size, transcendentals=0
        ),
        name="sum_gram",
    )(arrived)


def project_kernel(side, parts, left, out):
    block = jnp.sum(parts[...], axis=0)
    half = left.shape[1] // 2
    mine = jnp.where(side[0] == 0, left[:, :half], left[:, half:])
    turned = product3(block[:, :half], mine, ((1,), (1,)))
    whole = jnp.concatenate([turned, block[:, half:]], axis=1)
    out[...] = jnp.broadcast_to(whole[None], out.shape)


def projected_copies(arrived, left):
    side = lax.axis_index("sub") & 1
    vmem = pl.BlockSpec(memory_space=pltpu.VMEM)
    return pl.pallas_call(
        project_kernel,
        in_specs=[pl.BlockSpec(memory_space=pltpu.SMEM), vmem, vmem],
        out_specs=vmem,
        out_shape=jax.ShapeDtypeStruct((arrived.shape[0], 8, 256), F32),
        compiler_params=pltpu.CompilerParams(vmem_limit_bytes=8 << 20),
        cost_estimate=pl.CostEstimate(
            flops=arrived.size, bytes_accessed=8 * arrived.size, transcendentals=0
        ),
        name="project",
    )(side.reshape(1).astype(jnp.int32), arrived, left)


def gathered(copies):
    tiles = lax.all_to_all(copies, ALL, 0, 0, tiled=True)
    return tiles.reshape(64, 2, *tiles.shape[1:])


def inverse_factor(work):
    size = work.shape[0]
    for first in range(0, size, PANEL):
        last = first + PANEL
        panel = [work[first + 8 * g : first + 8 * g + 8, :] for g in range(PANEL // 8)]
        groups = PANEL // 8
        columns = {}
        for k in range(PANEL):
            for g in range(k // 8, groups):
                columns[k, g] = jnp.broadcast_to(
                    panel[g][:, first + k : first + k + 1], (8, 128)
                )
        place = lax.broadcasted_iota(jnp.int32, (8, 128), 0)
        for j in range(PANEL):
            gj, sj = divmod(j, 8)
            pivot = jnp.broadcast_to(columns[j, gj][sj : sj + 1], (8, 128))
            scale = lax.rsqrt(pivot)
            lower = {}
            for g in range(gj, groups):
                lower[g] = columns[j, g] * scale
            row = jnp.broadcast_to(panel[gj][sj : sj + 1], (8, 256))
            row = row * jnp.concatenate([scale, scale], axis=1)
            for k in range(j + 1, PANEL):
                gk, sk = divmod(k, 8)
                across = jnp.broadcast_to(lower[gk][sk : sk + 1], (8, 128))
                for g in range(gk, groups):
                    columns[k, g] = columns[k, g] - lower[g] * across
            for g in range(gj, groups):
                weight = lower[g]
                if g == gj:
                    weight = jnp.where(place > sj, weight, 0.0)
                wide = jnp.concatenate([weight, weight], axis=1)
                panel[g] = panel[g] - wide * row
            wide_place = lax.broadcasted_iota(jnp.int32, (8, 256), 0)
            panel[gj] = jnp.where(wide_place == sj, row, panel[gj])
        for g in range(groups):
            work[first + 8 * g : first + 8 * g + 8, :] = panel[g]
        if last < size:
            done = jnp.concatenate(panel, axis=0)
            u0, u1, u2 = split3(done)
            left = jnp.concatenate([u0, u0, u1, u1, u0, u2], axis=0)[:, :size]
            right = jnp.concatenate([u0, u1, u0, u1, u2, u0], axis=0)
            change = product(left, right, ((0,), (0,)))
            work[last:, :] -= change[last:, :]


def bases_kernel(gram, start, right_out, left_out, image_out, cross, basis, work):
    rank = cross.shape[0]
    half = rank // 2
    for side in range(2):
        cross[:, side * half : (side + 1) * half] = gram[:, side].reshape(rank, half)
    basis[...] = start[...].T
    size = basis.shape[0]
    eye = (
        lax.broadcasted_iota(jnp.int32, (size, size), 0)
        == lax.broadcasted_iota(jnp.int32, (size, size), 1)
    ).astype(F32)

    @pl.loop(0, 4)
    def _(turn):
        @pl.when(turn % 2 == 0)
        def _():
            image_out[...] = product3(basis[...], cross[...])

        @pl.when(turn % 2 == 1)
        def _():
            image_out[...] = product3(basis[...], cross[...], ((1,), (1,)))

        held = image_out[...]
        work[:, :size] = product6(held, held, ((1,), (1,)))
        work[:, size:] = eye
        inverse_factor(work)
        basis[...] = product6(work[:, size:], held)

        @pl.when(turn == 2)
        def _():
            right_out[...] = basis[...]

    left_out[...] = basis[...]


def bases(gram, start):
    rank, size = start.shape
    shape = jax.ShapeDtypeStruct((size, rank), F32)
    return pl.pallas_call(
        bases_kernel,
        out_shape=[shape, shape, shape],
        scratch_shapes=[
            pltpu.VMEM((rank, rank), F32),
            pltpu.VMEM((size, rank), F32),
            pltpu.VMEM((size, 2 * size), F32),
        ],
        compiler_params=pltpu.CompilerParams(vmem_limit_bytes=16 << 20),
        cost_estimate=pl.CostEstimate(
            flops=20_000_000_000, bytes_accessed=4 << 20, transcendentals=0
        ),
        name="bases",
    )(gram, start)


def finish_kernel(order, right, left, image, blocks, mass, state, inputs, outputs):
    size, rank = right.shape
    turned = (blocks[:, 0, :, :size] + blocks[:, 1, :, :size]).reshape(rank, size)
    few = blocks[:, 0, :, size:].reshape(rank, 128)
    kept_col = lax.broadcasted_iota(jnp.int32, (size, size), 0) < order[0]
    kept_row = lax.broadcasted_iota(jnp.int32, (size, size), 1) < order[0]
    kept = jnp.logical_and(kept_col, kept_row).astype(F32)
    mass[...] = kept * product6(left[...], image[...], ((1,), (1,)))
    state[...] = kept * product3(right[...], turned).T
    inputs[...] = (kept_row.astype(F32) * product3(left[...], few).T)[:4]
    outputs[...] = (kept_row.astype(F32) * product3(right[...], few).T)[4:8]


def finish(order, right, left, image, blocks):
    size, _ = right.shape
    vmem = pl.BlockSpec(memory_space=pltpu.VMEM)
    return pl.pallas_call(
        finish_kernel,
        in_specs=[pl.BlockSpec(memory_space=pltpu.SMEM)] + [vmem] * 4,
        out_specs=[vmem] * 4,
        out_shape=[
            jax.ShapeDtypeStruct((size, size), F32),
            jax.ShapeDtypeStruct((size, size), F32),
            jax.ShapeDtypeStruct((4, size), F32),
            jax.ShapeDtypeStruct((4, size), F32),
        ],
        compiler_params=pltpu.CompilerParams(vmem_limit_bytes=16 << 20),
        cost_estimate=pl.CostEstimate(
            flops=1_000_000_000, bytes_accessed=4 << 20, transcendentals=0
        ),
        name="finish",
    )(order, right, left, image, blocks)


def from_neighbours(low_face, high_face, axis):
    count = lax.axis_size(axis)
    up = [(i, i + 1) for i in range(count - 1)]
    down = [(b, a) for a, b in up]
    return lax.ppermute(high_face, axis, up), lax.ppermute(low_face, axis, down)


def reduced(factor_obs, factor_ctrl, diffusivity, input_map, output_map, start_block, order):
    planes, lines, points, rank = factor_ctrl.shape
    halves = (2 * planes, lines * points // 2, rank)
    gram, few_ctrl, zlow, zhigh, ylow, yhigh = local_gram(
        factor_obs.reshape(halves), factor_ctrl.reshape(halves), output_map, points
    )
    arrived = scattered(gram)
    zlow, zhigh = from_neighbours(zlow, zhigh, "slab")
    ylow, yhigh = from_neighbours(ylow, yhigh, "sub")
    inner, extra = inner_operator(factor_obs, factor_ctrl, diffusivity, input_map)
    gram = gathered(summed_copies(arrived))
    oper = with_outer(factor_obs, (zlow, zhigh, ylow, yhigh), diffusivity, inner, extra, few_ctrl)
    oper = scattered(oper)
    right, left, image = bases(gram, start_block)
    blocks = gathered(projected_copies(oper, left))
    mass, state, inputs, outputs = finish(order, right, left, image, blocks)
    return mass, state, inputs.T, outputs


def solution(mesh):
    placed = (
        P("slab", "sub", None, None),
        P("slab", "sub", None, None),
        P("slab", "sub"),
        P(None, "slab", "sub"),
        P(None, "slab", "sub"),
        P(),
        P(),
    )
    return jax.shard_map(
        reduced, mesh=mesh, in_specs=placed, out_specs=(P(), P(), P(), P()), check_vma=False
    )
```

```python
import functools

import jax
import jax.numpy as jnp
from jax import lax
from jax.experimental import pallas as pl
from jax.experimental.pallas import tpu as pltpu
from jax.sharding import PartitionSpec as P


ALL = ("slab", "sub")
F32 = jnp.float32
BF16 = jnp.bfloat16
PANEL = 32
AHEAD = 2


def split2(x):
    high = x.astype(BF16)
    return high, (x - high.astype(F32)).astype(BF16)


def split3(x):
    high = x.astype(BF16)
    rest = x - high.astype(F32)
    mid = rest.astype(BF16)
    return high, mid, (rest - mid.astype(F32)).astype(BF16)


def product(a, b, contract=((1,), (0,))):
    return lax.dot_general(a, b, (contract, ((), ())), preferred_element_type=F32)


def product3(a, b, contract=((1,), (0,))):
    ah, al = split2(a)
    bh, bl = split2(b)
    return product(ah, bh, contract) + (product(ah, bl, contract) + product(al, bh, contract))


def product6(a, b, contract=((1,), (0,))):
    a0, a1, a2 = split3(a)
    b0, b1, b2 = split3(b)
    dot = functools.partial(product, contract=contract)
    small = dot(a1, b1) + (dot(a0, b2) + dot(a2, b0))
    return dot(a0, b0) + ((dot(a0, b1) + dot(a1, b0)) + small)


def rows_split(rows):
    both = jnp.concatenate([rows, rows], axis=0)
    high = both.astype(BF16).astype(F32)
    place = lax.broadcasted_iota(jnp.int32, both.shape, 0)
    halves = jnp.where(place < rows.shape[0], high, both - high)
    return jnp.concatenate([halves, jnp.zeros_like(halves)], axis=0).astype(BF16)


def add_products(total, turned, right, extra=None, few=None):
    count = turned.shape[0]
    th, tl = split2(turned)
    rh, rl = split2(right)
    left = jnp.concatenate([th, tl, th], axis=1)
    if few is not None:
        bottom = jnp.concatenate([few, jnp.zeros_like(few), few], axis=1)
        left = jnp.concatenate([left, bottom], axis=0)
    result = product(left, jnp.concatenate([rh, rh, rl], axis=0))
    total[...] += result[:count]
    if few is not None:
        extra[...] += result[count:]


def plane_rows(rows, plane, first, size):
    chosen = jnp.zeros((rows.shape[0], size), F32)
    for p in range(rows.shape[1]):
        chosen = jnp.where(plane == p, rows[:, p, pl.ds(first, size)], chosen)
    return rows_split(chosen)


def in_hbm(value):
    return pltpu.with_memory_space_constraint(value, pltpu.HBM)


def gram_kernel(
    obs, ctrl, sense,
    gram, few_far, zlow, zhigh, ylow, yhigh,
    obs_here, ctrl_here, total, extra, sense_here, obs_sems, ctrl_sems, z_sems, low_sems, high_sems, other_sems,
):
    steps, rows, _ = obs.shape
    points = ylow.shape[1]

    def copies(i):
        return (
            pltpu.make_async_copy(obs.at[i], obs_here.at[i], obs_sems.at[i]),
            pltpu.make_async_copy(ctrl.at[i], ctrl_here.at[i], ctrl_sems.at[i]),
        )

    def z_copy(i):
        source = ctrl_here.at[i if i < 2 else steps - 4 + i]
        return pltpu.make_async_copy(source, (zlow if i < 2 else zhigh).at[i % 2], z_sems.at[i])

    def low_copy(p):
        source = ctrl_here.at[2 * p, pl.ds(0, points)]
        return pltpu.make_async_copy(source, ylow.at[p], low_sems.at[p])

    def high_copy(p):
        source = ctrl_here.at[2 * p + 1, pl.ds(rows - points, points)]
        return pltpu.make_async_copy(source, yhigh.at[p], high_sems.at[p])

    sense_copy = pltpu.make_async_copy(sense, sense_here, other_sems.at[0])
    for i in range(AHEAD):
        for copy in copies(i):
            copy.start()
        if i == 0:
            sense_copy.start()
    total[...] = jnp.zeros_like(total)
    extra[...] = jnp.zeros_like(extra)
    sense_copy.wait()

    @pl.loop(0, steps)
    def _(i):
        for copy in copies(i):
            copy.wait()

        @pl.when(i + AHEAD < steps)
        def _():
            for copy in copies(i + AHEAD):
                copy.start()

        for j in range(4):

            @pl.when(i == (j if j < 2 else steps - 4 + j))
            def _():
                z_copy(j).start()

        @pl.when(i % 2 == 0)
        def _():
            low_copy(i // 2).start()

        @pl.when(i % 2 == 1)
        def _():
            high_copy(i // 2).start()

        first = pl.multiple_of((i % 2) * rows, 128)
        some = plane_rows(sense_here, i // 2, first, rows)
        add_products(total, obs_here[i].T, ctrl_here[i], extra, some)

    few_copy = pltpu.make_async_copy(extra, few_far, other_sems.at[0])
    few_copy.start()
    width = total.shape[1] // 2
    for side in range(2):
        cols = total[:, side * width : (side + 1) * width]
        gram[:, side] = cols.reshape(gram.shape[0], gram.shape[2], width)
    few_copy.wait()
    for i in range(4):
        z_copy(i).wait()
    for p in range(steps // 2):
        low_copy(p).wait()
        high_copy(p).wait()


def local_gram(observe, control, sense, points):
    steps, rows, rank = observe.shape
    anywhere = pl.BlockSpec(memory_space=pltpu.HBM)
    vmem = pl.BlockSpec(memory_space=pltpu.VMEM)
    face = pltpu.HBM((2, rows, rank), F32)
    edge = pltpu.HBM((steps // 2, points, rank), F32)
    return pl.pallas_call(
        gram_kernel,
        in_specs=[anywhere] * 3,
        out_specs=[vmem] + [anywhere] * 5,
        out_shape=[
            jax.ShapeDtypeStruct((64, 2, 8, rank // 2), F32),
            pltpu.HBM((16, rank), F32),
            face,
            face,
            edge,
            edge,
        ],
        scratch_shapes=[
            pltpu.VMEM((steps, rows, rank), F32),
            pltpu.VMEM((steps, rows, rank), F32),
            pltpu.VMEM((rank, rank), F32),
            pltpu.VMEM((16, rank), F32),
            pltpu.VMEM(sense.shape, F32),
            pltpu.SemaphoreType.DMA((steps,)),
            pltpu.SemaphoreType.DMA((steps,)),
            pltpu.SemaphoreType.DMA((4,)),
            pltpu.SemaphoreType.DMA((steps // 2,)),
            pltpu.SemaphoreType.DMA((steps // 2,)),
            pltpu.SemaphoreType.DMA((1,)),
        ],
        compiler_params=pltpu.CompilerParams(vmem_limit_bytes=36 << 20),
        cost_estimate=pl.CostEstimate(
            flops=6 * steps * rows * rank * rank, bytes_accessed=24 << 20, transcendentals=0
        ),
        name="local_gram",
    )(in_hbm(observe), in_hbm(control), in_hbm(sense))


def inner_kernel(
    points, obs_far, ctrl_far, conduct, drive,
    total_far, extra_far, total, extra, obs, ctrl, conduct_here, drive_here, sems, obs_sems, ctrl_sems,
):
    steps, rows, rank = ctrl.shape
    planes = steps // 2
    small = [
        pltpu.make_async_copy(conduct, conduct_here, sems.at[0]),
        pltpu.make_async_copy(drive, drive_here, sems.at[1]),
    ]

    def ctrl_copy(i):
        return pltpu.make_async_copy(ctrl_far.at[i], ctrl.at[i], ctrl_sems.at[i])

    def obs_copy(i):
        return pltpu.make_async_copy(obs_far.at[i], obs.at[i], obs_sems.at[i])

    for i in (0, 1, 2):
        ctrl_copy(i).start()
    obs_copy(0).start()
    for copy in small:
        copy.start()
    ctrl_copy(3).start()
    obs_copy(1).start()
    total[...] = jnp.zeros_like(total)
    extra[...] = jnp.zeros_like(extra)
    for copy in small:
        copy.wait()
    ctrl_copy(0).wait()
    ctrl_copy(1).wait()
    empty = jnp.zeros((points, rank), F32)

    @pl.loop(0, planes)
    def _(p):
        up = jnp.minimum(p + 1, planes - 1)
        down = jnp.maximum(p - 1, 0)
        has_up = (p + 1 < planes).astype(F32)
        has_down = (p > 0).astype(F32)
        for half in range(2):

            @pl.when(p + 1 < planes)
            def _():
                ctrl_copy(2 * p + 2 + half).wait()

            @pl.when(p + 2 < planes)
            def _():
                ctrl_copy(2 * p + 4 + half).start()

            @pl.when(p + 1 < planes)
            def _():
                obs_copy(2 * p + 2 + half).start()

            obs_copy(2 * p + half).wait()
            center = ctrl[2 * p + half]
            beside = has_up * ctrl[2 * up + half] + has_down * ctrl[2 * down + half]
            if half == 0:
                before = empty
                after = ctrl[2 * p + 1, :points]
            else:
                before = ctrl[2 * p, rows - points :]
                after = empty
            beside = beside + jnp.concatenate([before, center[: rows - points]], axis=0)
            beside = beside + jnp.concatenate([center[points:], after], axis=0)
            place = lax.broadcasted_iota(jnp.int32, (rows, rank), 0) % points
            beside = beside + jnp.where(place > 0, pltpu.roll(center, 1, 0), 0.0)
            beside = beside + jnp.where(place < points - 1, pltpu.roll(center, rows - 1, 0), 0.0)
            first = half * rows
            scale = conduct_here[pl.ds(p, 1), first : first + rows] * (1.0 / 6.0)
            applied = (beside - 6.0 * center).T * scale
            some = plane_rows(drive_here, p, first, rows)
            add_products(total, applied, obs[2 * p + half], extra, some)

    results = [
        pltpu.make_async_copy(total, total_far, sems.at[0]),
        pltpu.make_async_copy(extra, extra_far, sems.at[1]),
    ]
    for copy in results:
        copy.start()
    for copy in results:
        copy.wait()


def inner_operator(observe, control, conduct, drive, points):
    steps, rows, rank = control.shape
    anywhere = pl.BlockSpec(memory_space=pltpu.HBM)
    return pl.pallas_call(
        functools.partial(inner_kernel, points),
        in_specs=[anywhere] * 4,
        out_specs=[anywhere] * 2,
        out_shape=[
            pltpu.HBM((rank, rank), F32),
            pltpu.HBM((16, rank), F32),
        ],
        scratch_shapes=[
            pltpu.VMEM((rank, rank), F32),
            pltpu.VMEM((16, rank), F32),
            pltpu.VMEM((steps, rows, rank), F32),
            pltpu.VMEM((steps, rows, rank), F32),
            pltpu.VMEM(conduct.shape, F32),
            pltpu.VMEM(drive.shape, F32),
            pltpu.SemaphoreType.DMA((2,)),
            pltpu.SemaphoreType.DMA((steps,)),
            pltpu.SemaphoreType.DMA((steps,)),
        ],
        compiler_params=pltpu.CompilerParams(vmem_limit_bytes=36 << 20),
        cost_estimate=pl.CostEstimate(
            flops=6 * steps * rows * rank * rank, bytes_accessed=18 << 20, transcendentals=0
        ),
        name="inner_operator",
    )(in_hbm(observe), in_hbm(control), in_hbm(conduct), in_hbm(drive))


def outer_kernel(
    points, obs, zlow, zhigh, ylow, yhigh, conduct, inner, extra_far, few_far,
    out, z_field, y_field, z_obs, y_obs, conduct_here, total, extra, few_ctrl, sems, obs_sems,
):
    steps, rows, rank = obs.shape
    planes = steps // 2
    conduct_copy = pltpu.make_async_copy(conduct, conduct_here, sems.at[0])
    inner_copy = pltpu.make_async_copy(inner, total, sems.at[7])
    few_copies = [
        pltpu.make_async_copy(extra_far, extra, sems.at[8]),
        pltpu.make_async_copy(few_far, few_ctrl, sems.at[9]),
    ]
    y_near = [
        pltpu.make_async_copy(
            obs.at[2 * p + i, pl.ds(i * (rows - points), points)],
            y_obs.at[i, pl.ds(p * points, points)],
            obs_sems.at[4 + planes * i + p],
        )
        for i in range(2)
        for p in range(planes)
    ]
    z_near = [
        pltpu.make_async_copy(
            obs.at[i if i < 2 else steps - 4 + i], z_obs.at[i], obs_sems.at[i]
        )
        for i in range(4)
    ]
    y_copies = [
        pltpu.make_async_copy(ylow, y_field.at[0], sems.at[1]),
        pltpu.make_async_copy(yhigh, y_field.at[1], sems.at[2]),
    ]
    z_copies = [
        pltpu.make_async_copy(face.at[half], z_field.at[2 * i + half], sems.at[3 + 2 * i + half])
        for i, face in enumerate((zlow, zhigh))
        for half in range(2)
    ]
    conduct_copy.start()
    for copy in y_copies + y_near + [inner_copy]:
        copy.start()
    for far, near in zip(z_copies, z_near):
        far.start()
        near.start()
    for copy in few_copies:
        copy.start()
    conduct_copy.wait()
    scale = conduct_here[...] * (1.0 / 6.0)
    for copy in y_copies + y_near + [inner_copy]:
        copy.wait()
    for i in range(2):
        cells = i * (2 * rows - points)
        near = y_obs[i]
        turned = [
            y_field[i, p].T * scale[p : p + 1, cells : cells + points] for p in range(planes)
        ]
        add_products(total, jnp.concatenate(turned, axis=1), near)
    for i in range(2):
        plane = (planes - 1) * i
        for half in range(2):
            z_copies[2 * i + half].wait()
            z_near[2 * i + half].wait()
            turned = z_field[2 * i + half].T
            turned = turned * scale[plane : plane + 1, half * rows : (half + 1) * rows]
            add_products(total, turned, z_obs[2 * i + half])

    for copy in few_copies:
        copy.wait()
    width = rank // 2
    for side in range(2):
        cols = total[:, side * width : (side + 1) * width]
        out[:, side, :, :width] = cols.reshape(out.shape[0], out.shape[2], width)
    summed = jnp.concatenate([extra[0:4] + extra[4:8], few_ctrl[0:4] + few_ctrl[4:8]], axis=0)
    wide = jnp.concatenate([summed, jnp.zeros((120, rank), F32)], axis=0).T
    out[:, 0, :, width:] = wide.reshape(out.shape[0], out.shape[2], 128)
    out[:, 1, :, width:] = jnp.zeros((out.shape[0], out.shape[2], 128), F32)


def with_outer(observe, faces, conduct, inner, extra, few_ctrl, points):
    steps, rows, rank = observe.shape
    anywhere = pl.BlockSpec(memory_space=pltpu.HBM)
    vmem = pl.BlockSpec(memory_space=pltpu.VMEM)
    return pl.pallas_call(
        functools.partial(outer_kernel, points),
        in_specs=[anywhere] * 9,
        out_specs=vmem,
        out_shape=jax.ShapeDtypeStruct((64, 2, 8, rank // 2 + 128), F32),
        scratch_shapes=[
            pltpu.VMEM((4, rows, rank), F32),
            pltpu.VMEM((2, steps // 2, points, rank), F32),
            pltpu.VMEM((4, rows, rank), F32),
            pltpu.VMEM((2, steps // 2 * points, rank), F32),
            pltpu.VMEM(conduct.shape, F32),
            pltpu.VMEM((rank, rank), F32),
            pltpu.VMEM(extra.shape, F32),
            pltpu.VMEM(few_ctrl.shape, F32),
            pltpu.SemaphoreType.DMA((10,)),
            pltpu.SemaphoreType.DMA((4 + steps,)),
        ],
        compiler_params=pltpu.CompilerParams(vmem_limit_bytes=36 << 20),
        cost_estimate=pl.CostEstimate(
            flops=30 * rows * rank * rank, bytes_accessed=7 << 20, transcendentals=0
        ),
        name="outer_operator",
    )(*map(in_hbm, (observe, *faces, conduct, inner, extra, few_ctrl)))


def sum_kernel(parts, out):
    whole = jnp.sum(parts[...], axis=0, keepdims=True)
    out[...] = jnp.broadcast_to(whole, out.shape)


def scattered(parts):
    tiles = parts.reshape(parts.shape[0] * parts.shape[1], *parts.shape[2:])
    return lax.all_to_all(tiles, ALL, 0, 0, tiled=True)


def summed_copies(arrived):
    return pl.pallas_call(
        sum_kernel,
        out_shape=jax.ShapeDtypeStruct(arrived.shape, F32),
        compiler_params=pltpu.CompilerParams(vmem_limit_bytes=6 << 20),
        cost_estimate=pl.CostEstimate(
            flops=arrived.size, bytes_accessed=8 * arrived.size, transcendentals=0
        ),
        name="sum_gram",
    )(arrived)


def project_kernel(side, parts, left, out):
    block = jnp.sum(parts[...], axis=0)
    half = left.shape[1] // 2
    mine = jnp.where(side[0] == 0, left[:, :half], left[:, half:])
    turned = product3(block[:, :half], mine, ((1,), (1,)))
    whole = jnp.concatenate([turned, block[:, half:]], axis=1)
    out[...] = jnp.broadcast_to(whole[None], out.shape)


def projected_copies(arrived, left):
    side = lax.axis_index("sub") & 1
    vmem = pl.BlockSpec(memory_space=pltpu.VMEM)
    return pl.pallas_call(
        project_kernel,
        in_specs=[pl.BlockSpec(memory_space=pltpu.SMEM), vmem, vmem],
        out_specs=vmem,
        out_shape=jax.ShapeDtypeStruct((arrived.shape[0], 8, 256), F32),
        compiler_params=pltpu.CompilerParams(vmem_limit_bytes=8 << 20),
        cost_estimate=pl.CostEstimate(
            flops=arrived.size, bytes_accessed=8 * arrived.size, transcendentals=0
        ),
        name="project",
    )(side.reshape(1).astype(jnp.int32), arrived, left)


def gathered(copies):
    tiles = lax.all_to_all(copies, ALL, 0, 0, tiled=True)
    return tiles.reshape(64, 2, *tiles.shape[1:])


def inverse_factor(work):
    size = work.shape[0]
    for first in range(0, size, PANEL):
        last = first + PANEL
        panel = [work[first + 8 * g : first + 8 * g + 8, :] for g in range(PANEL // 8)]
        groups = PANEL // 8
        columns = {}
        for k in range(PANEL):
            for g in range(k // 8, groups):
                columns[k, g] = jnp.broadcast_to(
                    panel[g][:, first + k : first + k + 1], (8, 128)
                )
        place = lax.broadcasted_iota(jnp.int32, (8, 128), 0)
        for j in range(PANEL):
            gj, sj = divmod(j, 8)
            pivot = jnp.broadcast_to(columns[j, gj][sj : sj + 1], (8, 128))
            scale = lax.rsqrt(pivot)
            lower = {}
            for g in range(gj, groups):
                lower[g] = columns[j, g] * scale
            row = jnp.broadcast_to(panel[gj][sj : sj + 1], (8, 256))
            row = row * jnp.concatenate([scale, scale], axis=1)
            for k in range(j + 1, PANEL):
                gk, sk = divmod(k, 8)
                across = jnp.broadcast_to(lower[gk][sk : sk + 1], (8, 128))
                for g in range(gk, groups):
                    columns[k, g] = columns[k, g] - lower[g] * across
            for g in range(gj, groups):
                weight = lower[g]
                if g == gj:
                    weight = jnp.where(place > sj, weight, 0.0)
                wide = jnp.concatenate([weight, weight], axis=1)
                panel[g] = panel[g] - wide * row
            wide_place = lax.broadcasted_iota(jnp.int32, (8, 256), 0)
            panel[gj] = jnp.where(wide_place == sj, row, panel[gj])
        for g in range(groups):
            work[first + 8 * g : first + 8 * g + 8, :] = panel[g]
        if last < size:
            done = jnp.concatenate(panel, axis=0)
            u0, u1, u2 = split3(done)
            left = jnp.concatenate([u0, u0, u1, u1, u0, u2], axis=0)[:, :size]
            right = jnp.concatenate([u0, u1, u0, u1, u2, u0], axis=0)
            change = product(left, right, ((0,), (0,)))
            work[last:, :] -= change[last:, :]


def bases_kernel(gram, start, right_out, left_out, image_out, high, low, basis, work):
    rank = high.shape[0]
    half = rank // 2
    for side in range(2):
        cols = gram[:, side].reshape(rank, half)
        place = slice(side * half, (side + 1) * half)
        high[:, place], low[:, place] = split2(cols)
    basis[...] = start[...].T
    size = basis.shape[0]
    eye = (
        lax.broadcasted_iota(jnp.int32, (size, size), 0)
        == lax.broadcasted_iota(jnp.int32, (size, size), 1)
    ).astype(F32)

    @pl.loop(0, 4)
    def _(turn):
        for parity, contract in enumerate((((1,), (0,)), ((1,), (1,)))):

            @pl.when(turn % 2 == parity)
            def _():
                bh, bl = split2(basis[...])
                small = product(bh, low[...], contract) + product(bl, high[...], contract)
                image_out[...] = product(bh, high[...], contract) + small

        held = image_out[...]
        work[:, :size] = product6(held, held, ((1,), (1,)))
        work[:, size:] = eye
        inverse_factor(work)
        basis[...] = product6(work[:, size:], held)

        @pl.when(turn == 2)
        def _():
            right_out[...] = basis[...]

    left_out[...] = basis[...]


def bases(gram, start):
    rank, size = start.shape
    shape = jax.ShapeDtypeStruct((size, rank), F32)
    return pl.pallas_call(
        bases_kernel,
        out_shape=[shape, shape, shape],
        scratch_shapes=[
            pltpu.VMEM((rank, rank), BF16),
            pltpu.VMEM((rank, rank), BF16),
            pltpu.VMEM((size, rank), F32),
            pltpu.VMEM((size, 2 * size), F32),
        ],
        compiler_params=pltpu.CompilerParams(vmem_limit_bytes=16 << 20),
        cost_estimate=pl.CostEstimate(
            flops=20_000_000_000, bytes_accessed=4 << 20, transcendentals=0
        ),
        name="bases",
    )(gram, start)


def finish_kernel(order, right, left, image, blocks, mass, state, inputs, outputs):
    size, rank = right.shape
    turned = (blocks[:, 0, :, :size] + blocks[:, 1, :, :size]).reshape(rank, size)
    few = blocks[:, 0, :, size:].reshape(rank, 128)
    kept_col = lax.broadcasted_iota(jnp.int32, (size, size), 0) < order[0]
    kept_row = lax.broadcasted_iota(jnp.int32, (size, size), 1) < order[0]
    kept = jnp.logical_and(kept_col, kept_row).astype(F32)
    mass[...] = kept * product6(left[...], image[...], ((1,), (1,)))
    state[...] = kept * product3(right[...], turned).T
    inputs[...] = (kept_row.astype(F32) * product3(left[...], few).T)[:4]
    outputs[...] = (kept_row.astype(F32) * product3(right[...], few).T)[4:8]


def finish(order, right, left, image, blocks):
    size, _ = right.shape
    vmem = pl.BlockSpec(memory_space=pltpu.VMEM)
    return pl.pallas_call(
        finish_kernel,
        in_specs=[pl.BlockSpec(memory_space=pltpu.SMEM)] + [vmem] * 4,
        out_specs=[vmem] * 4,
        out_shape=[
            jax.ShapeDtypeStruct((size, size), F32),
            jax.ShapeDtypeStruct((size, size), F32),
            jax.ShapeDtypeStruct((4, size), F32),
            jax.ShapeDtypeStruct((4, size), F32),
        ],
        compiler_params=pltpu.CompilerParams(vmem_limit_bytes=16 << 20),
        cost_estimate=pl.CostEstimate(
            flops=1_000_000_000, bytes_accessed=4 << 20, transcendentals=0
        ),
        name="finish",
    )(order, right, left, image, blocks)


def from_neighbours(low_face, high_face, axis):
    count = lax.axis_size(axis)
    up = [(i, i + 1) for i in range(count - 1)]
    down = [(b, a) for a, b in up]
    return lax.ppermute(high_face, axis, up), lax.ppermute(low_face, axis, down)


def reduced(factor_obs, factor_ctrl, diffusivity, input_map, output_map, start_block, order):
    planes, lines, points, rank = factor_ctrl.shape
    halves = (2 * planes, lines * points // 2, rank)
    observe = factor_obs.reshape(halves)
    control = factor_ctrl.reshape(halves)
    gram, few_ctrl, zlow, zhigh, ylow, yhigh = local_gram(
        observe, control, output_map, points
    )
    arrived = scattered(gram)
    zlow, zhigh = from_neighbours(zlow, zhigh, "slab")
    ylow, yhigh = from_neighbours(ylow, yhigh, "sub")
    inner, extra = inner_operator(observe, control, diffusivity, input_map, points)
    gram = gathered(summed_copies(arrived))
    faces = (zlow, zhigh, ylow, yhigh)
    oper = with_outer(observe, faces, diffusivity, inner, extra, few_ctrl, points)
    oper = scattered(oper)
    right, left, image = bases(gram, start_block)
    blocks = gathered(projected_copies(oper, left))
    mass, state, inputs, outputs = finish(order, right, left, image, blocks)
    return mass, state, inputs.T, outputs


def solution(mesh):
    placed = (
        P("slab", "sub", None, None),
        P("slab", "sub", None, None),
        P("slab", "sub"),
        P(None, "slab", "sub"),
        P(None, "slab", "sub"),
        P(),
        P(),
    )
    return jax.shard_map(
        reduced, mesh=mesh, in_specs=placed, out_specs=(P(), P(), P(), P()), check_vma=False
    )
```

```python
import functools

import jax
import jax.numpy as jnp
from jax import lax
from jax.experimental import pallas as pl
from jax.experimental.pallas import tpu as pltpu
from jax.sharding import Mesh
from jax.sharding import PartitionSpec as P


CHIPS = ("chip", "sub")
F32 = jnp.float32
BF16 = jnp.bfloat16
PANEL = 32
AHEAD = 2


def split2(x):
    high = x.astype(BF16)
    return high, (x - high.astype(F32)).astype(BF16)


def split3(x):
    high = x.astype(BF16)
    rest = x - high.astype(F32)
    mid = rest.astype(BF16)
    return high, mid, (rest - mid.astype(F32)).astype(BF16)


def product(a, b, contract=((1,), (0,))):
    return lax.dot_general(a, b, (contract, ((), ())), preferred_element_type=F32)


def product3(a, b, contract=((1,), (0,))):
    ah, al = split2(a)
    bh, bl = split2(b)
    return product(ah, bh, contract) + (product(ah, bl, contract) + product(al, bh, contract))


def product6(a, b, contract=((1,), (0,))):
    a0, a1, a2 = split3(a)
    b0, b1, b2 = split3(b)
    dot = functools.partial(product, contract=contract)
    small = dot(a1, b1) + (dot(a0, b2) + dot(a2, b0))
    return dot(a0, b0) + ((dot(a0, b1) + dot(a1, b0)) + small)


def rows_split(rows):
    both = jnp.concatenate([rows, rows], axis=0)
    high = both.astype(BF16).astype(F32)
    place = lax.broadcasted_iota(jnp.int32, both.shape, 0)
    halves = jnp.where(place < rows.shape[0], high, both - high)
    return jnp.concatenate([halves, jnp.zeros_like(halves)], axis=0).astype(BF16)


def add_products(total, turned, right, extra=None, few=None):
    count = turned.shape[0]
    th, tl = split2(turned)
    rh, rl = split2(right)
    left = jnp.concatenate([th, tl, th], axis=1)
    if few is not None:
        bottom = jnp.concatenate([few, jnp.zeros_like(few), few], axis=1)
        left = jnp.concatenate([left, bottom], axis=0)
    result = product(left, jnp.concatenate([rh, rh, rl], axis=0))
    total[...] += result[:count]
    if few is not None:
        extra[...] += result[count:]


def plane_rows(rows, plane, first, size):
    chosen = jnp.zeros((rows.shape[0], size), F32)
    for p in range(rows.shape[1]):
        chosen = jnp.where(plane == p, rows[:, p, pl.ds(first, size)], chosen)
    return rows_split(chosen)


def half_of(total, side):
    width = total.shape[1] // 2
    return total[:, pl.ds(pl.multiple_of(side * width, 128), width)]


def core_index():
    return lax.axis_index("core").reshape(1).astype(jnp.int32)


def in_hbm(value):
    return pltpu.with_memory_space_constraint(value, pltpu.HBM)


def gram_kernel(
    core, obs, ctrl, sense,
    own, other, few_far, zlow, zhigh, ylow, yhigh,
    obs_here, ctrl_here, total, extra, sense_here, obs_sems, ctrl_sems, z_sems, low_sems, high_sems, other_sems,
):
    steps, rows, _ = obs.shape
    points = ylow.shape[1]

    def copies(i):
        return (
            pltpu.make_async_copy(obs.at[i], obs_here.at[i], obs_sems.at[i]),
            pltpu.make_async_copy(ctrl.at[i], ctrl_here.at[i], ctrl_sems.at[i]),
        )

    def z_copy(i):
        source = ctrl_here.at[i if i < 2 else steps - 4 + i]
        return pltpu.make_async_copy(source, (zlow if i < 2 else zhigh).at[i % 2], z_sems.at[i])

    def low_copy(p):
        source = ctrl_here.at[2 * p, pl.ds(0, points)]
        return pltpu.make_async_copy(source, ylow.at[p], low_sems.at[p])

    def high_copy(p):
        source = ctrl_here.at[2 * p + 1, pl.ds(rows - points, points)]
        return pltpu.make_async_copy(source, yhigh.at[p], high_sems.at[p])

    sense_copy = pltpu.make_async_copy(sense, sense_here, other_sems.at[0])
    for i in range(AHEAD):
        for copy in copies(i):
            copy.start()
        if i == 0:
            sense_copy.start()
    total[...] = jnp.zeros_like(total)
    extra[...] = jnp.zeros_like(extra)
    sense_copy.wait()

    @pl.loop(0, steps)
    def _(i):
        for copy in copies(i):
            copy.wait()

        @pl.when(i + AHEAD < steps)
        def _():
            for copy in copies(i + AHEAD):
                copy.start()

        for j in range(4):

            @pl.when(i == (j if j < 2 else steps - 4 + j))
            def _():
                z_copy(j).start()

        @pl.when(i % 2 == 0)
        def _():
            low_copy(i // 2).start()

        @pl.when(i % 2 == 1)
        def _():
            high_copy(i // 2).start()

        first = pl.multiple_of((i % 2) * rows, 128)
        some = plane_rows(sense_here, i // 2, first, rows)
        add_products(total, obs_here[i].T, ctrl_here[i], extra, some)

    few_copy = pltpu.make_async_copy(extra, few_far, other_sems.at[0])
    few_copy.start()
    for slot, out in enumerate((own, other)):
        out[...] = half_of(total, core[0] ^ slot).reshape(out.shape)
    few_copy.wait()
    for i in range(4):
        z_copy(i).wait()
    for p in range(steps // 2):
        low_copy(p).wait()
        high_copy(p).wait()


def local_gram(observe, control, sense, points):
    steps, rows, rank = observe.shape
    anywhere = pl.BlockSpec(memory_space=pltpu.HBM)
    vmem = pl.BlockSpec(memory_space=pltpu.VMEM)
    face = pltpu.HBM((2, rows, rank), F32)
    edge = pltpu.HBM((steps // 2, points, rank), F32)
    return pl.pallas_call(
        gram_kernel,
        in_specs=[pl.BlockSpec(memory_space=pltpu.SMEM)] + [anywhere] * 3,
        out_specs=[vmem] * 2 + [anywhere] * 5,
        out_shape=[
            jax.ShapeDtypeStruct((rank // 8, 8, rank // 2), F32),
            jax.ShapeDtypeStruct((rank // 8, 8, rank // 2), F32),
            pltpu.HBM((16, rank), F32),
            face,
            face,
            edge,
            edge,
        ],
        scratch_shapes=[
            pltpu.VMEM((steps, rows, rank), F32),
            pltpu.VMEM((steps, rows, rank), F32),
            pltpu.VMEM((rank, rank), F32),
            pltpu.VMEM((16, rank), F32),
            pltpu.VMEM(sense.shape, F32),
            pltpu.SemaphoreType.DMA((steps,)),
            pltpu.SemaphoreType.DMA((steps,)),
            pltpu.SemaphoreType.DMA((4,)),
            pltpu.SemaphoreType.DMA((steps // 2,)),
            pltpu.SemaphoreType.DMA((steps // 2,)),
            pltpu.SemaphoreType.DMA((1,)),
        ],
        compiler_params=pltpu.CompilerParams(vmem_limit_bytes=36 << 20),
        cost_estimate=pl.CostEstimate(
            flops=6 * steps * rows * rank * rank, bytes_accessed=24 << 20, transcendentals=0
        ),
        name="local_gram",
    )(core_index(), in_hbm(observe), in_hbm(control), in_hbm(sense))


def inner_kernel(
    points, obs_far, ctrl_far, conduct, drive,
    total_far, extra_far, total, extra, obs, ctrl, conduct_here, drive_here, sems, obs_sems, ctrl_sems,
):
    steps, rows, rank = ctrl.shape
    planes = steps // 2
    small = [
        pltpu.make_async_copy(conduct, conduct_here, sems.at[0]),
        pltpu.make_async_copy(drive, drive_here, sems.at[1]),
    ]

    def ctrl_copy(i):
        return pltpu.make_async_copy(ctrl_far.at[i], ctrl.at[i], ctrl_sems.at[i])

    def obs_copy(i):
        return pltpu.make_async_copy(obs_far.at[i], obs.at[i], obs_sems.at[i])

    for i in (0, 1, 2):
        ctrl_copy(i).start()
    obs_copy(0).start()
    for copy in small:
        copy.start()
    ctrl_copy(3).start()
    obs_copy(1).start()
    total[...] = jnp.zeros_like(total)
    extra[...] = jnp.zeros_like(extra)
    for copy in small:
        copy.wait()
    ctrl_copy(0).wait()
    ctrl_copy(1).wait()
    empty = jnp.zeros((points, rank), F32)

    @pl.loop(0, planes)
    def _(p):
        up = jnp.minimum(p + 1, planes - 1)
        down = jnp.maximum(p - 1, 0)
        has_up = (p + 1 < planes).astype(F32)
        has_down = (p > 0).astype(F32)
        for half in range(2):

            @pl.when(p + 1 < planes)
            def _():
                ctrl_copy(2 * p + 2 + half).wait()

            @pl.when(p + 2 < planes)
            def _():
                ctrl_copy(2 * p + 4 + half).start()

            @pl.when(p + 1 < planes)
            def _():
                obs_copy(2 * p + 2 + half).start()

            obs_copy(2 * p + half).wait()
            center = ctrl[2 * p + half]
            beside = has_up * ctrl[2 * up + half] + has_down * ctrl[2 * down + half]
            if half == 0:
                before = empty
                after = ctrl[2 * p + 1, :points]
            else:
                before = ctrl[2 * p, rows - points :]
                after = empty
            beside = beside + jnp.concatenate([before, center[: rows - points]], axis=0)
            beside = beside + jnp.concatenate([center[points:], after], axis=0)
            place = lax.broadcasted_iota(jnp.int32, (rows, rank), 0) % points
            beside = beside + jnp.where(place > 0, pltpu.roll(center, 1, 0), 0.0)
            beside = beside + jnp.where(place < points - 1, pltpu.roll(center, rows - 1, 0), 0.0)
            first = half * rows
            scale = conduct_here[pl.ds(p, 1), first : first + rows] * (1.0 / 6.0)
            applied = (beside - 6.0 * center).T * scale
            some = plane_rows(drive_here, p, first, rows)
            add_products(total, applied, obs[2 * p + half], extra, some)

    results = [
        pltpu.make_async_copy(total, total_far, sems.at[0]),
        pltpu.make_async_copy(extra, extra_far, sems.at[1]),
    ]
    for copy in results:
        copy.start()
    for copy in results:
        copy.wait()


def inner_operator(observe, control, conduct, drive, points):
    steps, rows, rank = control.shape
    anywhere = pl.BlockSpec(memory_space=pltpu.HBM)
    return pl.pallas_call(
        functools.partial(inner_kernel, points),
        in_specs=[anywhere] * 4,
        out_specs=[anywhere] * 2,
        out_shape=[
            pltpu.HBM((rank, rank), F32),
            pltpu.HBM((16, rank), F32),
        ],
        scratch_shapes=[
            pltpu.VMEM((rank, rank), F32),
            pltpu.VMEM((16, rank), F32),
            pltpu.VMEM((steps, rows, rank), F32),
            pltpu.VMEM((steps, rows, rank), F32),
            pltpu.VMEM(conduct.shape, F32),
            pltpu.VMEM(drive.shape, F32),
            pltpu.SemaphoreType.DMA((2,)),
            pltpu.SemaphoreType.DMA((steps,)),
            pltpu.SemaphoreType.DMA((steps,)),
        ],
        compiler_params=pltpu.CompilerParams(vmem_limit_bytes=36 << 20),
        cost_estimate=pl.CostEstimate(
            flops=6 * steps * rows * rank * rank, bytes_accessed=18 << 20, transcendentals=0
        ),
        name="inner_operator",
    )(in_hbm(observe), in_hbm(control), in_hbm(conduct), in_hbm(drive))


def outer_kernel(
    points, core, obs, zlow, zhigh, ylow, yhigh, conduct, inner, extra_far, few_far,
    own, other, z_field, y_field, z_obs, y_obs, conduct_here, total, extra, few_ctrl, sems, obs_sems,
):
    steps, rows, rank = obs.shape
    planes = steps // 2
    conduct_copy = pltpu.make_async_copy(conduct, conduct_here, sems.at[0])
    inner_copy = pltpu.make_async_copy(inner, total, sems.at[7])
    few_copies = [
        pltpu.make_async_copy(extra_far, extra, sems.at[8]),
        pltpu.make_async_copy(few_far, few_ctrl, sems.at[9]),
    ]
    y_near = [
        pltpu.make_async_copy(
            obs.at[2 * p + i, pl.ds(i * (rows - points), points)],
            y_obs.at[i, pl.ds(p * points, points)],
            obs_sems.at[4 + planes * i + p],
        )
        for i in range(2)
        for p in range(planes)
    ]
    z_near = [
        pltpu.make_async_copy(
            obs.at[i if i < 2 else steps - 4 + i], z_obs.at[i], obs_sems.at[i]
        )
        for i in range(4)
    ]
    y_copies = [
        pltpu.make_async_copy(ylow, y_field.at[0], sems.at[1]),
        pltpu.make_async_copy(yhigh, y_field.at[1], sems.at[2]),
    ]
    z_copies = [
        pltpu.make_async_copy(face.at[half], z_field.at[2 * i + half], sems.at[3 + 2 * i + half])
        for i, face in enumerate((zlow, zhigh))
        for half in range(2)
    ]
    conduct_copy.start()
    for copy in y_copies + y_near + [inner_copy]:
        copy.start()
    for far, near in zip(z_copies, z_near):
        far.start()
        near.start()
    for copy in few_copies:
        copy.start()
    conduct_copy.wait()
    scale = conduct_here[...] * (1.0 / 6.0)
    for copy in y_copies + y_near + [inner_copy]:
        copy.wait()
    for i in range(2):
        cells = i * (2 * rows - points)
        near = y_obs[i]
        turned = [
            y_field[i, p].T * scale[p : p + 1, cells : cells + points] for p in range(planes)
        ]
        add_products(total, jnp.concatenate(turned, axis=1), near)
    for i in range(2):
        plane = (planes - 1) * i
        for half in range(2):
            z_copies[2 * i + half].wait()
            z_near[2 * i + half].wait()
            turned = z_field[2 * i + half].T
            turned = turned * scale[plane : plane + 1, half * rows : (half + 1) * rows]
            add_products(total, turned, z_obs[2 * i + half])

    for copy in few_copies:
        copy.wait()
    summed = jnp.concatenate([extra[0:4] + extra[4:8], few_ctrl[0:4] + few_ctrl[4:8]], axis=0)
    wide = jnp.concatenate([summed, jnp.zeros((120, rank), F32)], axis=0).T
    width = rank // 2
    for slot, out in enumerate((own, other)):
        side = core[0] ^ slot
        out[:, :, :width] = half_of(total, side).reshape(out.shape[0], out.shape[1], width)
        part = wide * (side == 0).astype(F32)
        out[:, :, width:] = part.reshape(out.shape[0], out.shape[1], 128)


def with_outer(observe, faces, conduct, inner, extra, few_ctrl, points):
    steps, rows, rank = observe.shape
    anywhere = pl.BlockSpec(memory_space=pltpu.HBM)
    vmem = pl.BlockSpec(memory_space=pltpu.VMEM)
    return pl.pallas_call(
        functools.partial(outer_kernel, points),
        in_specs=[pl.BlockSpec(memory_space=pltpu.SMEM)] + [anywhere] * 9,
        out_specs=[vmem] * 2,
        out_shape=[jax.ShapeDtypeStruct((rank // 8, 8, rank // 2 + 128), F32)] * 2,
        scratch_shapes=[
            pltpu.VMEM((4, rows, rank), F32),
            pltpu.VMEM((2, steps // 2, points, rank), F32),
            pltpu.VMEM((4, rows, rank), F32),
            pltpu.VMEM((2, steps // 2 * points, rank), F32),
            pltpu.VMEM(conduct.shape, F32),
            pltpu.VMEM((rank, rank), F32),
            pltpu.VMEM(extra.shape, F32),
            pltpu.VMEM(few_ctrl.shape, F32),
            pltpu.SemaphoreType.DMA((10,)),
            pltpu.SemaphoreType.DMA((4 + steps,)),
        ],
        compiler_params=pltpu.CompilerParams(vmem_limit_bytes=36 << 20),
        cost_estimate=pl.CostEstimate(
            flops=30 * rows * rank * rank, bytes_accessed=7 << 20, transcendentals=0
        ),
        name="outer_operator",
    )(core_index(), *map(in_hbm, (observe, *faces, conduct, inner, extra, few_ctrl)))


def sum_kernel(parts, out):
    whole = jnp.sum(parts[...], axis=0, keepdims=True)
    out[...] = jnp.broadcast_to(whole, out.shape)


def swapped(value):
    return lax.ppermute(value, "core", [(0, 1), (1, 0)])


def add_kernel(first, second, out):
    out[...] = first[...] + second[...]


def scattered(own, other):
    other = swapped(other)
    both = pl.pallas_call(
        add_kernel,
        out_shape=jax.ShapeDtypeStruct(own.shape, F32),
        compiler_params=pltpu.CompilerParams(vmem_limit_bytes=6 << 20),
        cost_estimate=pl.CostEstimate(
            flops=own.size, bytes_accessed=12 * own.size, transcendentals=0
        ),
    )(own, other)
    return lax.all_to_all(both, CHIPS, 0, 0, tiled=True)


def summed_copies(arrived):
    return pl.pallas_call(
        sum_kernel,
        out_shape=jax.ShapeDtypeStruct(arrived.shape, F32),
        compiler_params=pltpu.CompilerParams(vmem_limit_bytes=6 << 20),
        cost_estimate=pl.CostEstimate(
            flops=arrived.size, bytes_accessed=8 * arrived.size, transcendentals=0
        ),
        name="sum_gram",
    )(arrived)


def project_kernel(side, parts, left, out):
    block = jnp.sum(parts[...], axis=0)
    half = left.shape[1] // 2
    mine = jnp.where(side[0] == 0, left[:, :half], left[:, half:])
    turned = product3(block[:, :half], mine, ((1,), (1,)))
    whole = jnp.concatenate([turned, block[:, half:]], axis=1)
    out[...] = jnp.broadcast_to(whole[None], out.shape)


def projected_copies(arrived, left):
    vmem = pl.BlockSpec(memory_space=pltpu.VMEM)
    return pl.pallas_call(
        project_kernel,
        in_specs=[pl.BlockSpec(memory_space=pltpu.SMEM), vmem, vmem],
        out_specs=vmem,
        out_shape=jax.ShapeDtypeStruct((arrived.shape[0], 8, 256), F32),
        compiler_params=pltpu.CompilerParams(vmem_limit_bytes=8 << 20),
        cost_estimate=pl.CostEstimate(
            flops=arrived.size, bytes_accessed=8 * arrived.size, transcendentals=0
        ),
        name="project",
    )(core_index(), arrived, left)


def gathered(copies):
    mine = lax.all_to_all(copies, CHIPS, 0, 0, tiled=True)
    return mine, swapped(mine)


def inverse_factor(work):
    size = work.shape[0]
    for first in range(0, size, PANEL):
        last = first + PANEL
        panel = [work[first + 8 * g : first + 8 * g + 8, :] for g in range(PANEL // 8)]
        groups = PANEL // 8
        columns = {}
        for k in range(PANEL):
            for g in range(k // 8, groups):
                columns[k, g] = jnp.broadcast_to(
                    panel[g][:, first + k : first + k + 1], (8, 128)
                )
        place = lax.broadcasted_iota(jnp.int32, (8, 128), 0)
        for j in range(PANEL):
            gj, sj = divmod(j, 8)
            pivot = jnp.broadcast_to(columns[j, gj][sj : sj + 1], (8, 128))
            scale = lax.rsqrt(pivot)
            lower = {}
            for g in range(gj, groups):
                lower[g] = columns[j, g] * scale
            row = jnp.broadcast_to(panel[gj][sj : sj + 1], (8, 256))
            row = row * jnp.concatenate([scale, scale], axis=1)
            for k in range(j + 1, PANEL):
                gk, sk = divmod(k, 8)
                across = jnp.broadcast_to(lower[gk][sk : sk + 1], (8, 128))
                for g in range(gk, groups):
                    columns[k, g] = columns[k, g] - lower[g] * across
            for g in range(gj, groups):
                weight = lower[g]
                if g == gj:
                    weight = jnp.where(place > sj, weight, 0.0)
                wide = jnp.concatenate([weight, weight], axis=1)
                panel[g] = panel[g] - wide * row
            wide_place = lax.broadcasted_iota(jnp.int32, (8, 256), 0)
            panel[gj] = jnp.where(wide_place == sj, row, panel[gj])
        for g in range(groups):
            work[first + 8 * g : first + 8 * g + 8, :] = panel[g]
        if last < size:
            done = jnp.concatenate(panel, axis=0)
            u0, u1, u2 = split3(done)
            left = jnp.concatenate([u0, u0, u1, u1, u0, u2], axis=0)[:, :size]
            right = jnp.concatenate([u0, u1, u0, u1, u2, u0], axis=0)
            change = product(left, right, ((0,), (0,)))
            work[last:, :] -= change[last:, :]


def bases_kernel(core, mine, theirs, start, right_out, left_out, image_out, high, low, basis, work):
    rank = high.shape[0]
    half = rank // 2
    for slot, part in enumerate((mine, theirs)):
        place = pl.ds(pl.multiple_of((core[0] ^ slot) * half, 128), half)
        high[:, place], low[:, place] = split2(part[...].reshape(rank, half))
    basis[...] = start[...].T
    size = basis.shape[0]
    eye = (
        lax.broadcasted_iota(jnp.int32, (size, size), 0)
        == lax.broadcasted_iota(jnp.int32, (size, size), 1)
    ).astype(F32)

    @pl.loop(0, 4)
    def _(turn):
        for parity, contract in enumerate((((1,), (0,)), ((1,), (1,)))):

            @pl.when(turn % 2 == parity)
            def _():
                bh, bl = split2(basis[...])
                small = product(bh, low[...], contract) + product(bl, high[...], contract)
                image_out[...] = product(bh, high[...], contract) + small

        held = image_out[...]
        work[:, :size] = product6(held, held, ((1,), (1,)))
        work[:, size:] = eye
        inverse_factor(work)
        basis[...] = product6(work[:, size:], held)

        @pl.when(turn == 2)
        def _():
            right_out[...] = basis[...]

    left_out[...] = basis[...]


def bases(mine, theirs, start):
    rank, size = start.shape
    shape = jax.ShapeDtypeStruct((size, rank), F32)
    vmem = pl.BlockSpec(memory_space=pltpu.VMEM)
    return pl.pallas_call(
        bases_kernel,
        in_specs=[pl.BlockSpec(memory_space=pltpu.SMEM)] + [vmem] * 3,
        out_shape=[shape, shape, shape],
        scratch_shapes=[
            pltpu.VMEM((rank, rank), BF16),
            pltpu.VMEM((rank, rank), BF16),
            pltpu.VMEM((size, rank), F32),
            pltpu.VMEM((size, 2 * size), F32),
        ],
        compiler_params=pltpu.CompilerParams(vmem_limit_bytes=16 << 20),
        cost_estimate=pl.CostEstimate(
            flops=20_000_000_000, bytes_accessed=4 << 20, transcendentals=0
        ),
        name="bases",
    )(core_index(), mine, theirs, start)


def finish_kernel(order, right, left, image, mine, theirs, mass, state, inputs, outputs):
    size, rank = right.shape
    blocks = (mine[...] + theirs[...]).reshape(rank, size + 128)
    turned, few = blocks[:, :size], blocks[:, size:]
    kept_col = lax.broadcasted_iota(jnp.int32, (size, size), 0) < order[0]
    kept_row = lax.broadcasted_iota(jnp.int32, (size, size), 1) < order[0]
    kept = jnp.logical_and(kept_col, kept_row).astype(F32)
    mass[...] = kept * product6(left[...], image[...], ((1,), (1,)))
    state[...] = kept * product3(right[...], turned).T
    inputs[...] = (kept_row.astype(F32) * product3(left[...], few).T)[:4]
    outputs[...] = (kept_row.astype(F32) * product3(right[...], few).T)[4:8]


def finish(order, right, left, image, mine, theirs):
    size, _ = right.shape
    vmem = pl.BlockSpec(memory_space=pltpu.VMEM)
    return pl.pallas_call(
        finish_kernel,
        in_specs=[pl.BlockSpec(memory_space=pltpu.SMEM)] + [vmem] * 5,
        out_specs=[vmem] * 4,
        out_shape=[
            jax.ShapeDtypeStruct((size, size), F32),
            jax.ShapeDtypeStruct((size, size), F32),
            jax.ShapeDtypeStruct((4, size), F32),
            jax.ShapeDtypeStruct((4, size), F32),
        ],
        compiler_params=pltpu.CompilerParams(vmem_limit_bytes=16 << 20),
        cost_estimate=pl.CostEstimate(
            flops=1_000_000_000, bytes_accessed=4 << 20, transcendentals=0
        ),
        name="finish",
    )(order, right, left, image, mine, theirs)


def from_neighbours(low_face, high_face, axis):
    count = lax.axis_size(axis)
    up = [(i, i + 1) for i in range(count - 1)]
    down = [(b, a) for a, b in up]
    return lax.ppermute(high_face, axis, up), lax.ppermute(low_face, axis, down)


def reduced(factor_obs, factor_ctrl, diffusivity, input_map, output_map, start_block, order):
    planes, lines, points, rank = factor_ctrl.shape
    halves = (2 * planes, lines * points // 2, rank)
    observe = factor_obs.reshape(halves)
    control = factor_ctrl.reshape(halves)
    own, other, few_ctrl, zlow, zhigh, ylow, yhigh = local_gram(
        observe, control, output_map, points
    )
    arrived = scattered(own, other)
    zlow, zhigh = from_neighbours(zlow, zhigh, ("chip", "core"))
    ylow, yhigh = from_neighbours(ylow, yhigh, "sub")
    inner, extra = inner_operator(observe, control, diffusivity, input_map, points)
    gram = gathered(summed_copies(arrived))
    faces = (zlow, zhigh, ylow, yhigh)
    own, other = with_outer(observe, faces, diffusivity, inner, extra, few_ctrl, points)
    oper = scattered(own, other)
    right, left, image = bases(*gram, start_block)
    blocks = gathered(projected_copies(oper, left))
    mass, state, inputs, outputs = finish(order, right, left, image, *blocks)
    return mass, state, inputs.T, outputs


def solution(mesh):
    slab = mesh.shape["slab"]
    torus = Mesh(
        mesh.devices.reshape(slab // 2, 2, mesh.shape["sub"]), ("chip", "core", "sub")
    )
    slabs = ("chip", "core")
    placed = (
        P(slabs, "sub", None, None),
        P(slabs, "sub", None, None),
        P(slabs, "sub"),
        P(None, slabs, "sub"),
        P(None, slabs, "sub"),
        P(),
        P(),
    )
    return jax.shard_map(
        reduced, mesh=torus, in_specs=placed, out_specs=(P(), P(), P(), P()), check_vma=False
    )
```

```python
import functools

import jax
import jax.numpy as jnp
from jax import lax
from jax.experimental import pallas as pl
from jax.experimental.pallas import tpu as pltpu
from jax.sharding import Mesh
from jax.sharding import PartitionSpec as P


CHIPS = ("chip", "sub")
F32 = jnp.float32
BF16 = jnp.bfloat16
PANEL = 32


def split2(x):
    high = x.astype(BF16)
    return high, (x - high.astype(F32)).astype(BF16)


def split3(x):
    high = x.astype(BF16)
    rest = x - high.astype(F32)
    mid = rest.astype(BF16)
    return high, mid, (rest - mid.astype(F32)).astype(BF16)


def product(a, b, contract=((1,), (0,))):
    return lax.dot_general(a, b, (contract, ((), ())), preferred_element_type=F32)


def product3(a, b, contract=((1,), (0,))):
    ah, al = split2(a)
    bh, bl = split2(b)
    return product(ah, bh, contract) + (product(ah, bl, contract) + product(al, bh, contract))


def product6(a, b, contract=((1,), (0,))):
    a0, a1, a2 = split3(a)
    b0, b1, b2 = split3(b)
    dot = functools.partial(product, contract=contract)
    small = dot(a1, b1) + (dot(a0, b2) + dot(a2, b0))
    return dot(a0, b0) + ((dot(a0, b1) + dot(a1, b0)) + small)


def rows_split(rows):
    both = jnp.concatenate([rows, rows], axis=0)
    high = both.astype(BF16).astype(F32)
    place = lax.broadcasted_iota(jnp.int32, both.shape, 0)
    halves = jnp.where(place < rows.shape[0], high, both - high)
    return jnp.concatenate([halves, jnp.zeros_like(halves)], axis=0).astype(BF16)


def add_products(total, turned, right, extra=None, few=None):
    count = turned.shape[0]
    th, tl = split2(turned)
    rh, rl = split2(right)
    left = jnp.concatenate([th, tl, th], axis=1)
    if few is not None:
        bottom = jnp.concatenate([few, jnp.zeros_like(few), few], axis=1)
        left = jnp.concatenate([left, bottom], axis=0)
    result = product(left, jnp.concatenate([rh, rh, rl], axis=0))
    total[...] += result[:count]
    if few is not None:
        extra[...] += result[count:]


def plane_rows(rows, plane, first, size):
    chosen = jnp.zeros((rows.shape[0], size), F32)
    for p in range(rows.shape[1]):
        chosen = jnp.where(plane == p, rows[:, p, pl.ds(first, size)], chosen)
    return rows_split(chosen)


def half_of(total, side):
    width = total.shape[1] // 2
    return total[:, pl.ds(pl.multiple_of(side * width, 128), width)]


def core_index():
    return lax.axis_index("core").reshape(1).astype(jnp.int32)


def in_hbm(value):
    return pltpu.with_memory_space_constraint(value, pltpu.HBM)


def local_kernel(
    points, core, obs_far, ctrl_far, sense, conduct, drive,
    own, other, few_far, zlow, zhigh, ylow, yhigh, total_far, extra_far,
    obs, ctrl, gram, few, total, extra, sense_here, conduct_here, drive_here,
    obs_sems, ctrl_sems, z_sems, low_sems, high_sems, small_sems,
):
    steps, rows, rank = ctrl.shape
    planes = steps // 2

    def ctrl_copy(i):
        return pltpu.make_async_copy(ctrl_far.at[i], ctrl.at[i], ctrl_sems.at[i])

    def obs_copy(i):
        return pltpu.make_async_copy(obs_far.at[i], obs.at[i], obs_sems.at[i])

    def z_copy(i):
        source = ctrl.at[i if i < 2 else steps - 4 + i]
        return pltpu.make_async_copy(source, (zlow if i < 2 else zhigh).at[i % 2], z_sems.at[i])

    def low_copy(p):
        source = ctrl.at[2 * p, pl.ds(0, points)]
        return pltpu.make_async_copy(source, ylow.at[p], low_sems.at[p])

    def high_copy(p):
        source = ctrl.at[2 * p + 1, pl.ds(rows - points, points)]
        return pltpu.make_async_copy(source, yhigh.at[p], high_sems.at[p])

    small = [
        pltpu.make_async_copy(far, here, small_sems.at[i])
        for i, (far, here) in enumerate(
            ((sense, sense_here), (conduct, conduct_here), (drive, drive_here))
        )
    ]
    for i in (0, 1, 2):
        ctrl_copy(i).start()
    obs_copy(0).start()
    for copy in small:
        copy.start()
    ctrl_copy(3).start()
    obs_copy(1).start()
    for ref in (gram, few, total, extra):
        ref[...] = jnp.zeros_like(ref)
    for copy in small:
        copy.wait()
    for i in range(2):
        ctrl_copy(i).wait()
        z_copy(i).start()
    empty = jnp.zeros((points, rank), F32)

    @pl.loop(0, planes)
    def _(p):
        up = jnp.minimum(p + 1, planes - 1)
        down = jnp.maximum(p - 1, 0)
        has_up = (p + 1 < planes).astype(F32)
        has_down = (p > 0).astype(F32)
        low_copy(p).start()
        high_copy(p).start()
        for half in range(2):

            @pl.when(p + 1 < planes)
            def _():
                ctrl_copy(2 * p + 2 + half).wait()

            @pl.when(p + 2 < planes)
            def _():
                ctrl_copy(2 * p + 4 + half).start()

            @pl.when(p + 1 < planes)
            def _():
                obs_copy(2 * p + 2 + half).start()

            @pl.when(p + 2 == planes)
            def _():
                z_copy(2 + half).start()

            obs_copy(2 * p + half).wait()
            near = obs[2 * p + half]
            center = ctrl[2 * p + half]
            first = half * rows
            add_products(gram, near.T, center, few, plane_rows(sense_here, p, first, rows))
            beside = has_up * ctrl[2 * up + half] + has_down * ctrl[2 * down + half]
            if half == 0:
                before = empty
                after = ctrl[2 * p + 1, :points]
            else:
                before = ctrl[2 * p, rows - points :]
                after = empty
            beside = beside + jnp.concatenate([before, center[: rows - points]], axis=0)
            beside = beside + jnp.concatenate([center[points:], after], axis=0)
            place = lax.broadcasted_iota(jnp.int32, (rows, rank), 0) % points
            beside = beside + jnp.where(place > 0, pltpu.roll(center, 1, 0), 0.0)
            beside = beside + jnp.where(place < points - 1, pltpu.roll(center, rows - 1, 0), 0.0)
            scale = conduct_here[pl.ds(p, 1), first : first + rows] * (1.0 / 6.0)
            applied = (beside - 6.0 * center).T * scale
            add_products(total, applied, near, extra, plane_rows(drive_here, p, first, rows))

    results = [
        pltpu.make_async_copy(here, far, small_sems.at[i])
        for i, (here, far) in enumerate(((few, few_far), (total, total_far), (extra, extra_far)))
    ]
    for copy in results:
        copy.start()
    for slot, out in enumerate((own, other)):
        out[...] = half_of(gram, core[0] ^ slot).reshape(out.shape)
    for copy in results:
        copy.wait()
    for i in range(4):
        z_copy(i).wait()
    for p in range(planes):
        low_copy(p).wait()
        high_copy(p).wait()


def local_products(observe, control, sense, conduct, drive, points):
    steps, rows, rank = observe.shape
    anywhere = pl.BlockSpec(memory_space=pltpu.HBM)
    vmem = pl.BlockSpec(memory_space=pltpu.VMEM)
    chunks = jax.ShapeDtypeStruct((rank // 8, 8, rank // 2), F32)
    few = pltpu.HBM((16, rank), F32)
    face = pltpu.HBM((2, rows, rank), F32)
    edge = pltpu.HBM((steps // 2, points, rank), F32)
    return pl.pallas_call(
        functools.partial(local_kernel, points),
        in_specs=[pl.BlockSpec(memory_space=pltpu.SMEM)] + [anywhere] * 5,
        out_specs=[vmem] * 2 + [anywhere] * 7,
        out_shape=[chunks, chunks, few, face, face, edge, edge, pltpu.HBM((rank, rank), F32), few],
        scratch_shapes=[
            pltpu.VMEM((steps, rows, rank), F32),
            pltpu.VMEM((steps, rows, rank), F32),
            pltpu.VMEM((rank, rank), F32),
            pltpu.VMEM((16, rank), F32),
            pltpu.VMEM((rank, rank), F32),
            pltpu.VMEM((16, rank), F32),
            pltpu.VMEM(sense.shape, F32),
            pltpu.VMEM(conduct.shape, F32),
            pltpu.VMEM(drive.shape, F32),
            pltpu.SemaphoreType.DMA((steps,)),
            pltpu.SemaphoreType.DMA((steps,)),
            pltpu.SemaphoreType.DMA((4,)),
            pltpu.SemaphoreType.DMA((steps // 2,)),
            pltpu.SemaphoreType.DMA((steps // 2,)),
            pltpu.SemaphoreType.DMA((3,)),
        ],
        compiler_params=pltpu.CompilerParams(vmem_limit_bytes=44 << 20),
        cost_estimate=pl.CostEstimate(
            flops=12 * steps * rows * rank * rank, bytes_accessed=26 << 20, transcendentals=0
        ),
        name="local_products",
    )(core_index(), *map(in_hbm, (observe, control, sense, conduct, drive)))


def outer_kernel(
    points, obs, zlow, zhigh, ylow, yhigh, conduct, inner, extra_far, few_far,
    out, z_field, y_field, z_obs, y_obs, conduct_here, total, extra, few_ctrl, sems, obs_sems,
):
    steps, rows, rank = obs.shape
    planes = steps // 2
    conduct_copy = pltpu.make_async_copy(conduct, conduct_here, sems.at[0])
    inner_copy = pltpu.make_async_copy(inner, total, sems.at[7])
    few_copies = [
        pltpu.make_async_copy(extra_far, extra, sems.at[8]),
        pltpu.make_async_copy(few_far, few_ctrl, sems.at[9]),
    ]
    y_near = [
        pltpu.make_async_copy(
            obs.at[2 * p + i, pl.ds(i * (rows - points), points)],
            y_obs.at[i, pl.ds(p * points, points)],
            obs_sems.at[4 + planes * i + p],
        )
        for i in range(2)
        for p in range(planes)
    ]
    z_near = [
        pltpu.make_async_copy(
            obs.at[i if i < 2 else steps - 4 + i], z_obs.at[i], obs_sems.at[i]
        )
        for i in range(4)
    ]
    y_copies = [
        pltpu.make_async_copy(ylow, y_field.at[0], sems.at[1]),
        pltpu.make_async_copy(yhigh, y_field.at[1], sems.at[2]),
    ]
    z_copies = [
        pltpu.make_async_copy(face.at[half], z_field.at[2 * i + half], sems.at[3 + 2 * i + half])
        for i, face in enumerate((zlow, zhigh))
        for half in range(2)
    ]
    conduct_copy.start()
    for copy in y_copies + y_near + [inner_copy]:
        copy.start()
    for far, near in zip(z_copies, z_near):
        far.start()
        near.start()
    for copy in few_copies:
        copy.start()
    conduct_copy.wait()
    scale = conduct_here[...] * (1.0 / 6.0)
    for copy in y_copies + y_near + [inner_copy]:
        copy.wait()
    for i in range(2):
        cells = i * (2 * rows - points)
        near = y_obs[i]
        turned = [
            y_field[i, p].T * scale[p : p + 1, cells : cells + points] for p in range(planes)
        ]
        add_products(total, jnp.concatenate(turned, axis=1), near)
    for i in range(2):
        plane = (planes - 1) * i
        for half in range(2):
            z_copies[2 * i + half].wait()
            z_near[2 * i + half].wait()
            turned = z_field[2 * i + half].T
            turned = turned * scale[plane : plane + 1, half * rows : (half + 1) * rows]
            add_products(total, turned, z_obs[2 * i + half])

    for copy in few_copies:
        copy.wait()
    summed = jnp.concatenate([extra[0:4] + extra[4:8], few_ctrl[0:4] + few_ctrl[4:8]], axis=0)
    wide = jnp.concatenate([summed, jnp.zeros((120, rank), F32)], axis=0).T
    width = rank // 2
    for side in range(2):
        cols = total[:, side * width : (side + 1) * width]
        out[:, side, :, :width] = cols.reshape(out.shape[0], out.shape[2], width)
    out[:, 0, :, width:] = wide.reshape(out.shape[0], out.shape[2], 128)
    out[:, 1, :, width:] = jnp.zeros((out.shape[0], out.shape[2], 128), F32)


def with_outer(observe, faces, conduct, inner, extra, few_ctrl, points):
    steps, rows, rank = observe.shape
    anywhere = pl.BlockSpec(memory_space=pltpu.HBM)
    vmem = pl.BlockSpec(memory_space=pltpu.VMEM)
    return pl.pallas_call(
        functools.partial(outer_kernel, points),
        in_specs=[anywhere] * 9,
        out_specs=vmem,
        out_shape=jax.ShapeDtypeStruct((rank // 8, 2, 8, rank // 2 + 128), F32),
        scratch_shapes=[
            pltpu.VMEM((4, rows, rank), F32),
            pltpu.VMEM((2, steps // 2, points, rank), F32),
            pltpu.VMEM((4, rows, rank), F32),
            pltpu.VMEM((2, steps // 2 * points, rank), F32),
            pltpu.VMEM(conduct.shape, F32),
            pltpu.VMEM((rank, rank), F32),
            pltpu.VMEM(extra.shape, F32),
            pltpu.VMEM(few_ctrl.shape, F32),
            pltpu.SemaphoreType.DMA((10,)),
            pltpu.SemaphoreType.DMA((4 + steps,)),
        ],
        compiler_params=pltpu.CompilerParams(vmem_limit_bytes=36 << 20),
        cost_estimate=pl.CostEstimate(
            flops=30 * rows * rank * rank, bytes_accessed=7 << 20, transcendentals=0
        ),
        name="outer_operator",
    )(*map(in_hbm, (observe, *faces, conduct, inner, extra, few_ctrl)))


def sum_kernel(parts, out):
    whole = jnp.sum(parts[...], axis=0, keepdims=True)
    out[...] = jnp.broadcast_to(whole, out.shape)


def swapped(value):
    return lax.ppermute(value, "core", [(0, 1), (1, 0)])


def add_kernel(first, second, out):
    out[...] = first[...] + second[...]


def scattered(own, other):
    other = swapped(other)
    both = pl.pallas_call(
        add_kernel,
        out_shape=jax.ShapeDtypeStruct(own.shape, F32),
        compiler_params=pltpu.CompilerParams(vmem_limit_bytes=6 << 20),
        cost_estimate=pl.CostEstimate(
            flops=own.size, bytes_accessed=12 * own.size, transcendentals=0
        ),
    )(own, other)
    return lax.all_to_all(both, CHIPS, 0, 0, tiled=True)


def summed_copies(arrived):
    return pl.pallas_call(
        sum_kernel,
        out_shape=jax.ShapeDtypeStruct(arrived.shape, F32),
        compiler_params=pltpu.CompilerParams(vmem_limit_bytes=6 << 20),
        cost_estimate=pl.CostEstimate(
            flops=arrived.size, bytes_accessed=8 * arrived.size, transcendentals=0
        ),
        name="sum_gram",
    )(arrived)


def project_kernel(side, parts, left, out):
    block = jnp.sum(parts[...], axis=0)
    half = left.shape[1] // 2
    mine = jnp.where(side[0] == 0, left[:, :half], left[:, half:])
    turned = product3(block[:, :half], mine, ((1,), (1,)))
    whole = jnp.concatenate([turned, block[:, half:]], axis=1)
    out[...] = jnp.broadcast_to(whole[None], out.shape)


def projected_copies(arrived, left):
    vmem = pl.BlockSpec(memory_space=pltpu.VMEM)
    return pl.pallas_call(
        project_kernel,
        in_specs=[pl.BlockSpec(memory_space=pltpu.SMEM), vmem, vmem],
        out_specs=vmem,
        out_shape=jax.ShapeDtypeStruct((arrived.shape[0] // 2, 8, 256), F32),
        compiler_params=pltpu.CompilerParams(vmem_limit_bytes=8 << 20),
        cost_estimate=pl.CostEstimate(
            flops=arrived.size, bytes_accessed=8 * arrived.size, transcendentals=0
        ),
        name="project",
    )(core_index(), arrived, left)


def gathered(copies):
    mine = lax.all_to_all(copies, CHIPS, 0, 0, tiled=True)
    return mine, swapped(mine)


def inverse_factor(work):
    size = work.shape[0]
    for first in range(0, size, PANEL):
        last = first + PANEL
        panel = [work[first + 8 * g : first + 8 * g + 8, :] for g in range(PANEL // 8)]
        groups = PANEL // 8
        columns = {}
        for k in range(PANEL):
            for g in range(k // 8, groups):
                columns[k, g] = jnp.broadcast_to(
                    panel[g][:, first + k : first + k + 1], (8, 128)
                )
        place = lax.broadcasted_iota(jnp.int32, (8, 128), 0)
        for j in range(PANEL):
            gj, sj = divmod(j, 8)
            pivot = jnp.broadcast_to(columns[j, gj][sj : sj + 1], (8, 128))
            scale = lax.rsqrt(pivot)
            lower = {}
            for g in range(gj, groups):
                lower[g] = columns[j, g] * scale
            row = jnp.broadcast_to(panel[gj][sj : sj + 1], (8, 256))
            row = row * jnp.concatenate([scale, scale], axis=1)
            for k in range(j + 1, PANEL):
                gk, sk = divmod(k, 8)
                across = jnp.broadcast_to(lower[gk][sk : sk + 1], (8, 128))
                for g in range(gk, groups):
                    columns[k, g] = columns[k, g] - lower[g] * across
            for g in range(gj, groups):
                weight = lower[g]
                if g == gj:
                    weight = jnp.where(place > sj, weight, 0.0)
                wide = jnp.concatenate([weight, weight], axis=1)
                panel[g] = panel[g] - wide * row
            wide_place = lax.broadcasted_iota(jnp.int32, (8, 256), 0)
            panel[gj] = jnp.where(wide_place == sj, row, panel[gj])
        for g in range(groups):
            work[first + 8 * g : first + 8 * g + 8, :] = panel[g]
        if last < size:
            done = jnp.concatenate(panel, axis=0)
            u0, u1, u2 = split3(done)
            left = jnp.concatenate([u0, u0, u1, u1, u0, u2], axis=0)[:, :size]
            right = jnp.concatenate([u0, u1, u0, u1, u2, u0], axis=0)
            change = product(left, right, ((0,), (0,)))
            work[last:, :] -= change[last:, :]


def bases_kernel(
    core, mine, theirs, start, right_out, left_out, image_out,
    high, low, basis, work, first, sem,
):
    copy = pltpu.make_async_copy(start, first, sem.at[0])
    copy.start()
    rank = high.shape[0]
    half = rank // 2
    for slot, part in enumerate((mine, theirs)):
        place = pl.ds(pl.multiple_of((core[0] ^ slot) * half, 128), half)
        high[:, place], low[:, place] = split2(part[...].reshape(rank, half))
    copy.wait()
    basis[...] = first[...].T
    size = basis.shape[0]
    eye = (
        lax.broadcasted_iota(jnp.int32, (size, size), 0)
        == lax.broadcasted_iota(jnp.int32, (size, size), 1)
    ).astype(F32)

    @pl.loop(0, 4)
    def _(turn):
        for parity, contract in enumerate((((1,), (0,)), ((1,), (1,)))):

            @pl.when(turn % 2 == parity)
            def _():
                bh, bl = split2(basis[...])
                small = product(bh, low[...], contract) + product(bl, high[...], contract)
                image_out[...] = product(bh, high[...], contract) + small

        held = image_out[...]
        work[:, :size] = product6(held, held, ((1,), (1,)))
        work[:, size:] = eye
        inverse_factor(work)
        basis[...] = product6(work[:, size:], held)

        @pl.when(turn == 2)
        def _():
            right_out[...] = basis[...]

    left_out[...] = basis[...]


def bases(mine, theirs, start):
    rank, size = start.shape
    shape = jax.ShapeDtypeStruct((size, rank), F32)
    vmem = pl.BlockSpec(memory_space=pltpu.VMEM)
    return pl.pallas_call(
        bases_kernel,
        in_specs=[
            pl.BlockSpec(memory_space=pltpu.SMEM),
            vmem,
            vmem,
            pl.BlockSpec(memory_space=pltpu.HBM),
        ],
        out_shape=[shape, shape, shape],
        scratch_shapes=[
            pltpu.VMEM((rank, rank), BF16),
            pltpu.VMEM((rank, rank), BF16),
            pltpu.VMEM((size, rank), F32),
            pltpu.VMEM((size, 2 * size), F32),
            pltpu.VMEM((rank, size), F32),
            pltpu.SemaphoreType.DMA((1,)),
        ],
        compiler_params=pltpu.CompilerParams(vmem_limit_bytes=16 << 20),
        cost_estimate=pl.CostEstimate(
            flops=20_000_000_000, bytes_accessed=4 << 20, transcendentals=0
        ),
        name="bases",
    )(core_index(), mine, theirs, in_hbm(start))


def finish_kernel(order, right, left, image, mine, theirs, mass, state, inputs, outputs):
    size, rank = right.shape
    blocks = (mine[...] + theirs[...]).reshape(rank, size + 128)
    turned, few = blocks[:, :size], blocks[:, size:]
    kept_col = lax.broadcasted_iota(jnp.int32, (size, size), 0) < order[0]
    kept_row = lax.broadcasted_iota(jnp.int32, (size, size), 1) < order[0]
    kept = jnp.logical_and(kept_col, kept_row).astype(F32)
    mass[...] = kept * product6(left[...], image[...], ((1,), (1,)))
    state[...] = kept * product3(right[...], turned).T
    inputs[...] = (kept_row.astype(F32) * product3(left[...], few).T)[:4]
    outputs[...] = (kept_row.astype(F32) * product3(right[...], few).T)[4:8]


def finish(order, right, left, image, mine, theirs):
    size, _ = right.shape
    vmem = pl.BlockSpec(memory_space=pltpu.VMEM)
    return pl.pallas_call(
        finish_kernel,
        in_specs=[pl.BlockSpec(memory_space=pltpu.SMEM)] + [vmem] * 5,
        out_specs=[vmem] * 4,
        out_shape=[
            jax.ShapeDtypeStruct((size, size), F32),
            jax.ShapeDtypeStruct((size, size), F32),
            jax.ShapeDtypeStruct((4, size), F32),
            jax.ShapeDtypeStruct((4, size), F32),
        ],
        compiler_params=pltpu.CompilerParams(vmem_limit_bytes=16 << 20),
        cost_estimate=pl.CostEstimate(
            flops=1_000_000_000, bytes_accessed=4 << 20, transcendentals=0
        ),
        name="finish",
    )(order, right, left, image, mine, theirs)


def from_neighbours(low_face, high_face, axis):
    count = lax.axis_size(axis)
    up = [(i, i + 1) for i in range(count - 1)]
    down = [(b, a) for a, b in up]
    return lax.ppermute(high_face, axis, up), lax.ppermute(low_face, axis, down)


def reduced(factor_obs, factor_ctrl, diffusivity, input_map, output_map, start_block, order):
    planes, lines, points, rank = factor_ctrl.shape
    halves = (2 * planes, lines * points // 2, rank)
    observe = factor_obs.reshape(halves)
    own, other, few_ctrl, zlow, zhigh, ylow, yhigh, inner, extra = local_products(
        observe, factor_ctrl.reshape(halves), output_map, diffusivity, input_map, points
    )
    arrived = scattered(own, other)
    zlow, zhigh = from_neighbours(zlow, zhigh, ("chip", "core"))
    ylow, yhigh = from_neighbours(ylow, yhigh, "sub")
    gram = gathered(summed_copies(arrived))
    faces = (zlow, zhigh, ylow, yhigh)
    oper = with_outer(observe, faces, diffusivity, inner, extra, few_ctrl, points)
    tiles = oper.reshape(-1, *oper.shape[2:])
    oper = lax.all_to_all(tiles, CHIPS + ("core",), 0, 0, tiled=True)
    right, left, image = bases(*gram, start_block)
    blocks = gathered(projected_copies(oper, left))
    mass, state, inputs, outputs = finish(order, right, left, image, *blocks)
    return mass, state, inputs.T, outputs


def solution(mesh):
    slab = mesh.shape["slab"]
    torus = Mesh(
        mesh.devices.reshape(slab // 2, 2, mesh.shape["sub"]), ("chip", "core", "sub")
    )
    slabs = ("chip", "core")
    placed = (
        P(slabs, "sub", None, None),
        P(slabs, "sub", None, None),
        P(slabs, "sub"),
        P(None, slabs, "sub"),
        P(None, slabs, "sub"),
        P(),
        P(),
    )
    return jax.shard_map(
        reduced, mesh=torus, in_specs=placed, out_specs=(P(), P(), P(), P()), check_vma=False
    )
```

```python
import functools

import jax
import jax.numpy as jnp
from jax import lax
from jax.experimental import pallas as pl
from jax.experimental.pallas import tpu as pltpu
from jax.sharding import Mesh
from jax.sharding import PartitionSpec as P


CHIPS = ("chip", "sub")
F32 = jnp.float32
BF16 = jnp.bfloat16
PANEL = 32
AHEAD = 2


def split2(x):
    high = x.astype(BF16)
    return high, (x - high.astype(F32)).astype(BF16)


def split3(x):
    high = x.astype(BF16)
    rest = x - high.astype(F32)
    mid = rest.astype(BF16)
    return high, mid, (rest - mid.astype(F32)).astype(BF16)


def product(a, b, contract=((1,), (0,))):
    return lax.dot_general(a, b, (contract, ((), ())), preferred_element_type=F32)


def product3(a, b, contract=((1,), (0,))):
    ah, al = split2(a)
    bh, bl = split2(b)
    return product(ah, bh, contract) + (product(ah, bl, contract) + product(al, bh, contract))


def product6(a, b, contract=((1,), (0,))):
    a0, a1, a2 = split3(a)
    b0, b1, b2 = split3(b)
    dot = functools.partial(product, contract=contract)
    small = dot(a1, b1) + (dot(a0, b2) + dot(a2, b0))
    return dot(a0, b0) + ((dot(a0, b1) + dot(a1, b0)) + small)


def rows_split(rows):
    both = jnp.concatenate([rows, rows], axis=0)
    high = both.astype(BF16).astype(F32)
    place = lax.broadcasted_iota(jnp.int32, both.shape, 0)
    halves = jnp.where(place < rows.shape[0], high, both - high)
    return jnp.concatenate([halves, jnp.zeros_like(halves)], axis=0).astype(BF16)


def add_products(total, turned, right, extra=None, few=None):
    count = turned.shape[0]
    th, tl = split2(turned)
    rh, rl = split2(right)
    left = jnp.concatenate([th, tl, th], axis=1)
    if few is not None:
        bottom = jnp.concatenate([few, jnp.zeros_like(few), few], axis=1)
        left = jnp.concatenate([left, bottom], axis=0)
    result = product(left, jnp.concatenate([rh, rh, rl], axis=0))
    total[...] += result[:count]
    if few is not None:
        extra[...] += result[count:]


def plane_rows(rows, plane, first, size):
    chosen = jnp.zeros((rows.shape[0], size), F32)
    for p in range(rows.shape[1]):
        chosen = jnp.where(plane == p, rows[:, p, pl.ds(first, size)], chosen)
    return rows_split(chosen)


def half_of(total, side):
    width = total.shape[1] // 2
    return total[:, pl.ds(pl.multiple_of(side * width, 128), width)]


def core_index():
    return lax.axis_index("core").reshape(1).astype(jnp.int32)


def in_hbm(value):
    return pltpu.with_memory_space_constraint(value, pltpu.HBM)


def gram_kernel(
    core, obs, ctrl, sense,
    own, other, few_far, zlow, zhigh, ylow, yhigh,
    obs_here, ctrl_here, total, extra, sense_here, obs_sems, ctrl_sems, z_sems, low_sems, high_sems, other_sems,
):
    steps, rows, _ = obs.shape
    points = ylow.shape[1]

    def copies(i):
        return (
            pltpu.make_async_copy(obs.at[i], obs_here.at[i], obs_sems.at[i]),
            pltpu.make_async_copy(ctrl.at[i], ctrl_here.at[i], ctrl_sems.at[i]),
        )

    def z_copy(i):
        source = ctrl_here.at[i if i < 2 else steps - 4 + i]
        return pltpu.make_async_copy(source, (zlow if i < 2 else zhigh).at[i % 2], z_sems.at[i])

    def low_copy(p):
        source = ctrl_here.at[2 * p, pl.ds(0, points)]
        return pltpu.make_async_copy(source, ylow.at[p], low_sems.at[p])

    def high_copy(p):
        source = ctrl_here.at[2 * p + 1, pl.ds(rows - points, points)]
        return pltpu.make_async_copy(source, yhigh.at[p], high_sems.at[p])

    sense_copy = pltpu.make_async_copy(sense, sense_here, other_sems.at[0])
    for i in range(AHEAD):
        for copy in copies(i):
            copy.start()
        if i == 0:
            sense_copy.start()
    total[...] = jnp.zeros_like(total)
    extra[...] = jnp.zeros_like(extra)
    sense_copy.wait()

    @pl.loop(0, steps)
    def _(i):
        for copy in copies(i):
            copy.wait()

        @pl.when(i + AHEAD < steps)
        def _():
            for copy in copies(i + AHEAD):
                copy.start()

        for j in range(4):

            @pl.when(i == (j if j < 2 else steps - 4 + j))
            def _():
                z_copy(j).start()

        @pl.when(i % 2 == 0)
        def _():
            low_copy(i // 2).start()

        @pl.when(i % 2 == 1)
        def _():
            high_copy(i // 2).start()

        first = pl.multiple_of((i % 2) * rows, 128)
        some = plane_rows(sense_here, i // 2, first, rows)
        add_products(total, obs_here[i].T, ctrl_here[i], extra, some)

    few_copy = pltpu.make_async_copy(extra, few_far, other_sems.at[0])
    few_copy.start()
    for slot, out in enumerate((own, other)):
        out[...] = half_of(total, core[0] ^ slot).reshape(out.shape)
    few_copy.wait()
    for i in range(4):
        z_copy(i).wait()
    for p in range(steps // 2):
        low_copy(p).wait()
        high_copy(p).wait()


def local_gram(observe, control, sense, points):
    steps, rows, rank = observe.shape
    anywhere = pl.BlockSpec(memory_space=pltpu.HBM)
    vmem = pl.BlockSpec(memory_space=pltpu.VMEM)
    face = pltpu.HBM((2, rows, rank), F32)
    edge = pltpu.HBM((steps // 2, points, rank), F32)
    return pl.pallas_call(
        gram_kernel,
        in_specs=[pl.BlockSpec(memory_space=pltpu.SMEM)] + [anywhere] * 3,
        out_specs=[vmem] * 2 + [anywhere] * 5,
        out_shape=[
            jax.ShapeDtypeStruct((rank // 8, 8, rank // 2), F32),
            jax.ShapeDtypeStruct((rank // 8, 8, rank // 2), F32),
            pltpu.HBM((16, rank), F32),
            face,
            face,
            edge,
            edge,
        ],
        scratch_shapes=[
            pltpu.VMEM((steps, rows, rank), F32),
            pltpu.VMEM((steps, rows, rank), F32),
            pltpu.VMEM((rank, rank), F32),
            pltpu.VMEM((16, rank), F32),
            pltpu.VMEM(sense.shape, F32),
            pltpu.SemaphoreType.DMA((steps,)),
            pltpu.SemaphoreType.DMA((steps,)),
            pltpu.SemaphoreType.DMA((4,)),
            pltpu.SemaphoreType.DMA((steps // 2,)),
            pltpu.SemaphoreType.DMA((steps // 2,)),
            pltpu.SemaphoreType.DMA((1,)),
        ],
        compiler_params=pltpu.CompilerParams(vmem_limit_bytes=36 << 20),
        cost_estimate=pl.CostEstimate(
            flops=6 * steps * rows * rank * rank, bytes_accessed=24 << 20, transcendentals=0
        ),
        name="local_gram",
    )(core_index(), in_hbm(observe), in_hbm(control), in_hbm(sense))


def inner_kernel(
    points, obs_far, ctrl_far, conduct, drive,
    total_far, extra_far, total, extra, obs, ctrl, conduct_here, drive_here, sems, obs_sems, ctrl_sems,
):
    steps, rows, rank = ctrl.shape
    small = [
        pltpu.make_async_copy(conduct, conduct_here, sems.at[0]),
        pltpu.make_async_copy(drive, drive_here, sems.at[1]),
    ]

    def ctrl_copy(i):
        return pltpu.make_async_copy(ctrl_far.at[i], ctrl.at[i], ctrl_sems.at[i])

    def obs_copy(i):
        return pltpu.make_async_copy(obs_far.at[i], obs.at[i], obs_sems.at[i])

    for i in (0, 1, 2):
        ctrl_copy(i).start()
    obs_copy(0).start()
    for copy in small:
        copy.start()
    ctrl_copy(3).start()
    obs_copy(1).start()
    total[...] = jnp.zeros_like(total)
    extra[...] = jnp.zeros_like(extra)
    for copy in small:
        copy.wait()
    ctrl_copy(0).wait()
    ctrl_copy(1).wait()

    @pl.loop(0, steps)
    def _(i):
        @pl.when(i + 2 < steps)
        def _():
            ctrl_copy(i + 2).wait()
            obs_copy(i + 2).start()

        @pl.when(i + 4 < steps)
        def _():
            ctrl_copy(i + 4).start()

        obs_copy(i).wait()
        half = i % 2
        center = ctrl[i]
        beside = (i + 2 < steps).astype(F32) * ctrl[jnp.minimum(i + 2, steps - 1)]
        beside = beside + (i >= 2).astype(F32) * ctrl[jnp.maximum(i - 2, 0)]
        before = half.astype(F32) * ctrl[jnp.maximum(i - 1, 0), rows - points :]
        after = (1 - half).astype(F32) * ctrl[jnp.minimum(i + 1, steps - 1), :points]
        beside = beside + jnp.concatenate([before, center[: rows - points]], axis=0)
        beside = beside + jnp.concatenate([center[points:], after], axis=0)
        place = lax.broadcasted_iota(jnp.int32, (rows, rank), 0) % points
        beside = beside + jnp.where(place > 0, pltpu.roll(center, 1, 0), 0.0)
        beside = beside + jnp.where(place < points - 1, pltpu.roll(center, rows - 1, 0), 0.0)
        first = pl.multiple_of(half * rows, 128)
        scale = conduct_here[pl.ds(i // 2, 1), pl.ds(first, rows)] * (1.0 / 6.0)
        applied = (beside - 6.0 * center).T * scale
        some = plane_rows(drive_here, i // 2, first, rows)
        add_products(total, applied, obs[i], extra, some)

    results = [
        pltpu.make_async_copy(total, total_far, sems.at[0]),
        pltpu.make_async_copy(extra, extra_far, sems.at[1]),
    ]
    for copy in results:
        copy.start()
    for copy in results:
        copy.wait()


def inner_operator(observe, control, conduct, drive, points):
    steps, rows, rank = control.shape
    anywhere = pl.BlockSpec(memory_space=pltpu.HBM)
    return pl.pallas_call(
        functools.partial(inner_kernel, points),
        in_specs=[anywhere] * 4,
        out_specs=[anywhere] * 2,
        out_shape=[
            pltpu.HBM((rank, rank), F32),
            pltpu.HBM((16, rank), F32),
        ],
        scratch_shapes=[
            pltpu.VMEM((rank, rank), F32),
            pltpu.VMEM((16, rank), F32),
            pltpu.VMEM((steps, rows, rank), F32),
            pltpu.VMEM((steps, rows, rank), F32),
            pltpu.VMEM(conduct.shape, F32),
            pltpu.VMEM(drive.shape, F32),
            pltpu.SemaphoreType.DMA((2,)),
            pltpu.SemaphoreType.DMA((steps,)),
            pltpu.SemaphoreType.DMA((steps,)),
        ],
        compiler_params=pltpu.CompilerParams(vmem_limit_bytes=36 << 20),
        cost_estimate=pl.CostEstimate(
            flops=6 * steps * rows * rank * rank, bytes_accessed=18 << 20, transcendentals=0
        ),
        name="inner_operator",
    )(in_hbm(observe), in_hbm(control), in_hbm(conduct), in_hbm(drive))


def outer_kernel(
    points, obs, zlow, zhigh, ylow, yhigh, conduct, inner, extra_far, few_far,
    out, z_field, y_field, z_obs, y_obs, conduct_here, total, extra, few_ctrl, sems, obs_sems,
):
    steps, rows, rank = obs.shape
    planes = steps // 2
    conduct_copy = pltpu.make_async_copy(conduct, conduct_here, sems.at[0])
    inner_copy = pltpu.make_async_copy(inner, total, sems.at[7])
    few_copies = [
        pltpu.make_async_copy(extra_far, extra, sems.at[8]),
        pltpu.make_async_copy(few_far, few_ctrl, sems.at[9]),
    ]
    y_near = [
        pltpu.make_async_copy(
            obs.at[2 * p + i, pl.ds(i * (rows - points), points)],
            y_obs.at[pl.ds((planes * i + p) * points, points)],
            obs_sems.at[4 + planes * i + p],
        )
        for i in range(2)
        for p in range(planes)
    ]
    y_copies = [
        pltpu.make_async_copy(ylow, y_field.at[0], sems.at[1]),
        pltpu.make_async_copy(yhigh, y_field.at[1], sems.at[2]),
    ]

    def z_far(i):
        face = zlow if i < 2 else zhigh
        return pltpu.make_async_copy(face.at[i % 2], z_field.at[i], sems.at[3 + i])

    def z_near(i):
        place = i if i < 2 else steps - 4 + i
        return pltpu.make_async_copy(obs.at[place], z_obs.at[i], obs_sems.at[i])

    conduct_copy.start()
    for copy in y_copies + y_near + [inner_copy]:
        copy.start()
    for i in range(4):
        z_far(i).start()
        z_near(i).start()
    for copy in few_copies:
        copy.start()
    conduct_copy.wait()
    scale = conduct_here[...] * (1.0 / 6.0)
    for copy in y_copies + y_near + [inner_copy]:
        copy.wait()
    turned = [
        y_field[i, p].T * scale[p : p + 1, i * (2 * rows - points) :][:, :points]
        for i in range(2)
        for p in range(planes)
    ]
    add_products(total, jnp.concatenate(turned, axis=1), y_obs[...])

    @pl.loop(0, 4)
    def _(block):
        for i in range(4):

            @pl.when(block == i)
            def _():
                z_far(i).wait()
                z_near(i).wait()

        plane = (planes - 1) * (block // 2)
        first = pl.multiple_of((block % 2) * rows, 128)
        lanes = conduct_here[pl.ds(plane, 1), pl.ds(first, rows)] * (1.0 / 6.0)
        add_products(total, z_field[block].T * lanes, z_obs[block])

    for copy in few_copies:
        copy.wait()
    summed = jnp.concatenate([extra[0:4] + extra[4:8], few_ctrl[0:4] + few_ctrl[4:8]], axis=0)
    wide = jnp.concatenate([summed, jnp.zeros((120, rank), F32)], axis=0).T
    width = rank // 2
    for side in range(2):
        cols = total[:, side * width : (side + 1) * width]
        out[:, side, :, :width] = cols.reshape(out.shape[0], out.shape[2], width)
    out[:, 0, :, width:] = wide.reshape(out.shape[0], out.shape[2], 128)
    out[:, 1, :, width:] = jnp.zeros((out.shape[0], out.shape[2], 128), F32)


def with_outer(observe, faces, conduct, inner, extra, few_ctrl, points):
    steps, rows, rank = observe.shape
    anywhere = pl.BlockSpec(memory_space=pltpu.HBM)
    vmem = pl.BlockSpec(memory_space=pltpu.VMEM)
    return pl.pallas_call(
        functools.partial(outer_kernel, points),
        in_specs=[anywhere] * 9,
        out_specs=vmem,
        out_shape=jax.ShapeDtypeStruct((rank // 8, 2, 8, rank // 2 + 128), F32),
        scratch_shapes=[
            pltpu.VMEM((4, rows, rank), F32),
            pltpu.VMEM((2, steps // 2, points, rank), F32),
            pltpu.VMEM((4, rows, rank), F32),
            pltpu.VMEM((steps * points, rank), F32),
            pltpu.VMEM(conduct.shape, F32),
            pltpu.VMEM((rank, rank), F32),
            pltpu.VMEM(extra.shape, F32),
            pltpu.VMEM(few_ctrl.shape, F32),
            pltpu.SemaphoreType.DMA((10,)),
            pltpu.SemaphoreType.DMA((4 + steps,)),
        ],
        compiler_params=pltpu.CompilerParams(vmem_limit_bytes=36 << 20),
        cost_estimate=pl.CostEstimate(
            flops=30 * rows * rank * rank, bytes_accessed=7 << 20, transcendentals=0
        ),
        name="outer_operator",
    )(*map(in_hbm, (observe, *faces, conduct, inner, extra, few_ctrl)))


def sum_kernel(parts, out):
    whole = jnp.sum(parts[...], axis=0, keepdims=True)
    out[...] = jnp.broadcast_to(whole, out.shape)


def swapped(value):
    return lax.ppermute(value, "core", [(0, 1), (1, 0)])


def add_kernel(first, second, out):
    out[...] = first[...] + second[...]


def scattered(own, other):
    other = swapped(other)
    both = pl.pallas_call(
        add_kernel,
        out_shape=jax.ShapeDtypeStruct(own.shape, F32),
        compiler_params=pltpu.CompilerParams(vmem_limit_bytes=6 << 20),
        cost_estimate=pl.CostEstimate(
            flops=own.size, bytes_accessed=12 * own.size, transcendentals=0
        ),
    )(own, other)
    return lax.all_to_all(both, CHIPS, 0, 0, tiled=True)


def summed_copies(arrived):
    return pl.pallas_call(
        sum_kernel,
        out_shape=jax.ShapeDtypeStruct(arrived.shape, F32),
        compiler_params=pltpu.CompilerParams(vmem_limit_bytes=6 << 20),
        cost_estimate=pl.CostEstimate(
            flops=arrived.size, bytes_accessed=8 * arrived.size, transcendentals=0
        ),
        name="sum_gram",
    )(arrived)


def project_kernel(side, parts, left, out):
    block = jnp.sum(parts[...], axis=0)
    half = left.shape[1] // 2
    mine = jnp.where(side[0] == 0, left[:, :half], left[:, half:])
    turned = product3(block[:, :half], mine, ((1,), (1,)))
    whole = jnp.concatenate([turned, block[:, half:]], axis=1)
    out[...] = jnp.broadcast_to(whole[None], out.shape)


def projected_copies(arrived, left):
    vmem = pl.BlockSpec(memory_space=pltpu.VMEM)
    return pl.pallas_call(
        project_kernel,
        in_specs=[pl.BlockSpec(memory_space=pltpu.SMEM), vmem, vmem],
        out_specs=vmem,
        out_shape=jax.ShapeDtypeStruct((arrived.shape[0] // 2, 8, 256), F32),
        compiler_params=pltpu.CompilerParams(vmem_limit_bytes=8 << 20),
        cost_estimate=pl.CostEstimate(
            flops=arrived.size, bytes_accessed=8 * arrived.size, transcendentals=0
        ),
        name="project",
    )(core_index(), arrived, left)


def gathered(copies):
    mine = lax.all_to_all(copies, CHIPS, 0, 0, tiled=True)
    return mine, swapped(mine)


def lane(block, index):
    where = jnp.full(block.shape, index, jnp.int32)
    return jnp.take_along_axis(block, where, axis=1, mode="promise_in_bounds")


def inverse_factor(work):
    size = work.shape[0]
    groups = PANEL // 8

    @pl.loop(0, size // PANEL)
    def _(turn):
        first = pl.multiple_of(turn * PANEL, PANEL)
        panel = [work[pl.ds(first + 8 * g, 8), :] for g in range(groups)]
        columns = {}
        for k in range(PANEL):
            for g in range(k // 8, groups):
                columns[k, g] = lane(panel[g][:, :128], first + k)
        place = lax.broadcasted_iota(jnp.int32, (8, 128), 0)
        wide_place = lax.broadcasted_iota(jnp.int32, (8, 256), 0)
        for j in range(PANEL):
            gj, sj = divmod(j, 8)
            pivot = jnp.broadcast_to(columns[j, gj][sj : sj + 1], (8, 128))
            scale = lax.rsqrt(pivot)
            lower = {g: columns[j, g] * scale for g in range(gj, groups)}
            row = jnp.broadcast_to(panel[gj][sj : sj + 1], (8, 256))
            row = row * jnp.concatenate([scale, scale], axis=1)
            for k in range(j + 1, PANEL):
                gk, sk = divmod(k, 8)
                across = jnp.broadcast_to(lower[gk][sk : sk + 1], (8, 128))
                for g in range(gk, groups):
                    columns[k, g] = columns[k, g] - lower[g] * across
            for g in range(gj, groups):
                weight = lower[g]
                if g == gj:
                    weight = jnp.where(place > sj, weight, 0.0)
                wide = jnp.concatenate([weight, weight], axis=1)
                panel[g] = panel[g] - wide * row
            panel[gj] = jnp.where(wide_place == sj, row, panel[gj])
        for g in range(groups):
            work[pl.ds(first + 8 * g, 8), :] = panel[g]

        @pl.when(turn + 1 < size // PANEL)
        def _():
            done = jnp.concatenate(panel, axis=0)
            u0, u1, u2 = split3(done)
            left = jnp.concatenate([u0, u0, u1, u1, u0, u2], axis=0)[:, :size]
            right = jnp.concatenate([u0, u1, u0, u1, u2, u0], axis=0)
            change = product(left, right, ((0,), (0,)))
            below = lax.broadcasted_iota(jnp.int32, change.shape, 0) >= first + PANEL
            work[...] -= jnp.where(below, change, 0.0)


def bases_kernel(core, mine, theirs, start, right_out, left_out, image_out, high, low, basis, work):
    rank = high.shape[0]
    half = rank // 2
    for slot, part in enumerate((mine, theirs)):
        place = pl.ds(pl.multiple_of((core[0] ^ slot) * half, 128), half)
        high[:, place], low[:, place] = split2(part[...].reshape(rank, half))
    basis[...] = start[...].T
    size = basis.shape[0]
    eye = (
        lax.broadcasted_iota(jnp.int32, (size, size), 0)
        == lax.broadcasted_iota(jnp.int32, (size, size), 1)
    ).astype(F32)

    @pl.loop(0, 4)
    def _(turn):
        for parity, contract in enumerate((((1,), (0,)), ((1,), (1,)))):

            @pl.when(turn % 2 == parity)
            def _():
                bh, bl = split2(basis[...])
                small = product(bh, low[...], contract) + product(bl, high[...], contract)
                image_out[...] = product(bh, high[...], contract) + small

        held = image_out[...]
        work[:, :size] = product6(held, held, ((1,), (1,)))
        work[:, size:] = eye
        inverse_factor(work)
        basis[...] = product6(work[:, size:], held)

        @pl.when(turn == 2)
        def _():
            right_out[...] = basis[...]

    left_out[...] = basis[...]


def bases(mine, theirs, start):
    rank, size = start.shape
    shape = jax.ShapeDtypeStruct((size, rank), F32)
    vmem = pl.BlockSpec(memory_space=pltpu.VMEM)
    return pl.pallas_call(
        bases_kernel,
        in_specs=[pl.BlockSpec(memory_space=pltpu.SMEM)] + [vmem] * 3,
        out_shape=[shape, shape, shape],
        scratch_shapes=[
            pltpu.VMEM((rank, rank), BF16),
            pltpu.VMEM((rank, rank), BF16),
            pltpu.VMEM((size, rank), F32),
            pltpu.VMEM((size, 2 * size), F32),
        ],
        compiler_params=pltpu.CompilerParams(vmem_limit_bytes=16 << 20),
        cost_estimate=pl.CostEstimate(
            flops=20_000_000_000, bytes_accessed=4 << 20, transcendentals=0
        ),
        name="bases",
    )(core_index(), mine, theirs, start)


def finish_kernel(order, right, left, image, mine, theirs, mass, state, inputs, outputs):
    size, rank = right.shape
    blocks = (mine[...] + theirs[...]).reshape(rank, size + 128)
    turned, few = blocks[:, :size], blocks[:, size:]
    kept_col = lax.broadcasted_iota(jnp.int32, (size, size), 0) < order[0]
    kept_row = lax.broadcasted_iota(jnp.int32, (size, size), 1) < order[0]
    kept = jnp.logical_and(kept_col, kept_row).astype(F32)
    mass[...] = kept * product6(left[...], image[...], ((1,), (1,)))
    state[...] = kept * product3(right[...], turned).T
    inputs[...] = (kept_row.astype(F32) * product3(left[...], few).T)[:4]
    outputs[...] = (kept_row.astype(F32) * product3(right[...], few).T)[4:8]


def finish(order, right, left, image, mine, theirs):
    size, _ = right.shape
    vmem = pl.BlockSpec(memory_space=pltpu.VMEM)
    return pl.pallas_call(
        finish_kernel,
        in_specs=[pl.BlockSpec(memory_space=pltpu.SMEM)] + [vmem] * 5,
        out_specs=[vmem] * 4,
        out_shape=[
            jax.ShapeDtypeStruct((size, size), F32),
            jax.ShapeDtypeStruct((size, size), F32),
            jax.ShapeDtypeStruct((4, size), F32),
            jax.ShapeDtypeStruct((4, size), F32),
        ],
        compiler_params=pltpu.CompilerParams(vmem_limit_bytes=16 << 20),
        cost_estimate=pl.CostEstimate(
            flops=1_000_000_000, bytes_accessed=4 << 20, transcendentals=0
        ),
        name="finish",
    )(order, right, left, image, mine, theirs)


def from_neighbours(low_face, high_face, axis):
    count = lax.axis_size(axis)
    up = [(i, i + 1) for i in range(count - 1)]
    down = [(b, a) for a, b in up]
    return lax.ppermute(high_face, axis, up), lax.ppermute(low_face, axis, down)


def reduced(factor_obs, factor_ctrl, diffusivity, input_map, output_map, start_block, order):
    planes, lines, points, rank = factor_ctrl.shape
    halves = (2 * planes, lines * points // 2, rank)
    observe = factor_obs.reshape(halves)
    control = factor_ctrl.reshape(halves)
    own, other, few_ctrl, zlow, zhigh, ylow, yhigh = local_gram(
        observe, control, output_map, points
    )
    arrived = scattered(own, other)
    zlow, zhigh = from_neighbours(zlow, zhigh, ("chip", "core"))
    ylow, yhigh = from_neighbours(ylow, yhigh, "sub")
    inner, extra = inner_operator(observe, control, diffusivity, input_map, points)
    gram = gathered(summed_copies(arrived))
    faces = (zlow, zhigh, ylow, yhigh)
    oper = with_outer(observe, faces, diffusivity, inner, extra, few_ctrl, points)
    tiles = oper.reshape(-1, *oper.shape[2:])
    oper = lax.all_to_all(tiles, CHIPS + ("core",), 0, 0, tiled=True)
    right, left, image = bases(*gram, start_block)
    blocks = gathered(projected_copies(oper, left))
    mass, state, inputs, outputs = finish(order, right, left, image, *blocks)
    return mass, state, inputs.T, outputs


def solution(mesh):
    slab = mesh.shape["slab"]
    torus = Mesh(
        mesh.devices.reshape(slab // 2, 2, mesh.shape["sub"]), ("chip", "core", "sub")
    )
    slabs = ("chip", "core")
    placed = (
        P(slabs, "sub", None, None),
        P(slabs, "sub", None, None),
        P(slabs, "sub"),
        P(None, slabs, "sub"),
        P(None, slabs, "sub"),
        P(),
        P(),
    )
    return jax.shard_map(
        reduced, mesh=torus, in_specs=placed, out_specs=(P(), P(), P(), P()), check_vma=False
    )
```

```python
import functools

import jax
import jax.numpy as jnp
from jax import lax
from jax.experimental import pallas as pl
from jax.experimental.pallas import tpu as pltpu
from jax.sharding import Mesh
from jax.sharding import PartitionSpec as P


CHIPS = ("chip", "sub")
F32 = jnp.float32
BF16 = jnp.bfloat16
PANEL = 32
AHEAD = 2


def split2(x):
    high = x.astype(BF16)
    return high, (x - high.astype(F32)).astype(BF16)


def split3(x):
    high = x.astype(BF16)
    rest = x - high.astype(F32)
    mid = rest.astype(BF16)
    return high, mid, (rest - mid.astype(F32)).astype(BF16)


def product(a, b, contract=((1,), (0,))):
    return lax.dot_general(a, b, (contract, ((), ())), preferred_element_type=F32)


def product3(a, b, contract=((1,), (0,))):
    ah, al = split2(a)
    bh, bl = split2(b)
    return product(ah, bh, contract) + (product(ah, bl, contract) + product(al, bh, contract))


def product6(a, b, contract=((1,), (0,))):
    a0, a1, a2 = split3(a)
    b0, b1, b2 = split3(b)
    dot = functools.partial(product, contract=contract)
    small = dot(a1, b1) + (dot(a0, b2) + dot(a2, b0))
    return dot(a0, b0) + ((dot(a0, b1) + dot(a1, b0)) + small)


def rows_split(rows):
    both = jnp.concatenate([rows, rows], axis=0)
    high = both.astype(BF16).astype(F32)
    place = lax.broadcasted_iota(jnp.int32, both.shape, 0)
    halves = jnp.where(place < rows.shape[0], high, both - high)
    return jnp.concatenate([halves, jnp.zeros_like(halves)], axis=0).astype(BF16)


def add_products(total, turned, right, extra=None, few=None):
    count = turned.shape[0]
    th, tl = split2(turned)
    rh, rl = split2(right)
    left = jnp.concatenate([th, tl, th], axis=1)
    if few is not None:
        bottom = jnp.concatenate([few, jnp.zeros_like(few), few], axis=1)
        left = jnp.concatenate([left, bottom], axis=0)
    result = product(left, jnp.concatenate([rh, rh, rl], axis=0))
    total[...] += result[:count]
    if few is not None:
        extra[...] += result[count:]


def plane_rows(rows, plane, first, size):
    chosen = jnp.zeros((rows.shape[0], size), F32)
    for p in range(rows.shape[1]):
        chosen = jnp.where(plane == p, rows[:, p, pl.ds(first, size)], chosen)
    return rows_split(chosen)


def core_index():
    return lax.axis_index("core").reshape(1).astype(jnp.int32)


def in_hbm(value):
    return pltpu.with_memory_space_constraint(value, pltpu.HBM)


def gram_kernel(
    obs, ctrl, sense,
    gram, few_far, zlow, zhigh, ylow, yhigh,
    obs_here, ctrl_here, total, extra, sense_here, obs_sems, ctrl_sems, z_sems, low_sems, high_sems, other_sems,
):
    steps, rows, _ = obs.shape
    points = ylow.shape[1]

    def copies(i):
        return (
            pltpu.make_async_copy(obs.at[i], obs_here.at[i], obs_sems.at[i]),
            pltpu.make_async_copy(ctrl.at[i], ctrl_here.at[i], ctrl_sems.at[i]),
        )

    def z_copy(i):
        source = ctrl_here.at[i if i < 2 else steps - 4 + i]
        return pltpu.make_async_copy(source, (zlow if i < 2 else zhigh).at[i % 2], z_sems.at[i])

    def low_copy(p):
        source = ctrl_here.at[2 * p, pl.ds(0, points)]
        return pltpu.make_async_copy(source, ylow.at[p], low_sems.at[p])

    def high_copy(p):
        source = ctrl_here.at[2 * p + 1, pl.ds(rows - points, points)]
        return pltpu.make_async_copy(source, yhigh.at[p], high_sems.at[p])

    sense_copy = pltpu.make_async_copy(sense, sense_here, other_sems.at[0])
    for i in range(AHEAD):
        for copy in copies(i):
            copy.start()
        if i == 0:
            sense_copy.start()
    total[...] = jnp.zeros_like(total)
    extra[...] = jnp.zeros_like(extra)
    sense_copy.wait()

    @pl.loop(0, steps)
    def _(i):
        for copy in copies(i):
            copy.wait()

        @pl.when(i + AHEAD < steps)
        def _():
            for copy in copies(i + AHEAD):
                copy.start()

        for j in range(4):

            @pl.when(i == (j if j < 2 else steps - 4 + j))
            def _():
                z_copy(j).start()

        @pl.when(i % 2 == 0)
        def _():
            low_copy(i // 2).start()

        @pl.when(i % 2 == 1)
        def _():
            high_copy(i // 2).start()

        first = pl.multiple_of((i % 2) * rows, 128)
        some = plane_rows(sense_here, i // 2, first, rows)
        add_products(total, obs_here[i].T, ctrl_here[i], extra, some)

    few_copy = pltpu.make_async_copy(extra, few_far, other_sems.at[0])
    few_copy.start()
    width = total.shape[1] // 2
    for side in range(2):
        cols = total[:, side * width : (side + 1) * width]
        gram[:, side] = cols.reshape(gram.shape[0], gram.shape[2], width)
    few_copy.wait()
    for i in range(4):
        z_copy(i).wait()
    for p in range(steps // 2):
        low_copy(p).wait()
        high_copy(p).wait()


def local_gram(observe, control, sense, points):
    steps, rows, rank = observe.shape
    anywhere = pl.BlockSpec(memory_space=pltpu.HBM)
    vmem = pl.BlockSpec(memory_space=pltpu.VMEM)
    face = pltpu.HBM((2, rows, rank), F32)
    edge = pltpu.HBM((steps // 2, points, rank), F32)
    return pl.pallas_call(
        gram_kernel,
        in_specs=[anywhere] * 3,
        out_specs=[vmem] + [anywhere] * 5,
        out_shape=[
            jax.ShapeDtypeStruct((rank // 8, 2, 8, rank // 2), F32),
            pltpu.HBM((16, rank), F32),
            face,
            face,
            edge,
            edge,
        ],
        scratch_shapes=[
            pltpu.VMEM((steps, rows, rank), F32),
            pltpu.VMEM((steps, rows, rank), F32),
            pltpu.VMEM((rank, rank), F32),
            pltpu.VMEM((16, rank), F32),
            pltpu.VMEM(sense.shape, F32),
            pltpu.SemaphoreType.DMA((steps,)),
            pltpu.SemaphoreType.DMA((steps,)),
            pltpu.SemaphoreType.DMA((4,)),
            pltpu.SemaphoreType.DMA((steps // 2,)),
            pltpu.SemaphoreType.DMA((steps // 2,)),
            pltpu.SemaphoreType.DMA((1,)),
        ],
        compiler_params=pltpu.CompilerParams(vmem_limit_bytes=36 << 20),
        cost_estimate=pl.CostEstimate(
            flops=6 * steps * rows * rank * rank, bytes_accessed=24 << 20, transcendentals=0
        ),
        name="local_gram",
    )(in_hbm(observe), in_hbm(control), in_hbm(sense))


def inner_kernel(
    points, obs_far, ctrl_far, conduct, drive,
    total_far, extra_far, total, extra, obs, ctrl, conduct_here, drive_here, sems, obs_sems, ctrl_sems,
):
    steps, rows, rank = ctrl.shape
    small = [
        pltpu.make_async_copy(conduct, conduct_here, sems.at[0]),
        pltpu.make_async_copy(drive, drive_here, sems.at[1]),
    ]

    def ctrl_copy(i):
        return pltpu.make_async_copy(ctrl_far.at[i], ctrl.at[i], ctrl_sems.at[i])

    def obs_copy(i):
        return pltpu.make_async_copy(obs_far.at[i], obs.at[i], obs_sems.at[i])

    for i in (0, 1, 2):
        ctrl_copy(i).start()
    obs_copy(0).start()
    for copy in small:
        copy.start()
    ctrl_copy(3).start()
    obs_copy(1).start()
    total[...] = jnp.zeros_like(total)
    extra[...] = jnp.zeros_like(extra)
    for copy in small:
        copy.wait()
    ctrl_copy(0).wait()
    ctrl_copy(1).wait()

    @pl.loop(0, steps)
    def _(i):
        @pl.when(i + 2 < steps)
        def _():
            ctrl_copy(i + 2).wait()
            obs_copy(i + 2).start()

        @pl.when(i + 4 < steps)
        def _():
            ctrl_copy(i + 4).start()

        obs_copy(i).wait()
        half = i % 2
        center = ctrl[i]
        beside = (i + 2 < steps).astype(F32) * ctrl[jnp.minimum(i + 2, steps - 1)]
        beside = beside + (i >= 2).astype(F32) * ctrl[jnp.maximum(i - 2, 0)]
        before = half.astype(F32) * ctrl[jnp.maximum(i - 1, 0), rows - points :]
        after = (1 - half).astype(F32) * ctrl[jnp.minimum(i + 1, steps - 1), :points]
        beside = beside + jnp.concatenate([before, center[: rows - points]], axis=0)
        beside = beside + jnp.concatenate([center[points:], after], axis=0)
        place = lax.broadcasted_iota(jnp.int32, (rows, rank), 0) % points
        beside = beside + jnp.where(place > 0, pltpu.roll(center, 1, 0), 0.0)
        beside = beside + jnp.where(place < points - 1, pltpu.roll(center, rows - 1, 0), 0.0)
        first = pl.multiple_of(half * rows, 128)
        scale = conduct_here[pl.ds(i // 2, 1), pl.ds(first, rows)] * (1.0 / 6.0)
        applied = (beside - 6.0 * center).T * scale
        some = plane_rows(drive_here, i // 2, first, rows)
        add_products(total, applied, obs[i], extra, some)

    results = [
        pltpu.make_async_copy(total, total_far, sems.at[0]),
        pltpu.make_async_copy(extra, extra_far, sems.at[1]),
    ]
    for copy in results:
        copy.start()
    for copy in results:
        copy.wait()


def inner_operator(observe, control, conduct, drive, points):
    steps, rows, rank = control.shape
    anywhere = pl.BlockSpec(memory_space=pltpu.HBM)
    return pl.pallas_call(
        functools.partial(inner_kernel, points),
        in_specs=[anywhere] * 4,
        out_specs=[anywhere] * 2,
        out_shape=[
            pltpu.HBM((rank, rank), F32),
            pltpu.HBM((16, rank), F32),
        ],
        scratch_shapes=[
            pltpu.VMEM((rank, rank), F32),
            pltpu.VMEM((16, rank), F32),
            pltpu.VMEM((steps, rows, rank), F32),
            pltpu.VMEM((steps, rows, rank), F32),
            pltpu.VMEM(conduct.shape, F32),
            pltpu.VMEM(drive.shape, F32),
            pltpu.SemaphoreType.DMA((2,)),
            pltpu.SemaphoreType.DMA((steps,)),
            pltpu.SemaphoreType.DMA((steps,)),
        ],
        compiler_params=pltpu.CompilerParams(vmem_limit_bytes=36 << 20),
        cost_estimate=pl.CostEstimate(
            flops=6 * steps * rows * rank * rank, bytes_accessed=18 << 20, transcendentals=0
        ),
        name="inner_operator",
    )(in_hbm(observe), in_hbm(control), in_hbm(conduct), in_hbm(drive))


def outer_kernel(
    points, obs, zlow, zhigh, conduct, inner, extra_far, few_far, ylow, yhigh,
    out, z_field, z_obs, y_obs, conduct_here, total, extra, few_ctrl, inner_here, sems, obs_sems,
):
    steps, rows, rank = obs.shape
    planes = steps // 2
    conduct_copy = pltpu.make_async_copy(conduct, conduct_here, sems.at[0])
    inner_copy = pltpu.make_async_copy(inner, inner_here, sems.at[7])
    few_copies = [
        pltpu.make_async_copy(extra_far, extra, sems.at[8]),
        pltpu.make_async_copy(few_far, few_ctrl, sems.at[9]),
    ]
    y_near = [
        pltpu.make_async_copy(
            obs.at[2 * p + i, pl.ds(i * (rows - points), points)],
            y_obs.at[pl.ds((planes * i + p) * points, points)],
            obs_sems.at[4 + planes * i + p],
        )
        for i in range(2)
        for p in range(planes)
    ]

    def z_far(i):
        face = zlow if i < 2 else zhigh
        return pltpu.make_async_copy(face.at[i % 2], z_field.at[i], sems.at[3 + i])

    def z_near(i):
        place = i if i < 2 else steps - 4 + i
        return pltpu.make_async_copy(obs.at[place], z_obs.at[i], obs_sems.at[i])

    conduct_copy.start()
    for copy in y_near:
        copy.start()
    for i in range(4):
        z_far(i).start()
        z_near(i).start()
        if i == 1:
            inner_copy.start()
    for copy in few_copies:
        copy.start()
    conduct_copy.wait()
    scale = conduct_here[...] * (1.0 / 6.0)
    for copy in y_near:
        copy.wait()
    turned = [
        (yhigh if i else ylow)[p].T * scale[p : p + 1, i * (2 * rows - points) :][:, :points]
        for i in range(2)
        for p in range(planes)
    ]
    total[...] = jnp.zeros_like(total)
    add_products(total, jnp.concatenate(turned, axis=1), y_obs[...])

    @pl.loop(0, 4)
    def _(block):
        for i in range(4):

            @pl.when(block == i)
            def _():
                z_far(i).wait()
                z_near(i).wait()

        plane = (planes - 1) * (block // 2)
        first = pl.multiple_of((block % 2) * rows, 128)
        lanes = conduct_here[pl.ds(plane, 1), pl.ds(first, rows)] * (1.0 / 6.0)
        add_products(total, z_field[block].T * lanes, z_obs[block])

    for copy in few_copies + [inner_copy]:
        copy.wait()
    summed = jnp.concatenate([extra[0:4] + extra[4:8], few_ctrl[0:4] + few_ctrl[4:8]], axis=0)
    wide = jnp.concatenate([summed, jnp.zeros((120, rank), F32)], axis=0).T
    width = rank // 2
    for side in range(2):
        place = slice(side * width, (side + 1) * width)
        cols = total[:, place] + inner_here[:, place]
        out[:, side, :, :width] = cols.reshape(out.shape[0], out.shape[2], width)
    out[:, 0, :, width:] = wide.reshape(out.shape[0], out.shape[2], 128)
    out[:, 1, :, width:] = jnp.zeros((out.shape[0], out.shape[2], 128), F32)


def with_outer(observe, faces, conduct, inner, extra, few_ctrl, points):
    steps, rows, rank = observe.shape
    anywhere = pl.BlockSpec(memory_space=pltpu.HBM)
    vmem = pl.BlockSpec(memory_space=pltpu.VMEM)
    return pl.pallas_call(
        functools.partial(outer_kernel, points),
        in_specs=[anywhere] * 7 + [vmem] * 2,
        out_specs=vmem,
        out_shape=jax.ShapeDtypeStruct((rank // 8, 2, 8, rank // 2 + 128), F32),
        scratch_shapes=[
            pltpu.VMEM((4, rows, rank), F32),
            pltpu.VMEM((4, rows, rank), F32),
            pltpu.VMEM((steps * points, rank), F32),
            pltpu.VMEM(conduct.shape, F32),
            pltpu.VMEM((rank, rank), F32),
            pltpu.VMEM(extra.shape, F32),
            pltpu.VMEM(few_ctrl.shape, F32),
            pltpu.VMEM((rank, rank), F32),
            pltpu.SemaphoreType.DMA((10,)),
            pltpu.SemaphoreType.DMA((4 + steps,)),
        ],
        compiler_params=pltpu.CompilerParams(vmem_limit_bytes=36 << 20),
        cost_estimate=pl.CostEstimate(
            flops=30 * rows * rank * rank, bytes_accessed=7 << 20, transcendentals=0
        ),
        name="outer_operator",
    )(*map(in_hbm, (observe, *faces[:2], conduct, inner, extra, few_ctrl)), *faces[2:])


def sum_kernel(parts, out):
    whole = jnp.sum(parts[...], axis=0, keepdims=True)
    out[...] = jnp.broadcast_to(whole, out.shape)


def swapped(value):
    return lax.ppermute(value, "core", [(0, 1), (1, 0)])


def scattered(parts):
    tiles = parts.reshape(-1, *parts.shape[2:])
    return lax.all_to_all(tiles, CHIPS + ("core",), 0, 0, tiled=True)


def summed_copies(arrived):
    return pl.pallas_call(
        sum_kernel,
        out_shape=jax.ShapeDtypeStruct((arrived.shape[0] // 2, *arrived.shape[1:]), F32),
        compiler_params=pltpu.CompilerParams(vmem_limit_bytes=6 << 20),
        cost_estimate=pl.CostEstimate(
            flops=arrived.size, bytes_accessed=8 * arrived.size, transcendentals=0
        ),
        name="sum_gram",
    )(arrived)


def project_kernel(side, parts, left, out):
    block = jnp.sum(parts[...], axis=0)
    half = left.shape[1] // 2
    mine = jnp.where(side[0] == 0, left[:, :half], left[:, half:])
    turned = product3(block[:, :half], mine, ((1,), (1,)))
    whole = jnp.concatenate([turned, block[:, half:]], axis=1)
    out[...] = jnp.broadcast_to(whole[None], out.shape)


def projected_copies(arrived, left):
    vmem = pl.BlockSpec(memory_space=pltpu.VMEM)
    return pl.pallas_call(
        project_kernel,
        in_specs=[pl.BlockSpec(memory_space=pltpu.SMEM), vmem, vmem],
        out_specs=vmem,
        out_shape=jax.ShapeDtypeStruct((arrived.shape[0] // 2, 8, 256), F32),
        compiler_params=pltpu.CompilerParams(vmem_limit_bytes=8 << 20),
        cost_estimate=pl.CostEstimate(
            flops=arrived.size, bytes_accessed=8 * arrived.size, transcendentals=0
        ),
        name="project",
    )(core_index(), arrived, left)


def gathered(copies):
    mine = lax.all_to_all(copies, CHIPS, 0, 0, tiled=True)
    return mine, swapped(mine)


def lane(block, index):
    where = jnp.full(block.shape, index, jnp.int32)
    return jnp.take_along_axis(block, where, axis=1, mode="promise_in_bounds")


def inverse_factor(work):
    size = work.shape[0]
    groups = PANEL // 8

    @pl.loop(0, size // PANEL)
    def _(turn):
        first = pl.multiple_of(turn * PANEL, PANEL)
        panel = [work[pl.ds(first + 8 * g, 8), :] for g in range(groups)]
        columns = {}
        for k in range(PANEL):
            for g in range(k // 8, groups):
                columns[k, g] = lane(panel[g][:, :128], first + k)
        place = lax.broadcasted_iota(jnp.int32, (8, 128), 0)
        wide_place = lax.broadcasted_iota(jnp.int32, (8, 256), 0)
        for j in range(PANEL):
            gj, sj = divmod(j, 8)
            pivot = jnp.broadcast_to(columns[j, gj][sj : sj + 1], (8, 128))
            scale = lax.rsqrt(pivot)
            lower = {g: columns[j, g] * scale for g in range(gj, groups)}
            row = jnp.broadcast_to(panel[gj][sj : sj + 1], (8, 256))
            row = row * jnp.concatenate([scale, scale], axis=1)
            for k in range(j + 1, PANEL):
                gk, sk = divmod(k, 8)
                across = jnp.broadcast_to(lower[gk][sk : sk + 1], (8, 128))
                for g in range(gk, groups):
                    columns[k, g] = columns[k, g] - lower[g] * across
            for g in range(gj, groups):
                weight = lower[g]
                if g == gj:
                    weight = jnp.where(place > sj, weight, 0.0)
                wide = jnp.concatenate([weight, weight], axis=1)
                panel[g] = panel[g] - wide * row
            panel[gj] = jnp.where(wide_place == sj, row, panel[gj])
        for g in range(groups):
            work[pl.ds(first + 8 * g, 8), :] = panel[g]

        @pl.when(turn + 1 < size // PANEL)
        def _():
            done = jnp.concatenate(panel, axis=0)
            u0, u1, u2 = split3(done)
            left = jnp.concatenate([u0, u0, u1, u1, u0, u2], axis=0)[:, :size]
            right = jnp.concatenate([u0, u1, u0, u1, u2, u0], axis=0)
            change = product(left, right, ((0,), (0,)))
            below = lax.broadcasted_iota(jnp.int32, change.shape, 0) >= first + PANEL
            work[...] -= jnp.where(below, change, 0.0)


def bases_kernel(
    core, mine, theirs, start, right_out, left_out, image_out,
    high, low, basis, work, right, image, sems,
):
    right_copy = pltpu.make_async_copy(right, right_out, sems.at[0])
    image_copy = pltpu.make_async_copy(image, image_out, sems.at[1])
    rank = high.shape[0]
    half = rank // 2
    for slot, part in enumerate((mine, theirs)):
        place = pl.ds(pl.multiple_of((core[0] ^ slot) * half, 128), half)
        high[:, place], low[:, place] = split2(part[...].reshape(rank, half))
    basis[...] = start[...].T
    size = basis.shape[0]
    eye = (
        lax.broadcasted_iota(jnp.int32, (size, size), 0)
        == lax.broadcasted_iota(jnp.int32, (size, size), 1)
    ).astype(F32)

    @pl.loop(0, 4)
    def _(turn):
        for parity, contract in enumerate((((1,), (0,)), ((1,), (1,)))):

            @pl.when(turn % 2 == parity)
            def _():
                bh, bl = split2(basis[...])
                small = product(bh, low[...], contract) + product(bl, high[...], contract)
                image[...] = product(bh, high[...], contract) + small

        @pl.when(turn == 3)
        def _():
            image_copy.start()

        held = image[...]
        work[:, :size] = product6(held, held, ((1,), (1,)))
        work[:, size:] = eye
        inverse_factor(work)
        basis[...] = product6(work[:, size:], held)

        @pl.when(turn == 2)
        def _():
            right[...] = basis[...]
            right_copy.start()

    left_out[...] = basis[...]
    right_copy.wait()
    image_copy.wait()


def bases(mine, theirs, start):
    rank, size = start.shape
    shape = jax.ShapeDtypeStruct((size, rank), F32)
    vmem = pl.BlockSpec(memory_space=pltpu.VMEM)
    anywhere = pl.BlockSpec(memory_space=pltpu.HBM)
    return pl.pallas_call(
        bases_kernel,
        in_specs=[pl.BlockSpec(memory_space=pltpu.SMEM)] + [vmem] * 3,
        out_specs=[anywhere, vmem, anywhere],
        out_shape=[pltpu.HBM((size, rank), F32), shape, pltpu.HBM((size, rank), F32)],
        scratch_shapes=[
            pltpu.VMEM((rank, rank), BF16),
            pltpu.VMEM((rank, rank), BF16),
            pltpu.VMEM((size, rank), F32),
            pltpu.VMEM((size, 2 * size), F32),
            pltpu.VMEM((size, rank), F32),
            pltpu.VMEM((size, rank), F32),
            pltpu.SemaphoreType.DMA((2,)),
        ],
        compiler_params=pltpu.CompilerParams(vmem_limit_bytes=16 << 20),
        cost_estimate=pl.CostEstimate(
            flops=20_000_000_000, bytes_accessed=4 << 20, transcendentals=0
        ),
        name="bases",
    )(core_index(), mine, theirs, start)


def finish_kernel(order, right, left, image, mine, theirs, mass, state, inputs, outputs):
    size, rank = right.shape
    blocks = (mine[...] + theirs[...]).reshape(rank, size + 128)
    turned, few = blocks[:, :size], blocks[:, size:]
    kept_col = lax.broadcasted_iota(jnp.int32, (size, size), 0) < order[0]
    kept_row = lax.broadcasted_iota(jnp.int32, (size, size), 1) < order[0]
    kept = jnp.logical_and(kept_col, kept_row).astype(F32)
    mass[...] = kept * product6(left[...], image[...], ((1,), (1,)))
    state[...] = kept * product3(right[...], turned).T
    inputs[...] = (kept_row.astype(F32) * product3(left[...], few).T)[:4]
    outputs[...] = (kept_row.astype(F32) * product3(right[...], few).T)[4:8]


def finish(order, right, left, image, mine, theirs):
    size, _ = right.shape
    vmem = pl.BlockSpec(memory_space=pltpu.VMEM)
    return pl.pallas_call(
        finish_kernel,
        in_specs=[pl.BlockSpec(memory_space=pltpu.SMEM)] + [vmem] * 5,
        out_specs=[vmem] * 4,
        out_shape=[
            jax.ShapeDtypeStruct((size, size), F32),
            jax.ShapeDtypeStruct((size, size), F32),
            jax.ShapeDtypeStruct((4, size), F32),
            jax.ShapeDtypeStruct((4, size), F32),
        ],
        compiler_params=pltpu.CompilerParams(vmem_limit_bytes=16 << 20),
        cost_estimate=pl.CostEstimate(
            flops=1_000_000_000, bytes_accessed=4 << 20, transcendentals=0
        ),
        name="finish",
    )(order, right, left, image, mine, theirs)


def from_neighbours(low_face, high_face, axis):
    count = lax.axis_size(axis)
    up = [(i, i + 1) for i in range(count - 1)]
    down = [(b, a) for a, b in up]
    return lax.ppermute(high_face, axis, up), lax.ppermute(low_face, axis, down)


def reduced(factor_obs, factor_ctrl, diffusivity, input_map, output_map, start_block, order):
    planes, lines, points, rank = factor_ctrl.shape
    halves = (2 * planes, lines * points // 2, rank)
    observe = factor_obs.reshape(halves)
    control = factor_ctrl.reshape(halves)
    gram, few_ctrl, zlow, zhigh, ylow, yhigh = local_gram(
        observe, control, output_map, points
    )
    arrived = scattered(gram)
    zlow, zhigh = from_neighbours(zlow, zhigh, ("chip", "core"))
    ylow, yhigh = from_neighbours(ylow, yhigh, "sub")
    inner, extra = inner_operator(observe, control, diffusivity, input_map, points)
    gram = gathered(summed_copies(arrived))
    faces = (zlow, zhigh, ylow, yhigh)
    oper = with_outer(observe, faces, diffusivity, inner, extra, few_ctrl, points)
    oper = scattered(oper)
    right, left, image = bases(*gram, start_block)
    blocks = gathered(projected_copies(oper, left))
    mass, state, inputs, outputs = finish(order, right, left, image, *blocks)
    return mass, state, inputs.T, outputs


def solution(mesh):
    slab = mesh.shape["slab"]
    torus = Mesh(
        mesh.devices.reshape(slab // 2, 2, mesh.shape["sub"]), ("chip", "core", "sub")
    )
    slabs = ("chip", "core")
    placed = (
        P(slabs, "sub", None, None),
        P(slabs, "sub", None, None),
        P(slabs, "sub"),
        P(None, slabs, "sub"),
        P(None, slabs, "sub"),
        P(),
        P(),
    )
    return jax.shard_map(
        reduced, mesh=torus, in_specs=placed, out_specs=(P(), P(), P(), P()), check_vma=False
    )
```

```python
import functools

import jax
import jax.numpy as jnp
from jax import lax
from jax.experimental import pallas as pl
from jax.experimental.pallas import tpu as pltpu
from jax.sharding import Mesh
from jax.sharding import PartitionSpec as P


CHIPS = ("chip", "sub")
F32 = jnp.float32
BF16 = jnp.bfloat16
PANEL = 32
AHEAD = 2


def split2(x):
    high = x.astype(BF16)
    return high, (x - high.astype(F32)).astype(BF16)


def split3(x):
    high = x.astype(BF16)
    rest = x - high.astype(F32)
    mid = rest.astype(BF16)
    return high, mid, (rest - mid.astype(F32)).astype(BF16)


def product(a, b, contract=((1,), (0,))):
    return lax.dot_general(a, b, (contract, ((), ())), preferred_element_type=F32)


def product3(a, b, contract=((1,), (0,))):
    ah, al = split2(a)
    bh, bl = split2(b)
    return product(ah, bh, contract) + (product(ah, bl, contract) + product(al, bh, contract))


def product6(a, b, contract=((1,), (0,))):
    a0, a1, a2 = split3(a)
    b0, b1, b2 = split3(b)
    dot = functools.partial(product, contract=contract)
    small = dot(a1, b1) + (dot(a0, b2) + dot(a2, b0))
    return dot(a0, b0) + ((dot(a0, b1) + dot(a1, b0)) + small)


def rows_split(rows):
    both = jnp.concatenate([rows, rows], axis=0)
    high = both.astype(BF16).astype(F32)
    place = lax.broadcasted_iota(jnp.int32, both.shape, 0)
    halves = jnp.where(place < rows.shape[0], high, both - high)
    return jnp.concatenate([halves, jnp.zeros_like(halves)], axis=0).astype(BF16)


def add_products(total, turned, right, extra=None, few=None):
    count = turned.shape[0]
    th, tl = split2(turned)
    rh, rl = split2(right)
    left = jnp.concatenate([th, tl, th], axis=1)
    if few is not None:
        bottom = jnp.concatenate([few, jnp.zeros_like(few), few], axis=1)
        left = jnp.concatenate([left, bottom], axis=0)
    result = product(left, jnp.concatenate([rh, rh, rl], axis=0))
    total[...] += result[:count]
    if few is not None:
        extra[...] += result[count:]


def plane_rows(rows, plane, first, size):
    chosen = jnp.zeros((rows.shape[0], size), F32)
    for p in range(rows.shape[1]):
        chosen = jnp.where(plane == p, rows[:, p, pl.ds(first, size)], chosen)
    return rows_split(chosen)


def core_index():
    return lax.axis_index("core").reshape(1).astype(jnp.int32)


def in_hbm(value):
    return pltpu.with_memory_space_constraint(value, pltpu.HBM)


def gram_kernel(
    obs, ctrl, sense,
    gram, few_far, zlow, zhigh, ylow, yhigh,
    obs_here, ctrl_here, total, extra, sense_here, obs_sems, ctrl_sems, z_sems, low_sems, high_sems, other_sems,
):
    steps, rows, _ = obs.shape
    points = ylow.shape[1]

    def copies(i):
        return (
            pltpu.make_async_copy(obs.at[i], obs_here.at[i], obs_sems.at[i]),
            pltpu.make_async_copy(ctrl.at[i], ctrl_here.at[i], ctrl_sems.at[i]),
        )

    def z_copy(i):
        source = ctrl_here.at[i if i < 2 else steps - 4 + i]
        return pltpu.make_async_copy(source, (zlow if i < 2 else zhigh).at[i % 2], z_sems.at[i])

    def low_copy(p):
        source = ctrl_here.at[2 * p, pl.ds(0, points)]
        return pltpu.make_async_copy(source, ylow.at[p], low_sems.at[p])

    def high_copy(p):
        source = ctrl_here.at[2 * p + 1, pl.ds(rows - points, points)]
        return pltpu.make_async_copy(source, yhigh.at[p], high_sems.at[p])

    sense_copy = pltpu.make_async_copy(sense, sense_here, other_sems.at[0])
    for i in range(AHEAD):
        for copy in copies(i):
            copy.start()
        if i == 0:
            sense_copy.start()
    total[...] = jnp.zeros_like(total)
    extra[...] = jnp.zeros_like(extra)
    sense_copy.wait()

    @pl.loop(0, steps)
    def _(i):
        for copy in copies(i):
            copy.wait()

        @pl.when(i + AHEAD < steps)
        def _():
            for copy in copies(i + AHEAD):
                copy.start()

        for j in range(4):

            @pl.when(i == (j if j < 2 else steps - 4 + j))
            def _():
                z_copy(j).start()

        @pl.when(i % 2 == 0)
        def _():
            low_copy(i // 2).start()

        @pl.when(i % 2 == 1)
        def _():
            high_copy(i // 2).start()

        first = pl.multiple_of((i % 2) * rows, 128)
        some = plane_rows(sense_here, i // 2, first, rows)
        add_products(total, obs_here[i].T, ctrl_here[i], extra, some)

    few_copy = pltpu.make_async_copy(extra, few_far, other_sems.at[0])
    few_copy.start()
    width = total.shape[1] // 2
    for side in range(2):
        cols = total[:, side * width : (side + 1) * width]
        gram[:, side] = cols.reshape(gram.shape[0], gram.shape[2], width)
    few_copy.wait()
    for i in range(4):
        z_copy(i).wait()
    for p in range(steps // 2):
        low_copy(p).wait()
        high_copy(p).wait()


def local_gram(observe, control, sense, points):
    steps, rows, rank = observe.shape
    anywhere = pl.BlockSpec(memory_space=pltpu.HBM)
    vmem = pl.BlockSpec(memory_space=pltpu.VMEM)
    face = pltpu.HBM((2, rows, rank), F32)
    edge = pltpu.HBM((steps // 2, points, rank), F32)
    return pl.pallas_call(
        gram_kernel,
        in_specs=[anywhere] * 3,
        out_specs=[vmem] + [anywhere] * 5,
        out_shape=[
            jax.ShapeDtypeStruct((rank // 8, 2, 8, rank // 2), F32),
            pltpu.HBM((16, rank), F32),
            face,
            face,
            edge,
            edge,
        ],
        scratch_shapes=[
            pltpu.VMEM((steps, rows, rank), F32),
            pltpu.VMEM((steps, rows, rank), F32),
            pltpu.VMEM((rank, rank), F32),
            pltpu.VMEM((16, rank), F32),
            pltpu.VMEM(sense.shape, F32),
            pltpu.SemaphoreType.DMA((steps,)),
            pltpu.SemaphoreType.DMA((steps,)),
            pltpu.SemaphoreType.DMA((4,)),
            pltpu.SemaphoreType.DMA((steps // 2,)),
            pltpu.SemaphoreType.DMA((steps // 2,)),
            pltpu.SemaphoreType.DMA((1,)),
        ],
        compiler_params=pltpu.CompilerParams(vmem_limit_bytes=36 << 20),
        cost_estimate=pl.CostEstimate(
            flops=6 * steps * rows * rank * rank, bytes_accessed=24 << 20, transcendentals=0
        ),
        name="local_gram",
    )(in_hbm(observe), in_hbm(control), in_hbm(sense))


def inner_kernel(
    points, obs_far, ctrl_far, conduct, drive,
    total_far, extra_far, total, extra, obs, ctrl, conduct_here, drive_here, sems, obs_sems, ctrl_sems,
):
    steps, rows, rank = ctrl.shape
    small = [
        pltpu.make_async_copy(conduct, conduct_here, sems.at[0]),
        pltpu.make_async_copy(drive, drive_here, sems.at[1]),
    ]

    def ctrl_copy(i):
        return pltpu.make_async_copy(ctrl_far.at[i], ctrl.at[i], ctrl_sems.at[i])

    def obs_copy(i):
        return pltpu.make_async_copy(obs_far.at[i], obs.at[i], obs_sems.at[i])

    for i in (0, 1, 2):
        ctrl_copy(i).start()
    obs_copy(0).start()
    for copy in small:
        copy.start()
    ctrl_copy(3).start()
    obs_copy(1).start()
    total[...] = jnp.zeros_like(total)
    extra[...] = jnp.zeros_like(extra)
    for copy in small:
        copy.wait()
    ctrl_copy(0).wait()
    ctrl_copy(1).wait()

    @pl.loop(0, steps)
    def _(i):
        @pl.when(i + 2 < steps)
        def _():
            ctrl_copy(i + 2).wait()
            obs_copy(i + 2).start()

        @pl.when(i + 4 < steps)
        def _():
            ctrl_copy(i + 4).start()

        obs_copy(i).wait()
        half = i % 2
        center = ctrl[i]
        beside = (i + 2 < steps).astype(F32) * ctrl[jnp.minimum(i + 2, steps - 1)]
        beside = beside + (i >= 2).astype(F32) * ctrl[jnp.maximum(i - 2, 0)]
        before = half.astype(F32) * ctrl[jnp.maximum(i - 1, 0), rows - points :]
        after = (1 - half).astype(F32) * ctrl[jnp.minimum(i + 1, steps - 1), :points]
        beside = beside + jnp.concatenate([before, center[: rows - points]], axis=0)
        beside = beside + jnp.concatenate([center[points:], after], axis=0)
        place = lax.broadcasted_iota(jnp.int32, (rows, rank), 0) % points
        beside = beside + jnp.where(place > 0, pltpu.roll(center, 1, 0), 0.0)
        beside = beside + jnp.where(place < points - 1, pltpu.roll(center, rows - 1, 0), 0.0)
        first = pl.multiple_of(half * rows, 128)
        scale = conduct_here[pl.ds(i // 2, 1), pl.ds(first, rows)] * (1.0 / 6.0)
        applied = (beside - 6.0 * center).T * scale
        some = plane_rows(drive_here, i // 2, first, rows)
        add_products(total, applied, obs[i], extra, some)

    results = [
        pltpu.make_async_copy(total, total_far, sems.at[0]),
        pltpu.make_async_copy(extra, extra_far, sems.at[1]),
    ]
    for copy in results:
        copy.start()
    for copy in results:
        copy.wait()


def inner_operator(observe, control, conduct, drive, points):
    steps, rows, rank = control.shape
    anywhere = pl.BlockSpec(memory_space=pltpu.HBM)
    return pl.pallas_call(
        functools.partial(inner_kernel, points),
        in_specs=[anywhere] * 4,
        out_specs=[anywhere] * 2,
        out_shape=[
            pltpu.HBM((rank, rank), F32),
            pltpu.HBM((16, rank), F32),
        ],
        scratch_shapes=[
            pltpu.VMEM((rank, rank), F32),
            pltpu.VMEM((16, rank), F32),
            pltpu.VMEM((steps, rows, rank), F32),
            pltpu.VMEM((steps, rows, rank), F32),
            pltpu.VMEM(conduct.shape, F32),
            pltpu.VMEM(drive.shape, F32),
            pltpu.SemaphoreType.DMA((2,)),
            pltpu.SemaphoreType.DMA((steps,)),
            pltpu.SemaphoreType.DMA((steps,)),
        ],
        compiler_params=pltpu.CompilerParams(vmem_limit_bytes=36 << 20),
        cost_estimate=pl.CostEstimate(
            flops=6 * steps * rows * rank * rank, bytes_accessed=18 << 20, transcendentals=0
        ),
        name="inner_operator",
    )(in_hbm(observe), in_hbm(control), in_hbm(conduct), in_hbm(drive))


def outer_kernel(
    points, obs, zlow, zhigh, conduct, inner, ylow, yhigh,
    out, z_field, z_obs, y_obs, conduct_here, total, inner_here, sems, obs_sems,
):
    steps, rows, rank = obs.shape
    planes = steps // 2
    conduct_copy = pltpu.make_async_copy(conduct, conduct_here, sems.at[0])
    inner_copy = pltpu.make_async_copy(inner, inner_here, sems.at[7])
    y_near = [
        pltpu.make_async_copy(
            obs.at[2 * p + i, pl.ds(i * (rows - points), points)],
            y_obs.at[pl.ds((planes * i + p) * points, points)],
            obs_sems.at[4 + planes * i + p],
        )
        for i in range(2)
        for p in range(planes)
    ]

    def z_far(i):
        face = zlow if i < 2 else zhigh
        return pltpu.make_async_copy(face.at[i % 2], z_field.at[i], sems.at[3 + i])

    def z_near(i):
        place = i if i < 2 else steps - 4 + i
        return pltpu.make_async_copy(obs.at[place], z_obs.at[i], obs_sems.at[i])

    conduct_copy.start()
    for copy in y_near:
        copy.start()
    for i in range(4):
        z_far(i).start()
        z_near(i).start()
        if i == 1:
            inner_copy.start()
    conduct_copy.wait()
    scale = conduct_here[...] * (1.0 / 6.0)
    for copy in y_near:
        copy.wait()
    turned = [
        (yhigh if i else ylow)[p].T * scale[p : p + 1, i * (2 * rows - points) :][:, :points]
        for i in range(2)
        for p in range(planes)
    ]
    total[...] = jnp.zeros_like(total)
    add_products(total, jnp.concatenate(turned, axis=1), y_obs[...])

    @pl.loop(0, 4)
    def _(block):
        for i in range(4):

            @pl.when(block == i)
            def _():
                z_far(i).wait()
                z_near(i).wait()

        plane = (planes - 1) * (block // 2)
        first = pl.multiple_of((block % 2) * rows, 128)
        lanes = conduct_here[pl.ds(plane, 1), pl.ds(first, rows)] * (1.0 / 6.0)
        add_products(total, z_field[block].T * lanes, z_obs[block])

    inner_copy.wait()
    width = rank // 2
    for side in range(2):
        place = slice(side * width, (side + 1) * width)
        cols = total[:, place] + inner_here[:, place]
        out[:, side] = cols.reshape(out.shape[0], out.shape[2], width)


def with_outer(observe, faces, conduct, inner, points):
    steps, rows, rank = observe.shape
    anywhere = pl.BlockSpec(memory_space=pltpu.HBM)
    vmem = pl.BlockSpec(memory_space=pltpu.VMEM)
    return pl.pallas_call(
        functools.partial(outer_kernel, points),
        in_specs=[anywhere] * 5 + [vmem] * 2,
        out_specs=vmem,
        out_shape=jax.ShapeDtypeStruct((rank // 8, 2, 8, rank // 2), F32),
        scratch_shapes=[
            pltpu.VMEM((4, rows, rank), F32),
            pltpu.VMEM((4, rows, rank), F32),
            pltpu.VMEM((steps * points, rank), F32),
            pltpu.VMEM(conduct.shape, F32),
            pltpu.VMEM((rank, rank), F32),
            pltpu.VMEM((rank, rank), F32),
            pltpu.SemaphoreType.DMA((8,)),
            pltpu.SemaphoreType.DMA((4 + steps,)),
        ],
        compiler_params=pltpu.CompilerParams(vmem_limit_bytes=36 << 20),
        cost_estimate=pl.CostEstimate(
            flops=30 * rows * rank * rank, bytes_accessed=7 << 20, transcendentals=0
        ),
        name="outer_operator",
    )(*map(in_hbm, (observe, *faces[:2], conduct, inner)), *faces[2:])


def sum_kernel(parts, out):
    whole = jnp.sum(parts[...], axis=0, keepdims=True)
    out[...] = jnp.broadcast_to(whole, out.shape)


def swapped(value):
    return lax.ppermute(value, "core", [(0, 1), (1, 0)])


def scattered(parts):
    tiles = parts.reshape(-1, *parts.shape[2:])
    return lax.all_to_all(tiles, CHIPS + ("core",), 0, 0, tiled=True)


def summed_copies(arrived):
    return pl.pallas_call(
        sum_kernel,
        out_shape=jax.ShapeDtypeStruct((arrived.shape[0] // 2, *arrived.shape[1:]), F32),
        compiler_params=pltpu.CompilerParams(vmem_limit_bytes=6 << 20),
        cost_estimate=pl.CostEstimate(
            flops=arrived.size, bytes_accessed=8 * arrived.size, transcendentals=0
        ),
        name="sum_gram",
    )(arrived)


def project_kernel(side, parts, left, few, out):
    block = jnp.sum(parts[...], axis=0)
    half = left.shape[1] // 2
    mine = jnp.where(side[0] == 0, left[:, :half], left[:, half:])
    turned = product3(block, mine, ((1,), (1,)))
    whole = jnp.concatenate([turned, few[...]], axis=1)
    out[...] = jnp.broadcast_to(whole[None], out.shape)


def projected_copies(arrived, left, few):
    vmem = pl.BlockSpec(memory_space=pltpu.VMEM)
    return pl.pallas_call(
        project_kernel,
        in_specs=[pl.BlockSpec(memory_space=pltpu.SMEM), vmem, vmem, vmem],
        out_specs=vmem,
        out_shape=jax.ShapeDtypeStruct((arrived.shape[0] // 2, 8, 256), F32),
        compiler_params=pltpu.CompilerParams(vmem_limit_bytes=8 << 20),
        cost_estimate=pl.CostEstimate(
            flops=arrived.size, bytes_accessed=8 * arrived.size, transcendentals=0
        ),
        name="project",
    )(core_index(), arrived, left, few)


def gathered(copies):
    mine = lax.all_to_all(copies, CHIPS, 0, 0, tiled=True)
    return mine, swapped(mine)


def lane(block, index):
    where = jnp.full(block.shape, index, jnp.int32)
    return jnp.take_along_axis(block, where, axis=1, mode="promise_in_bounds")


def inverse_factor(work):
    size = work.shape[0]
    groups = PANEL // 8

    @pl.loop(0, size // PANEL)
    def _(turn):
        first = pl.multiple_of(turn * PANEL, PANEL)
        panel = [work[pl.ds(first + 8 * g, 8), :] for g in range(groups)]
        columns = {}
        for k in range(PANEL):
            for g in range(k // 8, groups):
                columns[k, g] = lane(panel[g][:, :128], first + k)
        place = lax.broadcasted_iota(jnp.int32, (8, 128), 0)
        wide_place = lax.broadcasted_iota(jnp.int32, (8, 256), 0)
        for j in range(PANEL):
            gj, sj = divmod(j, 8)
            pivot = jnp.broadcast_to(columns[j, gj][sj : sj + 1], (8, 128))
            scale = lax.rsqrt(pivot)
            lower = {g: columns[j, g] * scale for g in range(gj, groups)}
            row = jnp.broadcast_to(panel[gj][sj : sj + 1], (8, 256))
            row = row * jnp.concatenate([scale, scale], axis=1)
            for k in range(j + 1, PANEL):
                gk, sk = divmod(k, 8)
                across = jnp.broadcast_to(lower[gk][sk : sk + 1], (8, 128))
                for g in range(gk, groups):
                    columns[k, g] = columns[k, g] - lower[g] * across
            for g in range(gj, groups):
                weight = lower[g]
                if g == gj:
                    weight = jnp.where(place > sj, weight, 0.0)
                wide = jnp.concatenate([weight, weight], axis=1)
                panel[g] = panel[g] - wide * row
            panel[gj] = jnp.where(wide_place == sj, row, panel[gj])
        for g in range(groups):
            work[pl.ds(first + 8 * g, 8), :] = panel[g]

        @pl.when(turn + 1 < size // PANEL)
        def _():
            done = jnp.concatenate(panel, axis=0)
            u0, u1, u2 = split3(done)
            left = jnp.concatenate([u0, u0, u1, u1, u0, u2], axis=0)[:, :size]
            right = jnp.concatenate([u0, u1, u0, u1, u2, u0], axis=0)
            change = product(left, right, ((0,), (0,)))
            below = lax.broadcasted_iota(jnp.int32, change.shape, 0) >= first + PANEL
            work[...] -= jnp.where(below, change, 0.0)


def bases_kernel(
    core, mine, theirs, start, drive_far, sense_far,
    right_out, left_out, image_out, few_out,
    high, low, basis, work, right, image, drive, sense, sems,
):
    small = [
        pltpu.make_async_copy(drive_far, drive, sems.at[2]),
        pltpu.make_async_copy(sense_far, sense, sems.at[3]),
    ]
    for copy in small:
        copy.start()
    right_copy = pltpu.make_async_copy(right, right_out, sems.at[0])
    image_copy = pltpu.make_async_copy(image, image_out, sems.at[1])
    rank = high.shape[0]
    half = rank // 2
    for slot, part in enumerate((mine, theirs)):
        place = pl.ds(pl.multiple_of((core[0] ^ slot) * half, 128), half)
        high[:, place], low[:, place] = split2(part[...].reshape(rank, half))
    basis[...] = start[...].T
    size = basis.shape[0]
    eye = (
        lax.broadcasted_iota(jnp.int32, (size, size), 0)
        == lax.broadcasted_iota(jnp.int32, (size, size), 1)
    ).astype(F32)

    @pl.loop(0, 4)
    def _(turn):
        for parity, contract in enumerate((((1,), (0,)), ((1,), (1,)))):

            @pl.when(turn % 2 == parity)
            def _():
                bh, bl = split2(basis[...])
                small = product(bh, low[...], contract) + product(bl, high[...], contract)
                image[...] = product(bh, high[...], contract) + small

        @pl.when(turn == 3)
        def _():
            image_copy.start()

        held = image[...]
        work[:, :size] = product6(held, held, ((1,), (1,)))
        work[:, size:] = eye
        inverse_factor(work)
        basis[...] = product6(work[:, size:], held)

        @pl.when(turn == 2)
        def _():
            right[...] = basis[...]
            right_copy.start()

    left_out[...] = basis[...]
    for copy in small:
        copy.wait()
    rows = jnp.concatenate([drive[0:4] + drive[4:8], sense[0:4] + sense[4:8]], axis=0)
    both = ((1,), (1,))
    place = lax.broadcasted_iota(jnp.int32, few_out.shape, 0)
    by_left, by_right = product3(rows, basis[...], both), product3(rows, right[...], both)
    few_out[...] = jnp.where(place < 4, by_left, by_right)
    right_copy.wait()
    image_copy.wait()


def bases(mine, theirs, start, drive, sense):
    rank, size = start.shape
    shape = jax.ShapeDtypeStruct((size, rank), F32)
    vmem = pl.BlockSpec(memory_space=pltpu.VMEM)
    anywhere = pl.BlockSpec(memory_space=pltpu.HBM)
    return pl.pallas_call(
        bases_kernel,
        in_specs=[pl.BlockSpec(memory_space=pltpu.SMEM)] + [vmem] * 3 + [anywhere] * 2,
        out_specs=[anywhere, vmem, anywhere, vmem],
        out_shape=[
            pltpu.HBM((size, rank), F32),
            shape,
            pltpu.HBM((size, rank), F32),
            jax.ShapeDtypeStruct((8, size), F32),
        ],
        scratch_shapes=[
            pltpu.VMEM((rank, rank), BF16),
            pltpu.VMEM((rank, rank), BF16),
            pltpu.VMEM((size, rank), F32),
            pltpu.VMEM((size, 2 * size), F32),
            pltpu.VMEM((size, rank), F32),
            pltpu.VMEM((size, rank), F32),
            pltpu.VMEM(drive.shape, F32),
            pltpu.VMEM(sense.shape, F32),
            pltpu.SemaphoreType.DMA((4,)),
        ],
        compiler_params=pltpu.CompilerParams(vmem_limit_bytes=16 << 20),
        cost_estimate=pl.CostEstimate(
            flops=20_000_000_000, bytes_accessed=4 << 20, transcendentals=0
        ),
        name="bases",
    )(core_index(), mine, theirs, start, in_hbm(drive), in_hbm(sense))


def finish_kernel(order, right, left, image, mine, theirs, mass, state, inputs, outputs):
    size, rank = right.shape
    blocks = (mine[...] + theirs[...]).reshape(rank, 2 * size)
    turned = blocks[:, :size]
    few = jnp.sum(blocks[:, size:].reshape(rank // 8, 8, size), axis=0)
    kept_col = lax.broadcasted_iota(jnp.int32, (size, size), 0) < order[0]
    kept_row = lax.broadcasted_iota(jnp.int32, (size, size), 1) < order[0]
    kept = jnp.logical_and(kept_col, kept_row).astype(F32)
    mass[...] = kept * product6(left[...], image[...], ((1,), (1,)))
    state[...] = kept * product3(right[...], turned).T
    few = kept_row[:8].astype(F32) * few
    inputs[...] = few[:4]
    outputs[...] = few[4:]


def finish(order, right, left, image, mine, theirs):
    size, _ = right.shape
    vmem = pl.BlockSpec(memory_space=pltpu.VMEM)
    return pl.pallas_call(
        finish_kernel,
        in_specs=[pl.BlockSpec(memory_space=pltpu.SMEM)] + [vmem] * 5,
        out_specs=[vmem] * 4,
        out_shape=[
            jax.ShapeDtypeStruct((size, size), F32),
            jax.ShapeDtypeStruct((size, size), F32),
            jax.ShapeDtypeStruct((4, size), F32),
            jax.ShapeDtypeStruct((4, size), F32),
        ],
        compiler_params=pltpu.CompilerParams(vmem_limit_bytes=16 << 20),
        cost_estimate=pl.CostEstimate(
            flops=1_000_000_000, bytes_accessed=4 << 20, transcendentals=0
        ),
        name="finish",
    )(order, right, left, image, mine, theirs)


def from_neighbours(low_face, high_face, axis):
    count = lax.axis_size(axis)
    up = [(i, i + 1) for i in range(count - 1)]
    down = [(b, a) for a, b in up]
    return lax.ppermute(high_face, axis, up), lax.ppermute(low_face, axis, down)


def reduced(factor_obs, factor_ctrl, diffusivity, input_map, output_map, start_block, order):
    planes, lines, points, rank = factor_ctrl.shape
    halves = (2 * planes, lines * points // 2, rank)
    observe = factor_obs.reshape(halves)
    control = factor_ctrl.reshape(halves)
    gram, few_ctrl, zlow, zhigh, ylow, yhigh = local_gram(
        observe, control, output_map, points
    )
    arrived = scattered(gram)
    zlow, zhigh = from_neighbours(zlow, zhigh, ("chip", "core"))
    ylow, yhigh = from_neighbours(ylow, yhigh, "sub")
    inner, extra = inner_operator(observe, control, diffusivity, input_map, points)
    gram = gathered(summed_copies(arrived))
    faces = (zlow, zhigh, ylow, yhigh)
    oper = with_outer(observe, faces, diffusivity, inner, points)
    oper = scattered(oper)
    right, left, image, few = bases(*gram, start_block, extra, few_ctrl)
    blocks = gathered(projected_copies(oper, left, few))
    mass, state, inputs, outputs = finish(order, right, left, image, *blocks)
    return mass, state, inputs.T, outputs


def solution(mesh):
    slab = mesh.shape["slab"]
    torus = Mesh(
        mesh.devices.reshape(slab // 2, 2, mesh.shape["sub"]), ("chip", "core", "sub")
    )
    slabs = ("chip", "core")
    placed = (
        P(slabs, "sub", None, None),
        P(slabs, "sub", None, None),
        P(slabs, "sub"),
        P(None, slabs, "sub"),
        P(None, slabs, "sub"),
        P(),
        P(),
    )
    return jax.shard_map(
        reduced, mesh=torus, in_specs=placed, out_specs=(P(), P(), P(), P()), check_vma=False
    )
```

```python
import functools

import jax
import jax.numpy as jnp
from jax import lax
from jax.experimental import pallas as pl
from jax.experimental.pallas import tpu as pltpu
from jax.sharding import Mesh
from jax.sharding import PartitionSpec as P


CHIPS = ("chip", "sub")
F32 = jnp.float32
BF16 = jnp.bfloat16
PANEL = 32
AHEAD = 2


def split2(x):
    high = x.astype(BF16)
    return high, (x - high.astype(F32)).astype(BF16)


def split3(x):
    high = x.astype(BF16)
    rest = x - high.astype(F32)
    mid = rest.astype(BF16)
    return high, mid, (rest - mid.astype(F32)).astype(BF16)


def product(a, b, contract=((1,), (0,))):
    return lax.dot_general(a, b, (contract, ((), ())), preferred_element_type=F32)


def product3(a, b, contract=((1,), (0,))):
    ah, al = split2(a)
    bh, bl = split2(b)
    return product(ah, bh, contract) + (product(ah, bl, contract) + product(al, bh, contract))


def product6(a, b, contract=((1,), (0,))):
    a0, a1, a2 = split3(a)
    b0, b1, b2 = split3(b)
    dot = functools.partial(product, contract=contract)
    small = dot(a1, b1) + (dot(a0, b2) + dot(a2, b0))
    return dot(a0, b0) + ((dot(a0, b1) + dot(a1, b0)) + small)


def rows_split(rows):
    both = jnp.concatenate([rows, rows], axis=0)
    high = both.astype(BF16).astype(F32)
    place = lax.broadcasted_iota(jnp.int32, both.shape, 0)
    halves = jnp.where(place < rows.shape[0], high, both - high)
    return jnp.concatenate([halves, jnp.zeros_like(halves)], axis=0).astype(BF16)


def add_products(total, turned, right, extra=None, few=None):
    count = turned.shape[0]
    th, tl = split2(turned)
    rh, rl = split2(right)
    left = jnp.concatenate([th, tl, th], axis=1)
    if few is not None:
        bottom = jnp.concatenate([few, jnp.zeros_like(few), few], axis=1)
        left = jnp.concatenate([left, bottom], axis=0)
    result = product(left, jnp.concatenate([rh, rh, rl], axis=0))
    total[...] += result[:count]
    if few is not None:
        extra[...] += result[count:]


def plane_rows(rows, plane, first, size):
    chosen = jnp.zeros((rows.shape[0], size), F32)
    for p in range(rows.shape[1]):
        chosen = jnp.where(plane == p, rows[:, p, pl.ds(first, size)], chosen)
    return rows_split(chosen)


def core_index():
    return lax.axis_index("core").reshape(1).astype(jnp.int32)


def in_hbm(value):
    return pltpu.with_memory_space_constraint(value, pltpu.HBM)


def gram_kernel(
    obs, ctrl, sense,
    gram, few_far, zlow, zhigh, ylow, yhigh,
    obs_here, ctrl_here, total, extra, sense_here, obs_sems, ctrl_sems, z_sems, low_sems, high_sems, other_sems,
):
    steps, rows, _ = obs.shape
    points = ylow.shape[1]

    def copies(i):
        return (
            pltpu.make_async_copy(obs.at[i], obs_here.at[i], obs_sems.at[i]),
            pltpu.make_async_copy(ctrl.at[i], ctrl_here.at[i], ctrl_sems.at[i]),
        )

    def z_copy(i):
        source = ctrl_here.at[i if i < 2 else steps - 4 + i]
        return pltpu.make_async_copy(source, (zlow if i < 2 else zhigh).at[i % 2], z_sems.at[i])

    def low_copy(p):
        source = ctrl_here.at[2 * p, pl.ds(0, points)]
        return pltpu.make_async_copy(source, ylow.at[p], low_sems.at[p])

    def high_copy(p):
        source = ctrl_here.at[2 * p + 1, pl.ds(rows - points, points)]
        return pltpu.make_async_copy(source, yhigh.at[p], high_sems.at[p])

    sense_copy = pltpu.make_async_copy(sense, sense_here, other_sems.at[0])
    for i in range(AHEAD):
        for copy in copies(i):
            copy.start()
        if i == 0:
            sense_copy.start()
    total[...] = jnp.zeros_like(total)
    extra[...] = jnp.zeros_like(extra)
    sense_copy.wait()

    @pl.loop(0, steps)
    def _(i):
        for copy in copies(i):
            copy.wait()

        @pl.when(i + AHEAD < steps)
        def _():
            for copy in copies(i + AHEAD):
                copy.start()

        for j in range(4):

            @pl.when(i == (j if j < 2 else steps - 4 + j))
            def _():
                z_copy(j).start()

        @pl.when(i % 2 == 0)
        def _():
            low_copy(i // 2).start()

        @pl.when(i % 2 == 1)
        def _():
            high_copy(i // 2).start()

        first = pl.multiple_of((i % 2) * rows, 128)
        some = plane_rows(sense_here, i // 2, first, rows)
        add_products(total, obs_here[i].T, ctrl_here[i], extra, some)

    few_copy = pltpu.make_async_copy(extra, few_far, other_sems.at[0])
    few_copy.start()
    width = total.shape[1] // 2
    for side in range(2):
        cols = total[:, side * width : (side + 1) * width]
        gram[:, side] = cols.reshape(gram.shape[0], gram.shape[2], width)
    few_copy.wait()
    for i in range(4):
        z_copy(i).wait()
    for p in range(steps // 2):
        low_copy(p).wait()
        high_copy(p).wait()


def local_gram(observe, control, sense, points):
    steps, rows, rank = observe.shape
    anywhere = pl.BlockSpec(memory_space=pltpu.HBM)
    vmem = pl.BlockSpec(memory_space=pltpu.VMEM)
    face = pltpu.HBM((2, rows, rank), F32)
    edge = pltpu.HBM((steps // 2, points, rank), F32)
    return pl.pallas_call(
        gram_kernel,
        in_specs=[anywhere] * 3,
        out_specs=[vmem] + [anywhere] * 5,
        out_shape=[
            jax.ShapeDtypeStruct((rank // 8, 2, 8, rank // 2), F32),
            pltpu.HBM((16, rank), F32),
            face,
            face,
            edge,
            edge,
        ],
        scratch_shapes=[
            pltpu.VMEM((steps, rows, rank), F32),
            pltpu.VMEM((steps, rows, rank), F32),
            pltpu.VMEM((rank, rank), F32),
            pltpu.VMEM((16, rank), F32),
            pltpu.VMEM(sense.shape, F32),
            pltpu.SemaphoreType.DMA((steps,)),
            pltpu.SemaphoreType.DMA((steps,)),
            pltpu.SemaphoreType.DMA((4,)),
            pltpu.SemaphoreType.DMA((steps // 2,)),
            pltpu.SemaphoreType.DMA((steps // 2,)),
            pltpu.SemaphoreType.DMA((1,)),
        ],
        compiler_params=pltpu.CompilerParams(vmem_limit_bytes=36 << 20),
        cost_estimate=pl.CostEstimate(
            flops=6 * steps * rows * rank * rank, bytes_accessed=24 << 20, transcendentals=0
        ),
        name="local_gram",
    )(in_hbm(observe), in_hbm(control), in_hbm(sense))


def inner_kernel(
    points, obs_far, ctrl_far, conduct, drive,
    total_far, extra_far, total, extra, obs, ctrl, conduct_here, drive_here, sems, obs_sems, ctrl_sems,
):
    steps, rows, rank = obs.shape
    small = [
        pltpu.make_async_copy(conduct, conduct_here, sems.at[0]),
        pltpu.make_async_copy(drive, drive_here, sems.at[1]),
    ]

    def ctrl_copy(i):
        return pltpu.make_async_copy(ctrl_far.at[i], ctrl.at[i + 2], ctrl_sems.at[i])

    def obs_copy(i):
        return pltpu.make_async_copy(obs_far.at[i], obs.at[i], obs_sems.at[i])

    for i in (0, 1, 2):
        ctrl_copy(i).start()
    obs_copy(0).start()
    for copy in small:
        copy.start()
    ctrl_copy(3).start()
    obs_copy(1).start()
    total[...] = jnp.zeros_like(total)
    extra[...] = jnp.zeros_like(extra)
    for i in (0, 1, steps + 2, steps + 3):
        ctrl[i] = jnp.zeros((rows, rank), F32)
    for copy in small:
        copy.wait()
    ctrl_copy(0).wait()
    ctrl_copy(1).wait()

    @pl.loop(0, steps)
    def _(i):
        @pl.when(i + 2 < steps)
        def _():
            ctrl_copy(i + 2).wait()
            obs_copy(i + 2).start()

        @pl.when(i + 4 < steps)
        def _():
            ctrl_copy(i + 4).start()

        obs_copy(i).wait()
        half = i % 2
        center = ctrl[i + 2]
        beside = ctrl[i + 4] + ctrl[i]
        before = half.astype(F32) * ctrl[i + 1, rows - points :]
        after = (1 - half).astype(F32) * ctrl[i + 3, :points]
        beside = beside + jnp.concatenate([before, center[: rows - points]], axis=0)
        beside = beside + jnp.concatenate([center[points:], after], axis=0)
        place = lax.broadcasted_iota(jnp.int32, (rows, rank), 0) % points
        beside = beside + jnp.where(place > 0, pltpu.roll(center, 1, 0), 0.0)
        beside = beside + jnp.where(place < points - 1, pltpu.roll(center, rows - 1, 0), 0.0)
        first = pl.multiple_of(half * rows, 128)
        scale = conduct_here[pl.ds(i // 2, 1), pl.ds(first, rows)] * (1.0 / 6.0)
        applied = (beside - 6.0 * center).T * scale
        some = plane_rows(drive_here, i // 2, first, rows)
        add_products(total, applied, obs[i], extra, some)

    results = [
        pltpu.make_async_copy(total, total_far, sems.at[0]),
        pltpu.make_async_copy(extra, extra_far, sems.at[1]),
    ]
    for copy in results:
        copy.start()
    for copy in results:
        copy.wait()


def inner_operator(observe, control, conduct, drive, points):
    steps, rows, rank = control.shape
    anywhere = pl.BlockSpec(memory_space=pltpu.HBM)
    return pl.pallas_call(
        functools.partial(inner_kernel, points),
        in_specs=[anywhere] * 4,
        out_specs=[anywhere] * 2,
        out_shape=[
            pltpu.HBM((rank, rank), F32),
            pltpu.HBM((16, rank), F32),
        ],
        scratch_shapes=[
            pltpu.VMEM((rank, rank), F32),
            pltpu.VMEM((16, rank), F32),
            pltpu.VMEM((steps, rows, rank), F32),
            pltpu.VMEM((steps + 4, rows, rank), F32),
            pltpu.VMEM(conduct.shape, F32),
            pltpu.VMEM(drive.shape, F32),
            pltpu.SemaphoreType.DMA((2,)),
            pltpu.SemaphoreType.DMA((steps,)),
            pltpu.SemaphoreType.DMA((steps,)),
        ],
        compiler_params=pltpu.CompilerParams(vmem_limit_bytes=40 << 20),
        cost_estimate=pl.CostEstimate(
            flops=6 * steps * rows * rank * rank, bytes_accessed=18 << 20, transcendentals=0
        ),
        name="inner_operator",
    )(in_hbm(observe), in_hbm(control), in_hbm(conduct), in_hbm(drive))


def outer_kernel(
    points, obs, zlow, zhigh, conduct, inner, ylow, yhigh,
    out, z_field, z_obs, y_obs, conduct_here, total, inner_here, sems, obs_sems,
):
    steps, rows, rank = obs.shape
    planes = steps // 2
    conduct_copy = pltpu.make_async_copy(conduct, conduct_here, sems.at[0])
    inner_copy = pltpu.make_async_copy(inner, inner_here, sems.at[7])
    y_near = [
        pltpu.make_async_copy(
            obs.at[2 * p + i, pl.ds(i * (rows - points), points)],
            y_obs.at[pl.ds((planes * i + p) * points, points)],
            obs_sems.at[4 + planes * i + p],
        )
        for i in range(2)
        for p in range(planes)
    ]

    def z_far(i):
        face = zlow if i < 2 else zhigh
        return pltpu.make_async_copy(face.at[i % 2], z_field.at[i], sems.at[3 + i])

    def z_near(i):
        place = i if i < 2 else steps - 4 + i
        return pltpu.make_async_copy(obs.at[place], z_obs.at[i], obs_sems.at[i])

    conduct_copy.start()
    for copy in y_near:
        copy.start()
    for i in range(4):
        z_far(i).start()
        z_near(i).start()
        if i == 1:
            inner_copy.start()
    conduct_copy.wait()
    scale = conduct_here[...] * (1.0 / 6.0)
    for copy in y_near:
        copy.wait()
    turned = [
        (yhigh if i else ylow)[p].T * scale[p : p + 1, i * (2 * rows - points) :][:, :points]
        for i in range(2)
        for p in range(planes)
    ]
    total[...] = jnp.zeros_like(total)
    add_products(total, jnp.concatenate(turned, axis=1), y_obs[...])

    @pl.loop(0, 4)
    def _(block):
        for i in range(4):

            @pl.when(block == i)
            def _():
                z_far(i).wait()
                z_near(i).wait()

        plane = (planes - 1) * (block // 2)
        first = pl.multiple_of((block % 2) * rows, 128)
        lanes = conduct_here[pl.ds(plane, 1), pl.ds(first, rows)] * (1.0 / 6.0)
        add_products(total, z_field[block].T * lanes, z_obs[block])

    inner_copy.wait()
    width = rank // 2
    for side in range(2):
        place = slice(side * width, (side + 1) * width)
        cols = total[:, place] + inner_here[:, place]
        out[:, side] = cols.reshape(out.shape[0], out.shape[2], width)


def with_outer(observe, faces, conduct, inner, points):
    steps, rows, rank = observe.shape
    anywhere = pl.BlockSpec(memory_space=pltpu.HBM)
    vmem = pl.BlockSpec(memory_space=pltpu.VMEM)
    return pl.pallas_call(
        functools.partial(outer_kernel, points),
        in_specs=[anywhere] * 5 + [vmem] * 2,
        out_specs=vmem,
        out_shape=jax.ShapeDtypeStruct((rank // 8, 2, 8, rank // 2), F32),
        scratch_shapes=[
            pltpu.VMEM((4, rows, rank), F32),
            pltpu.VMEM((4, rows, rank), F32),
            pltpu.VMEM((steps * points, rank), F32),
            pltpu.VMEM(conduct.shape, F32),
            pltpu.VMEM((rank, rank), F32),
            pltpu.VMEM((rank, rank), F32),
            pltpu.SemaphoreType.DMA((8,)),
            pltpu.SemaphoreType.DMA((4 + steps,)),
        ],
        compiler_params=pltpu.CompilerParams(vmem_limit_bytes=36 << 20),
        cost_estimate=pl.CostEstimate(
            flops=30 * rows * rank * rank, bytes_accessed=7 << 20, transcendentals=0
        ),
        name="outer_operator",
    )(*map(in_hbm, (observe, *faces[:2], conduct, inner)), *faces[2:])


def sum_kernel(parts, out):
    whole = jnp.sum(parts[...], axis=0, keepdims=True)
    out[...] = jnp.broadcast_to(whole, out.shape)


def swapped(value):
    return lax.ppermute(value, "core", [(0, 1), (1, 0)])


def scattered(parts):
    tiles = parts.reshape(-1, *parts.shape[2:])
    return lax.all_to_all(tiles, CHIPS + ("core",), 0, 0, tiled=True)


def summed_copies(arrived):
    return pl.pallas_call(
        sum_kernel,
        out_shape=jax.ShapeDtypeStruct((arrived.shape[0] // 2, *arrived.shape[1:]), F32),
        compiler_params=pltpu.CompilerParams(vmem_limit_bytes=6 << 20),
        cost_estimate=pl.CostEstimate(
            flops=arrived.size, bytes_accessed=8 * arrived.size, transcendentals=0
        ),
        name="sum_gram",
    )(arrived)


def project_kernel(side, parts, left, few, out):
    block = jnp.sum(parts[...], axis=0)
    half = left.shape[1] // 2
    mine = jnp.where(side[0] == 0, left[:, :half], left[:, half:])
    turned = product3(block, mine, ((1,), (1,)))
    out[...] = jnp.concatenate([turned, few[...]], axis=1)


def spread_kernel(side, mine, theirs, out):
    both = mine[...] + theirs[...]
    half = both.shape[1] // 2
    chosen = jnp.where(side[0] == 0, both[:, :half], both[:, half:])
    out[...] = jnp.broadcast_to(chosen[None], out.shape)


def projected_copies(arrived, left, few):
    smem = pl.BlockSpec(memory_space=pltpu.SMEM)
    vmem = pl.BlockSpec(memory_space=pltpu.VMEM)
    cost = pl.CostEstimate(
        flops=arrived.size, bytes_accessed=8 * arrived.size, transcendentals=0
    )
    mine = pl.pallas_call(
        project_kernel,
        in_specs=[smem, vmem, vmem, vmem],
        out_specs=vmem,
        out_shape=jax.ShapeDtypeStruct((8, 256), F32),
        compiler_params=pltpu.CompilerParams(vmem_limit_bytes=8 << 20),
        cost_estimate=cost,
        name="project",
    )(core_index(), arrived, left, few)
    return pl.pallas_call(
        spread_kernel,
        in_specs=[smem, vmem, vmem],
        out_specs=vmem,
        out_shape=jax.ShapeDtypeStruct((arrived.shape[0] // 2, 8, 128), F32),
        compiler_params=pltpu.CompilerParams(vmem_limit_bytes=4 << 20),
        cost_estimate=cost,
        name="spread",
    )(core_index(), mine, swapped(mine))


def gathered(copies):
    mine = lax.all_to_all(copies, CHIPS, 0, 0, tiled=True)
    return mine, swapped(mine)


def lane(block, index):
    where = jnp.full(block.shape, index, jnp.int32)
    return jnp.take_along_axis(block, where, axis=1, mode="promise_in_bounds")


def inverse_factor(work):
    size = work.shape[0]
    groups = PANEL // 8

    @pl.loop(0, size // PANEL)
    def _(turn):
        first = pl.multiple_of(turn * PANEL, PANEL)
        panel = [work[pl.ds(first + 8 * g, 8), :] for g in range(groups)]
        columns = {}
        for k in range(PANEL):
            for g in range(k // 8, groups):
                columns[k, g] = lane(panel[g][:, :128], first + k)
        place = lax.broadcasted_iota(jnp.int32, (8, 128), 0)
        wide_place = lax.broadcasted_iota(jnp.int32, (8, 256), 0)
        for j in range(PANEL):
            gj, sj = divmod(j, 8)
            pivot = jnp.broadcast_to(columns[j, gj][sj : sj + 1], (8, 128))
            scale = lax.rsqrt(pivot)
            lower = {g: columns[j, g] * scale for g in range(gj, groups)}
            row = jnp.broadcast_to(panel[gj][sj : sj + 1], (8, 256))
            row = row * jnp.concatenate([scale, scale], axis=1)
            for k in range(j + 1, PANEL):
                gk, sk = divmod(k, 8)
                across = jnp.broadcast_to(lower[gk][sk : sk + 1], (8, 128))
                for g in range(gk, groups):
                    columns[k, g] = columns[k, g] - lower[g] * across
            for g in range(gj, groups):
                weight = lower[g]
                if g == gj:
                    weight = jnp.where(place > sj, weight, 0.0)
                wide = jnp.concatenate([weight, weight], axis=1)
                panel[g] = panel[g] - wide * row
            panel[gj] = jnp.where(wide_place == sj, row, panel[gj])
        for g in range(groups):
            work[pl.ds(first + 8 * g, 8), :] = panel[g]

        @pl.when(turn + 1 < size // PANEL)
        def _():
            done = jnp.concatenate(panel, axis=0)
            u0, u1, u2 = split3(done)
            left = jnp.concatenate([u0, u0, u1, u1, u0, u2], axis=0)[:, :size]
            right = jnp.concatenate([u0, u1, u0, u1, u2, u0], axis=0)
            change = product(left, right, ((0,), (0,)))
            below = lax.broadcasted_iota(jnp.int32, change.shape, 0) >= first + PANEL
            work[...] -= jnp.where(below, change, 0.0)


def bases_kernel(
    core, mine, theirs, start, drive_far, sense_far,
    right_out, left_out, image_out, few_out,
    high, low, basis, work, right, image, drive, sense, sems,
):
    small = [
        pltpu.make_async_copy(drive_far, drive, sems.at[2]),
        pltpu.make_async_copy(sense_far, sense, sems.at[3]),
    ]
    for copy in small:
        copy.start()
    right_copy = pltpu.make_async_copy(right, right_out, sems.at[0])
    image_copy = pltpu.make_async_copy(image, image_out, sems.at[1])
    rank = high.shape[0]
    half = rank // 2
    for slot, part in enumerate((mine, theirs)):
        place = pl.ds(pl.multiple_of((core[0] ^ slot) * half, 128), half)
        high[:, place], low[:, place] = split2(part[...].reshape(rank, half))
    basis[...] = start[...].T
    size = basis.shape[0]
    eye = (
        lax.broadcasted_iota(jnp.int32, (size, size), 0)
        == lax.broadcasted_iota(jnp.int32, (size, size), 1)
    ).astype(F32)

    @pl.loop(0, 4)
    def _(turn):
        for parity, contract in enumerate((((1,), (0,)), ((1,), (1,)))):

            @pl.when(turn % 2 == parity)
            def _():
                bh, bl = split2(basis[...])
                small = product(bh, low[...], contract) + product(bl, high[...], contract)
                image[...] = product(bh, high[...], contract) + small

        @pl.when(turn == 3)
        def _():
            image_copy.start()

        held = image[...]
        work[:, :size] = product6(held, held, ((1,), (1,)))
        work[:, size:] = eye
        inverse_factor(work)
        basis[...] = product6(work[:, size:], held)

        @pl.when(turn == 2)
        def _():
            right[...] = basis[...]
            right_copy.start()

    left_out[...] = basis[...]
    for copy in small:
        copy.wait()
    rows = jnp.concatenate([drive[0:4] + drive[4:8], sense[0:4] + sense[4:8]], axis=0)
    both = ((1,), (1,))
    place = lax.broadcasted_iota(jnp.int32, few_out.shape, 0)
    by_left, by_right = product3(rows, basis[...], both), product3(rows, right[...], both)
    few_out[...] = jnp.where(place < 4, by_left, by_right)
    right_copy.wait()
    image_copy.wait()


def bases(mine, theirs, start, drive, sense):
    rank, size = start.shape
    shape = jax.ShapeDtypeStruct((size, rank), F32)
    vmem = pl.BlockSpec(memory_space=pltpu.VMEM)
    anywhere = pl.BlockSpec(memory_space=pltpu.HBM)
    return pl.pallas_call(
        bases_kernel,
        in_specs=[pl.BlockSpec(memory_space=pltpu.SMEM)] + [vmem] * 3 + [anywhere] * 2,
        out_specs=[anywhere, vmem, anywhere, vmem],
        out_shape=[
            pltpu.HBM((size, rank), F32),
            shape,
            pltpu.HBM((size, rank), F32),
            jax.ShapeDtypeStruct((8, size), F32),
        ],
        scratch_shapes=[
            pltpu.VMEM((rank, rank), BF16),
            pltpu.VMEM((rank, rank), BF16),
            pltpu.VMEM((size, rank), F32),
            pltpu.VMEM((size, 2 * size), F32),
            pltpu.VMEM((size, rank), F32),
            pltpu.VMEM((size, rank), F32),
            pltpu.VMEM(drive.shape, F32),
            pltpu.VMEM(sense.shape, F32),
            pltpu.SemaphoreType.DMA((4,)),
        ],
        compiler_params=pltpu.CompilerParams(vmem_limit_bytes=16 << 20),
        cost_estimate=pl.CostEstimate(
            flops=20_000_000_000, bytes_accessed=4 << 20, transcendentals=0
        ),
        name="bases",
    )(core_index(), mine, theirs, start, in_hbm(drive), in_hbm(sense))


def finish_kernel(order, side, right, left, image, mine, theirs, mass, state, inputs, outputs):
    size, rank = right.shape
    first = side[0] == 0
    turned = jnp.where(first, mine[...], theirs[...]).reshape(rank, size)
    few = jnp.sum(jnp.where(first, theirs[...], mine[...]), axis=0)
    kept_col = lax.broadcasted_iota(jnp.int32, (size, size), 0) < order[0]
    kept_row = lax.broadcasted_iota(jnp.int32, (size, size), 1) < order[0]
    kept = jnp.logical_and(kept_col, kept_row).astype(F32)
    mass[...] = kept * product6(left[...], image[...], ((1,), (1,)))
    state[...] = kept * product3(right[...], turned).T
    few = kept_row[:8].astype(F32) * few
    inputs[...] = few[:4]
    outputs[...] = few[4:]


def finish(order, right, left, image, mine, theirs):
    size, _ = right.shape
    vmem = pl.BlockSpec(memory_space=pltpu.VMEM)
    return pl.pallas_call(
        finish_kernel,
        in_specs=[pl.BlockSpec(memory_space=pltpu.SMEM)] * 2 + [vmem] * 5,
        out_specs=[vmem] * 4,
        out_shape=[
            jax.ShapeDtypeStruct((size, size), F32),
            jax.ShapeDtypeStruct((size, size), F32),
            jax.ShapeDtypeStruct((4, size), F32),
            jax.ShapeDtypeStruct((4, size), F32),
        ],
        compiler_params=pltpu.CompilerParams(vmem_limit_bytes=16 << 20),
        cost_estimate=pl.CostEstimate(
            flops=1_000_000_000, bytes_accessed=4 << 20, transcendentals=0
        ),
        name="finish",
    )(order, core_index(), right, left, image, mine, theirs)


def from_neighbours(low_face, high_face, axis):
    count = lax.axis_size(axis)
    up = [(i, i + 1) for i in range(count - 1)]
    down = [(b, a) for a, b in up]
    return lax.ppermute(high_face, axis, up), lax.ppermute(low_face, axis, down)


def reduced(factor_obs, factor_ctrl, diffusivity, input_map, output_map, start_block, order):
    planes, lines, points, rank = factor_ctrl.shape
    halves = (2 * planes, lines * points // 2, rank)
    observe = factor_obs.reshape(halves)
    control = factor_ctrl.reshape(halves)
    gram, few_ctrl, zlow, zhigh, ylow, yhigh = local_gram(
        observe, control, output_map, points
    )
    arrived = scattered(gram)
    zlow, zhigh = from_neighbours(zlow, zhigh, ("chip", "core"))
    ylow, yhigh = from_neighbours(ylow, yhigh, "sub")
    inner, extra = inner_operator(observe, control, diffusivity, input_map, points)
    gram = gathered(summed_copies(arrived))
    faces = (zlow, zhigh, ylow, yhigh)
    oper = with_outer(observe, faces, diffusivity, inner, points)
    oper = scattered(oper)
    right, left, image, few = bases(*gram, start_block, extra, few_ctrl)
    blocks = gathered(projected_copies(oper, left, few))
    mass, state, inputs, outputs = finish(order, right, left, image, *blocks)
    return mass, state, inputs.T, outputs


def solution(mesh):
    slab = mesh.shape["slab"]
    torus = Mesh(
        mesh.devices.reshape(slab // 2, 2, mesh.shape["sub"]), ("chip", "core", "sub")
    )
    slabs = ("chip", "core")
    placed = (
        P(slabs, "sub", None, None),
        P(slabs, "sub", None, None),
        P(slabs, "sub"),
        P(None, slabs, "sub"),
        P(None, slabs, "sub"),
        P(),
        P(),
    )
    return jax.shard_map(
        reduced, mesh=torus, in_specs=placed, out_specs=(P(), P(), P(), P()), check_vma=False
    )
```

```python
import functools

import jax
import jax.numpy as jnp
from jax import lax
from jax.experimental import pallas as pl
from jax.experimental.pallas import tpu as pltpu
from jax.sharding import Mesh
from jax.sharding import PartitionSpec as P


CHIPS = ("chip", "sub")
F32 = jnp.float32
BF16 = jnp.bfloat16
PANEL = 32
AHEAD = 2


def split2(x):
    high = x.astype(BF16)
    return high, (x - high.astype(F32)).astype(BF16)


def split3(x):
    high = x.astype(BF16)
    rest = x - high.astype(F32)
    mid = rest.astype(BF16)
    return high, mid, (rest - mid.astype(F32)).astype(BF16)


def product(a, b, contract=((1,), (0,))):
    return lax.dot_general(a, b, (contract, ((), ())), preferred_element_type=F32)


def product3(a, b, contract=((1,), (0,))):
    ah, al = split2(a)
    bh, bl = split2(b)
    return product(ah, bh, contract) + (product(ah, bl, contract) + product(al, bh, contract))


def product6(a, b, contract=((1,), (0,))):
    a0, a1, a2 = split3(a)
    b0, b1, b2 = split3(b)
    dot = functools.partial(product, contract=contract)
    small = dot(a1, b1) + (dot(a0, b2) + dot(a2, b0))
    return dot(a0, b0) + ((dot(a0, b1) + dot(a1, b0)) + small)


def rows_split(rows):
    both = jnp.concatenate([rows, rows], axis=0)
    high = both.astype(BF16).astype(F32)
    place = lax.broadcasted_iota(jnp.int32, both.shape, 0)
    halves = jnp.where(place < rows.shape[0], high, both - high)
    return jnp.concatenate([halves, jnp.zeros_like(halves)], axis=0).astype(BF16)


def add_products(total, turned, right, extra=None, few=None):
    count = turned.shape[0]
    th, tl = split2(turned)
    rh, rl = split2(right)
    left = jnp.concatenate([th, tl, th], axis=1)
    if few is not None:
        bottom = jnp.concatenate([few, jnp.zeros_like(few), few], axis=1)
        left = jnp.concatenate([left, bottom], axis=0)
    result = product(left, jnp.concatenate([rh, rh, rl], axis=0))
    total[...] += result[:count]
    if few is not None:
        extra[...] += result[count:]


def plane_rows(rows, plane, first, size):
    chosen = jnp.zeros((rows.shape[0], size), F32)
    for p in range(rows.shape[1]):
        chosen = jnp.where(plane == p, rows[:, p, pl.ds(first, size)], chosen)
    return rows_split(chosen)


def core_index():
    return lax.axis_index("core").reshape(1).astype(jnp.int32)


def in_hbm(value):
    return pltpu.with_memory_space_constraint(value, pltpu.HBM)


def gram_kernel(
    obs, ctrl, sense,
    gram, few_far, zlow, zhigh, ylow, yhigh,
    obs_here, ctrl_here, total, extra, sense_here, obs_sems, ctrl_sems, z_sems, low_sems, high_sems, other_sems,
):
    steps, rows, _ = obs.shape
    points = ylow.shape[1]

    def copies(i):
        return (
            pltpu.make_async_copy(obs.at[i], obs_here.at[i], obs_sems.at[i]),
            pltpu.make_async_copy(ctrl.at[i], ctrl_here.at[i], ctrl_sems.at[i]),
        )

    def z_copy(i):
        source = ctrl_here.at[i if i < 2 else steps - 4 + i]
        return pltpu.make_async_copy(source, (zlow if i < 2 else zhigh).at[i % 2], z_sems.at[i])

    def low_copy(p):
        source = ctrl_here.at[2 * p, pl.ds(0, points)]
        return pltpu.make_async_copy(source, ylow.at[p], low_sems.at[p])

    def high_copy(p):
        source = ctrl_here.at[2 * p + 1, pl.ds(rows - points, points)]
        return pltpu.make_async_copy(source, yhigh.at[p], high_sems.at[p])

    late = steps // 2
    sense_copy = pltpu.make_async_copy(sense, sense_here, other_sems.at[0])
    for i in range(AHEAD):
        for copy in copies(i):
            copy.start()
        if i == 0:
            sense_copy.start()
    total[...] = jnp.zeros_like(total)
    extra[...] = jnp.zeros_like(extra)
    sense_copy.wait()

    @pl.loop(0, steps)
    def _(i):
        for copy in copies(i):
            copy.wait()

        @pl.when(i + AHEAD < steps)
        def _():
            for copy in copies(i + AHEAD):
                copy.start()

        for j in range(4):

            @pl.when(i == (j + late if j < 2 else steps - 4 + j))
            def _():
                z_copy(j).start()

        @pl.when(i == late)
        def _():
            for p in range(late // 2):
                low_copy(p).start()
                high_copy(p).start()

        @pl.when(jnp.logical_and(i >= late, i % 2 == 0))
        def _():
            low_copy(i // 2).start()

        @pl.when(jnp.logical_and(i > late, i % 2 == 1))
        def _():
            high_copy(i // 2).start()

        first = pl.multiple_of((i % 2) * rows, 128)
        some = plane_rows(sense_here, i // 2, first, rows)
        add_products(total, obs_here[i].T, ctrl_here[i], extra, some)

    few_copy = pltpu.make_async_copy(extra, few_far, other_sems.at[0])
    few_copy.start()
    width = total.shape[1] // 2
    for side in range(2):
        cols = total[:, side * width : (side + 1) * width]
        gram[:, side] = cols.reshape(gram.shape[0], gram.shape[2], width)
    few_copy.wait()
    for i in range(4):
        z_copy(i).wait()
    for p in range(steps // 2):
        low_copy(p).wait()
        high_copy(p).wait()


def local_gram(observe, control, sense, points):
    steps, rows, rank = observe.shape
    anywhere = pl.BlockSpec(memory_space=pltpu.HBM)
    vmem = pl.BlockSpec(memory_space=pltpu.VMEM)
    face = pltpu.HBM((2, rows, rank), F32)
    edge = pltpu.HBM((steps // 2, points, rank), F32)
    return pl.pallas_call(
        gram_kernel,
        in_specs=[anywhere] * 3,
        out_specs=[vmem] + [anywhere] * 5,
        out_shape=[
            jax.ShapeDtypeStruct((rank // 8, 2, 8, rank // 2), F32),
            pltpu.HBM((16, rank), F32),
            face,
            face,
            edge,
            edge,
        ],
        scratch_shapes=[
            pltpu.VMEM((steps, rows, rank), F32),
            pltpu.VMEM((steps, rows, rank), F32),
            pltpu.VMEM((rank, rank), F32),
            pltpu.VMEM((16, rank), F32),
            pltpu.VMEM(sense.shape, F32),
            pltpu.SemaphoreType.DMA((steps,)),
            pltpu.SemaphoreType.DMA((steps,)),
            pltpu.SemaphoreType.DMA((4,)),
            pltpu.SemaphoreType.DMA((steps // 2,)),
            pltpu.SemaphoreType.DMA((steps // 2,)),
            pltpu.SemaphoreType.DMA((1,)),
        ],
        compiler_params=pltpu.CompilerParams(vmem_limit_bytes=36 << 20),
        cost_estimate=pl.CostEstimate(
            flops=6 * steps * rows * rank * rank, bytes_accessed=24 << 20, transcendentals=0
        ),
        name="local_gram",
    )(in_hbm(observe), in_hbm(control), in_hbm(sense))


def inner_kernel(
    points, obs_far, ctrl_far, conduct, drive,
    total_far, extra_far, total, extra, obs, ctrl, conduct_here, drive_here, sems, obs_sems, ctrl_sems,
):
    steps, rows, rank = obs.shape
    small = [
        pltpu.make_async_copy(conduct, conduct_here, sems.at[0]),
        pltpu.make_async_copy(drive, drive_here, sems.at[1]),
    ]

    def ctrl_copy(i):
        return pltpu.make_async_copy(ctrl_far.at[i], ctrl.at[i + 2], ctrl_sems.at[i])

    def obs_copy(i):
        return pltpu.make_async_copy(obs_far.at[i], obs.at[i], obs_sems.at[i])

    for i in (0, 1, 2):
        ctrl_copy(i).start()
    obs_copy(0).start()
    for copy in small:
        copy.start()
    ctrl_copy(3).start()
    obs_copy(1).start()
    total[...] = jnp.zeros_like(total)
    extra[...] = jnp.zeros_like(extra)
    for i in (0, 1, steps + 2, steps + 3):
        ctrl[i] = jnp.zeros((rows, rank), F32)
    for copy in small:
        copy.wait()
    ctrl_copy(0).wait()
    ctrl_copy(1).wait()

    @pl.loop(0, steps)
    def _(i):
        @pl.when(i + 2 < steps)
        def _():
            ctrl_copy(i + 2).wait()
            obs_copy(i + 2).start()

        @pl.when(i + 4 < steps)
        def _():
            ctrl_copy(i + 4).start()

        obs_copy(i).wait()
        half = i % 2
        center = ctrl[i + 2]
        beside = ctrl[i + 4] + ctrl[i]
        before = half.astype(F32) * ctrl[i + 1, rows - points :]
        after = (1 - half).astype(F32) * ctrl[i + 3, :points]
        beside = beside + jnp.concatenate([before, center[: rows - points]], axis=0)
        beside = beside + jnp.concatenate([center[points:], after], axis=0)
        place = lax.broadcasted_iota(jnp.int32, (rows, rank), 0) % points
        beside = beside + jnp.where(place > 0, pltpu.roll(center, 1, 0), 0.0)
        beside = beside + jnp.where(place < points - 1, pltpu.roll(center, rows - 1, 0), 0.0)
        first = pl.multiple_of(half * rows, 128)
        scale = conduct_here[pl.ds(i // 2, 1), pl.ds(first, rows)] * (1.0 / 6.0)
        applied = (beside - 6.0 * center).T * scale
        some = plane_rows(drive_here, i // 2, first, rows)
        add_products(total, applied, obs[i], extra, some)

    results = [
        pltpu.make_async_copy(total, total_far, sems.at[0]),
        pltpu.make_async_copy(extra, extra_far, sems.at[1]),
    ]
    for copy in results:
        copy.start()
    for copy in results:
        copy.wait()


def inner_operator(observe, control, conduct, drive, points):
    steps, rows, rank = control.shape
    anywhere = pl.BlockSpec(memory_space=pltpu.HBM)
    return pl.pallas_call(
        functools.partial(inner_kernel, points),
        in_specs=[anywhere] * 4,
        out_specs=[anywhere] * 2,
        out_shape=[
            pltpu.HBM((rank, rank), F32),
            pltpu.HBM((16, rank), F32),
        ],
        scratch_shapes=[
            pltpu.VMEM((rank, rank), F32),
            pltpu.VMEM((16, rank), F32),
            pltpu.VMEM((steps, rows, rank), F32),
            pltpu.VMEM((steps + 4, rows, rank), F32),
            pltpu.VMEM(conduct.shape, F32),
            pltpu.VMEM(drive.shape, F32),
            pltpu.SemaphoreType.DMA((2,)),
            pltpu.SemaphoreType.DMA((steps,)),
            pltpu.SemaphoreType.DMA((steps,)),
        ],
        compiler_params=pltpu.CompilerParams(vmem_limit_bytes=40 << 20),
        cost_estimate=pl.CostEstimate(
            flops=6 * steps * rows * rank * rank, bytes_accessed=18 << 20, transcendentals=0
        ),
        name="inner_operator",
    )(in_hbm(observe), in_hbm(control), in_hbm(conduct), in_hbm(drive))


def outer_kernel(
    points, obs, zlow, zhigh, conduct, inner, ylow, yhigh,
    out, z_field, z_obs, y_obs, conduct_here, total, inner_here, sems, obs_sems,
):
    steps, rows, rank = obs.shape
    planes = steps // 2
    conduct_copy = pltpu.make_async_copy(conduct, conduct_here, sems.at[0])
    inner_copy = pltpu.make_async_copy(inner, inner_here, sems.at[7])
    y_near = [
        pltpu.make_async_copy(
            obs.at[2 * p + i, pl.ds(i * (rows - points), points)],
            y_obs.at[pl.ds((planes * i + p) * points, points)],
            obs_sems.at[4 + planes * i + p],
        )
        for i in range(2)
        for p in range(planes)
    ]

    def z_far(i):
        face = zlow if i < 2 else zhigh
        return pltpu.make_async_copy(face.at[i % 2], z_field.at[i], sems.at[3 + i])

    def z_near(i):
        place = i if i < 2 else steps - 4 + i
        return pltpu.make_async_copy(obs.at[place], z_obs.at[i], obs_sems.at[i])

    conduct_copy.start()
    for copy in y_near:
        copy.start()
    for i in range(4):
        z_far(i).start()
        z_near(i).start()
        if i == 1:
            inner_copy.start()
    conduct_copy.wait()
    scale = conduct_here[...] * (1.0 / 6.0)
    for copy in y_near:
        copy.wait()
    turned = [
        (yhigh if i else ylow)[p].T * scale[p : p + 1, i * (2 * rows - points) :][:, :points]
        for i in range(2)
        for p in range(planes)
    ]
    total[...] = jnp.zeros_like(total)
    add_products(total, jnp.concatenate(turned, axis=1), y_obs[...])

    @pl.loop(0, 4)
    def _(block):
        for i in range(4):

            @pl.when(block == i)
            def _():
                z_far(i).wait()
                z_near(i).wait()

        plane = (planes - 1) * (block // 2)
        first = pl.multiple_of((block % 2) * rows, 128)
        lanes = conduct_here[pl.ds(plane, 1), pl.ds(first, rows)] * (1.0 / 6.0)
        add_products(total, z_field[block].T * lanes, z_obs[block])

    inner_copy.wait()
    width = rank // 2
    for side in range(2):
        place = slice(side * width, (side + 1) * width)
        cols = total[:, place] + inner_here[:, place]
        out[:, side] = cols.reshape(out.shape[0], out.shape[2], width)


def with_outer(observe, faces, conduct, inner, points):
    steps, rows, rank = observe.shape
    anywhere = pl.BlockSpec(memory_space=pltpu.HBM)
    vmem = pl.BlockSpec(memory_space=pltpu.VMEM)
    return pl.pallas_call(
        functools.partial(outer_kernel, points),
        in_specs=[anywhere] * 5 + [vmem] * 2,
        out_specs=vmem,
        out_shape=jax.ShapeDtypeStruct((rank // 8, 2, 8, rank // 2), F32),
        scratch_shapes=[
            pltpu.VMEM((4, rows, rank), F32),
            pltpu.VMEM((4, rows, rank), F32),
            pltpu.VMEM((steps * points, rank), F32),
            pltpu.VMEM(conduct.shape, F32),
            pltpu.VMEM((rank, rank), F32),
            pltpu.VMEM((rank, rank), F32),
            pltpu.SemaphoreType.DMA((8,)),
            pltpu.SemaphoreType.DMA((4 + steps,)),
        ],
        compiler_params=pltpu.CompilerParams(vmem_limit_bytes=36 << 20),
        cost_estimate=pl.CostEstimate(
            flops=30 * rows * rank * rank, bytes_accessed=7 << 20, transcendentals=0
        ),
        name="outer_operator",
    )(*map(in_hbm, (observe, *faces[:2], conduct, inner)), *faces[2:])


def sum_kernel(parts, out):
    whole = jnp.sum(parts[...], axis=0, keepdims=True)
    out[...] = jnp.broadcast_to(whole, out.shape)


def swapped(value):
    return lax.ppermute(value, "core", [(0, 1), (1, 0)])


def scattered(parts):
    tiles = parts.reshape(-1, *parts.shape[2:])
    return lax.all_to_all(tiles, CHIPS + ("core",), 0, 0, tiled=True)


def summed_copies(arrived):
    return pl.pallas_call(
        sum_kernel,
        out_shape=jax.ShapeDtypeStruct((arrived.shape[0] // 2, *arrived.shape[1:]), F32),
        compiler_params=pltpu.CompilerParams(vmem_limit_bytes=6 << 20),
        cost_estimate=pl.CostEstimate(
            flops=arrived.size, bytes_accessed=8 * arrived.size, transcendentals=0
        ),
        name="sum_gram",
    )(arrived)


def project_kernel(side, parts, left, few, out):
    block = jnp.sum(parts[...], axis=0)
    half = left.shape[1] // 2
    mine = jnp.where(side[0] == 0, left[:, :half], left[:, half:])
    turned = product3(block, mine, ((1,), (1,)))
    out[...] = jnp.concatenate([turned, few[...]], axis=1)


def spread_kernel(side, mine, theirs, out):
    both = mine[...] + theirs[...]
    half = both.shape[1] // 2
    chosen = jnp.where(side[0] == 0, both[:, :half], both[:, half:])
    out[...] = jnp.broadcast_to(chosen[None], out.shape)


def projected_copies(arrived, left, few):
    smem = pl.BlockSpec(memory_space=pltpu.SMEM)
    vmem = pl.BlockSpec(memory_space=pltpu.VMEM)
    cost = pl.CostEstimate(
        flops=arrived.size, bytes_accessed=8 * arrived.size, transcendentals=0
    )
    mine = pl.pallas_call(
        project_kernel,
        in_specs=[smem, vmem, vmem, vmem],
        out_specs=vmem,
        out_shape=jax.ShapeDtypeStruct((8, 256), F32),
        compiler_params=pltpu.CompilerParams(vmem_limit_bytes=8 << 20),
        cost_estimate=cost,
        name="project",
    )(core_index(), arrived, left, few)
    return pl.pallas_call(
        spread_kernel,
        in_specs=[smem, vmem, vmem],
        out_specs=vmem,
        out_shape=jax.ShapeDtypeStruct((arrived.shape[0] // 2, 8, 128), F32),
        compiler_params=pltpu.CompilerParams(vmem_limit_bytes=4 << 20),
        cost_estimate=cost,
        name="spread",
    )(core_index(), mine, swapped(mine))


def gathered(copies):
    mine = lax.all_to_all(copies, CHIPS, 0, 0, tiled=True)
    return mine, swapped(mine)


def lane(block, index):
    where = jnp.full(block.shape, index, jnp.int32)
    return jnp.take_along_axis(block, where, axis=1, mode="promise_in_bounds")


def inverse_factor(work):
    size = work.shape[0]
    groups = PANEL // 8

    @pl.loop(0, size // PANEL)
    def _(turn):
        first = pl.multiple_of(turn * PANEL, PANEL)
        panel = [work[pl.ds(first + 8 * g, 8), :] for g in range(groups)]
        columns = {}
        for k in range(PANEL):
            for g in range(k // 8, groups):
                columns[k, g] = lane(panel[g][:, :128], first + k)
        place = lax.broadcasted_iota(jnp.int32, (8, 128), 0)
        wide_place = lax.broadcasted_iota(jnp.int32, (8, 256), 0)
        for j in range(PANEL):
            gj, sj = divmod(j, 8)
            pivot = jnp.broadcast_to(columns[j, gj][sj : sj + 1], (8, 128))
            scale = lax.rsqrt(pivot)
            lower = {g: columns[j, g] * scale for g in range(gj, groups)}
            row = jnp.broadcast_to(panel[gj][sj : sj + 1], (8, 256))
            row = row * jnp.concatenate([scale, scale], axis=1)
            for k in range(j + 1, PANEL):
                gk, sk = divmod(k, 8)
                across = jnp.broadcast_to(lower[gk][sk : sk + 1], (8, 128))
                for g in range(gk, groups):
                    columns[k, g] = columns[k, g] - lower[g] * across
            for g in range(gj, groups):
                weight = lower[g]
                if g == gj:
                    weight = jnp.where(place > sj, weight, 0.0)
                wide = jnp.concatenate([weight, weight], axis=1)
                panel[g] = panel[g] - wide * row
            panel[gj] = jnp.where(wide_place == sj, row, panel[gj])
        for g in range(groups):
            work[pl.ds(first + 8 * g, 8), :] = panel[g]

        @pl.when(turn + 1 < size // PANEL)
        def _():
            done = jnp.concatenate(panel, axis=0)
            u0, u1, u2 = split3(done)
            left = jnp.concatenate([u0, u0, u1, u1, u0, u2], axis=0)[:, :size]
            right = jnp.concatenate([u0, u1, u0, u1, u2, u0], axis=0)
            change = product(left, right, ((0,), (0,)))
            below = lax.broadcasted_iota(jnp.int32, change.shape, 0) >= first + PANEL
            work[...] -= jnp.where(below, change, 0.0)


def bases_kernel(
    core, mine, theirs, start, drive_far, sense_far,
    right_out, left_out, image_out, few_out,
    high, low, basis, work, right, image, drive, sense, sems,
):
    small = [
        pltpu.make_async_copy(drive_far, drive, sems.at[2]),
        pltpu.make_async_copy(sense_far, sense, sems.at[3]),
    ]
    for copy in small:
        copy.start()
    right_copy = pltpu.make_async_copy(right, right_out, sems.at[0])
    image_copy = pltpu.make_async_copy(image, image_out, sems.at[1])
    rank = high.shape[0]
    half = rank // 2
    for slot, part in enumerate((mine, theirs)):
        place = pl.ds(pl.multiple_of((core[0] ^ slot) * half, 128), half)
        high[:, place], low[:, place] = split2(part[...].reshape(rank, half))
    basis[...] = start[...].T
    size = basis.shape[0]
    eye = (
        lax.broadcasted_iota(jnp.int32, (size, size), 0)
        == lax.broadcasted_iota(jnp.int32, (size, size), 1)
    ).astype(F32)

    @pl.loop(0, 4)
    def _(turn):
        for parity, contract in enumerate((((1,), (0,)), ((1,), (1,)))):

            @pl.when(turn % 2 == parity)
            def _():
                bh, bl = split2(basis[...])
                small = product(bh, low[...], contract) + product(bl, high[...], contract)
                image[...] = product(bh, high[...], contract) + small

        @pl.when(turn == 3)
        def _():
            image_copy.start()

        held = image[...]
        work[:, :size] = product6(held, held, ((1,), (1,)))
        work[:, size:] = eye
        inverse_factor(work)
        basis[...] = product6(work[:, size:], held)

        @pl.when(turn == 2)
        def _():
            right[...] = basis[...]
            right_copy.start()

    left_out[...] = basis[...]
    for copy in small:
        copy.wait()
    rows = jnp.concatenate([drive[0:4] + drive[4:8], sense[0:4] + sense[4:8]], axis=0)
    both = ((1,), (1,))
    place = lax.broadcasted_iota(jnp.int32, few_out.shape, 0)
    by_left, by_right = product3(rows, basis[...], both), product3(rows, right[...], both)
    few_out[...] = jnp.where(place < 4, by_left, by_right)
    right_copy.wait()
    image_copy.wait()


def bases(mine, theirs, start, drive, sense):
    rank, size = start.shape
    shape = jax.ShapeDtypeStruct((size, rank), F32)
    vmem = pl.BlockSpec(memory_space=pltpu.VMEM)
    anywhere = pl.BlockSpec(memory_space=pltpu.HBM)
    return pl.pallas_call(
        bases_kernel,
        in_specs=[pl.BlockSpec(memory_space=pltpu.SMEM)] + [vmem] * 3 + [anywhere] * 2,
        out_specs=[anywhere, vmem, anywhere, vmem],
        out_shape=[
            pltpu.HBM((size, rank), F32),
            shape,
            pltpu.HBM((size, rank), F32),
            jax.ShapeDtypeStruct((8, size), F32),
        ],
        scratch_shapes=[
            pltpu.VMEM((rank, rank), BF16),
            pltpu.VMEM((rank, rank), BF16),
            pltpu.VMEM((size, rank), F32),
            pltpu.VMEM((size, 2 * size), F32),
            pltpu.VMEM((size, rank), F32),
            pltpu.VMEM((size, rank), F32),
            pltpu.VMEM(drive.shape, F32),
            pltpu.VMEM(sense.shape, F32),
            pltpu.SemaphoreType.DMA((4,)),
        ],
        compiler_params=pltpu.CompilerParams(vmem_limit_bytes=16 << 20),
        cost_estimate=pl.CostEstimate(
            flops=20_000_000_000, bytes_accessed=4 << 20, transcendentals=0
        ),
        name="bases",
    )(core_index(), mine, theirs, start, in_hbm(drive), in_hbm(sense))


def finish_kernel(order, side, right, left, image, mine, theirs, mass, state, inputs, outputs):
    size, rank = right.shape
    first = side[0] == 0
    turned = jnp.where(first, mine[...], theirs[...]).reshape(rank, size)
    few = jnp.sum(jnp.where(first, theirs[...], mine[...]), axis=0)
    kept_col = lax.broadcasted_iota(jnp.int32, (size, size), 0) < order[0]
    kept_row = lax.broadcasted_iota(jnp.int32, (size, size), 1) < order[0]
    kept = jnp.logical_and(kept_col, kept_row).astype(F32)
    mass[...] = kept * product6(left[...], image[...], ((1,), (1,)))
    state[...] = kept * product3(right[...], turned).T
    few = kept_row[:8].astype(F32) * few
    inputs[...] = few[:4]
    outputs[...] = few[4:]


def finish(order, right, left, image, mine, theirs):
    size, _ = right.shape
    vmem = pl.BlockSpec(memory_space=pltpu.VMEM)
    return pl.pallas_call(
        finish_kernel,
        in_specs=[pl.BlockSpec(memory_space=pltpu.SMEM)] * 2 + [vmem] * 5,
        out_specs=[vmem] * 4,
        out_shape=[
            jax.ShapeDtypeStruct((size, size), F32),
            jax.ShapeDtypeStruct((size, size), F32),
            jax.ShapeDtypeStruct((4, size), F32),
            jax.ShapeDtypeStruct((4, size), F32),
        ],
        compiler_params=pltpu.CompilerParams(vmem_limit_bytes=16 << 20),
        cost_estimate=pl.CostEstimate(
            flops=1_000_000_000, bytes_accessed=4 << 20, transcendentals=0
        ),
        name="finish",
    )(order, core_index(), right, left, image, mine, theirs)


def from_neighbours(low_face, high_face, axis):
    count = lax.axis_size(axis)
    up = [(i, i + 1) for i in range(count - 1)]
    down = [(b, a) for a, b in up]
    return lax.ppermute(high_face, axis, up), lax.ppermute(low_face, axis, down)


def reduced(factor_obs, factor_ctrl, diffusivity, input_map, output_map, start_block, order):
    planes, lines, points, rank = factor_ctrl.shape
    halves = (2 * planes, lines * points // 2, rank)
    observe = factor_obs.reshape(halves)
    control = factor_ctrl.reshape(halves)
    gram, few_ctrl, zlow, zhigh, ylow, yhigh = local_gram(
        observe, control, output_map, points
    )
    arrived = scattered(gram)
    zlow, zhigh = from_neighbours(zlow, zhigh, ("chip", "core"))
    ylow, yhigh = from_neighbours(ylow, yhigh, "sub")
    inner, extra = inner_operator(observe, control, diffusivity, input_map, points)
    gram = gathered(summed_copies(arrived))
    faces = (zlow, zhigh, ylow, yhigh)
    oper = with_outer(observe, faces, diffusivity, inner, points)
    oper = scattered(oper)
    right, left, image, few = bases(*gram, start_block, extra, few_ctrl)
    blocks = gathered(projected_copies(oper, left, few))
    mass, state, inputs, outputs = finish(order, right, left, image, *blocks)
    return mass, state, inputs.T, outputs


def solution(mesh):
    slab = mesh.shape["slab"]
    torus = Mesh(
        mesh.devices.reshape(slab // 2, 2, mesh.shape["sub"]), ("chip", "core", "sub")
    )
    slabs = ("chip", "core")
    placed = (
        P(slabs, "sub", None, None),
        P(slabs, "sub", None, None),
        P(slabs, "sub"),
        P(None, slabs, "sub"),
        P(None, slabs, "sub"),
        P(),
        P(),
    )
    return jax.shard_map(
        reduced, mesh=torus, in_specs=placed, out_specs=(P(), P(), P(), P()), check_vma=False
    )
```
